16 devices in a mesh: nodes: 16 (over z, y, x, core).
Axes of the slice: x: 2, y: 2, z: 2, core: 2. Of those that a mesh axis runs over, the one named last changes fastest.
Arguments:
- adjacency: bfloat16 [16384, 16384], P('nodes')
- features: bfloat16 [16384, 128], P('nodes')
- w_one: float32 [128, 256], replicated
- w_two: float32 [256, 349], replicated
- labels: int32 [16384], P('nodes')
- label_mask: int32 [16384], P('nodes')
Outputs:
- output 1: float32 [], replicated
- output 2: float32 [128, 256], replicated
- output 3: float32 [256, 349], replicated
All inputs are finite; a program needn't handle non-finite values.
Results may differ from the reference program's by a relative error of at most 0.00164724.
Values are sent between devices in bfloat16 or wider.
A program may use at most 1 GiB of HBM per device.

```python
import jax
import jax.numpy as jnp
from jax import lax

NUM_NODES = 16384
F_IN = 128
HIDDEN = 256
CLASSES = 349
COMMUNITIES = 8
EDGE_IN = 40
EDGE_OUT = 8
HASH_MOD = 128
HASH_SHIFT = 2048
HASH_RANGE = 32768
LABEL_RATE = 4


def draw_graph(key_base):
    key_mult, key_add, key_comm = jax.random.split(key_base, 3)
    mult_ids = jax.random.randint(key_mult, (NUM_NODES,), 0, HASH_RANGE, dtype=jnp.int32)
    add_ids = jax.random.randint(key_add, (NUM_NODES,), 0, HASH_RANGE, dtype=jnp.int32)
    comm_ids = jax.random.randint(key_comm, (NUM_NODES,), 0, COMMUNITIES, dtype=jnp.int32)
    hashed = (mult_ids[:, None] * mult_ids[None, :] // HASH_SHIFT + add_ids[:, None] + add_ids[None, :]) % HASH_MOD
    edge_limit = jnp.where(comm_ids[:, None] == comm_ids[None, :], EDGE_IN, EDGE_OUT)
    node_ids = jnp.arange(NUM_NODES, dtype=jnp.int32)
    linked = (hashed < edge_limit) | (node_ids[:, None] == node_ids[None, :])
    degree = jnp.sum(linked.astype(jnp.int32), axis=1).astype(jnp.float32)
    inv_root = lax.rsqrt(degree)
    adjacency = jnp.where(linked, inv_root[:, None] * inv_root[None, :], 0.0).astype(jnp.bfloat16)
    return adjacency, jnp.sqrt(jnp.mean(degree))


def draw_mask(key_base):
    key_rate, key_pick = jax.random.split(key_base)
    chosen = jax.random.randint(key_rate, (NUM_NODES,), 0, LABEL_RATE, dtype=jnp.int32) == 0
    forced = jax.random.randint(key_pick, (), 0, NUM_NODES, dtype=jnp.int32)
    return (chosen | (jnp.arange(NUM_NODES, dtype=jnp.int32) == forced)).astype(jnp.int32)


def setup_inputs(seed: int = 0) -> dict:
    key_base = jax.random.key(seed)
    key_graph, key_feat, key_one, key_two, key_label, key_mask = jax.random.split(key_base, 6)
    adjacency, weight_gain = draw_graph(key_graph)
    features = jax.random.normal(key_feat, (NUM_NODES, F_IN), jnp.float32).astype(jnp.bfloat16)
    w_one = jax.random.normal(key_one, (F_IN, HIDDEN), jnp.float32) * (weight_gain * F_IN ** -0.5)
    raw_two = jax.random.normal(key_two, (HIDDEN, CLASSES), jnp.float32)
    w_two = (raw_two - jnp.mean(raw_two, axis=0, keepdims=True)) * (1.5 * weight_gain * HIDDEN ** -0.5)
    labels = jax.random.randint(key_label, (NUM_NODES,), 0, CLASSES, dtype=jnp.int32)
    label_mask = draw_mask(key_mask)
    return {'adjacency': adjacency, 'features': features, 'w_one': w_one, 'w_two': w_two, 'labels': labels, 'label_mask': label_mask}


def contract_rows(left, right):
    return lax.dot_general(left, right, (((0,), (0,)), ((), ())), preferred_element_type=jnp.float32)


def reference(adjacency, features, w_one, w_two, labels, label_mask):
    w_one_b = w_one.astype(jnp.bfloat16)
    w_two_b = w_two.astype(jnp.bfloat16)
    y_one = jnp.dot(features, w_one_b, preferred_element_type=jnp.float32).astype(jnp.bfloat16)
    z_one = jnp.dot(adjacency, y_one, preferred_element_type=jnp.float32)
    h_one = jnp.maximum(z_one, 0.0).astype(jnp.bfloat16)
    y_two = jnp.dot(h_one, w_two_b, preferred_element_type=jnp.float32).astype(jnp.bfloat16)
    z_two = jnp.dot(adjacency, y_two, preferred_element_type=jnp.float32)
    mask_f = label_mask.astype(jnp.float32)
    label_count = jnp.sum(mask_f)
    log_norm = jax.nn.logsumexp(z_two, axis=1)
    onehot = (labels[:, None] == jnp.arange(CLASSES, dtype=jnp.int32)[None, :]).astype(jnp.float32)
    picked = jnp.sum(z_two * onehot, axis=1)
    loss_value = jnp.sum(mask_f * (log_norm - picked)) / label_count
    soft_probs = jnp.exp(z_two - log_norm[:, None])
    g_two = ((soft_probs - onehot) * (mask_f / label_count)[:, None]).astype(jnp.bfloat16)
    grad_y2 = contract_rows(adjacency, g_two).astype(jnp.bfloat16)
    grad_two = contract_rows(h_one, grad_y2)
    grad_h1 = lax.dot_general(grad_y2, w_two_b, (((1,), (1,)), ((), ())), preferred_element_type=jnp.float32)
    grad_z1 = jnp.where(z_one > 0.0, grad_h1, 0.0).astype(jnp.bfloat16)
    grad_y1 = contract_rows(adjacency, grad_z1).astype(jnp.bfloat16)
    grad_one = contract_rows(features, grad_y1)
    return (loss_value, grad_one, grad_two)
```

```python
import functools

import jax
import jax.numpy as jnp
from jax import lax
from jax.experimental import pallas as pl
from jax.experimental.pallas import tpu as pltpu
from jax.sharding import PartitionSpec as P

F32 = jnp.float32
BF16 = jnp.bfloat16
MESH = pl.DeviceIdType.MESH
DEVICES = 16
UNITS = 4
LANES = 128


def dot(a, b):
    return jnp.dot(a, b, preferred_element_type=F32)


def dot_tn(a, b):
    return lax.dot_general(a, b, (((0,), (0,)), ((), ())), preferred_element_type=F32)


def dot_nt(a, b):
    return lax.dot_general(a, b, (((1,), (1,)), ((), ())), preferred_element_type=F32)


def step_kernel(classes, adj, x_ref, w1_ref, w2_ref, lab_ref, msk_ref,
                loss_out, g1_out, g2_out,
                a_v, gb, hb, acc1, acc2, ys, hown, e2own, labb, mskb, w1b, w2b,
                w2acc, w2rcv, w2f, w1p, w1r, w1f, cnt_src, cnt_rcv, loss_acc,
                a_sem, rsem, ssem, sib_rsem, sib_ssem, cs_sem, cr_sem,
                w2s_sem, w2r_sem, w1s_sem, w1r_sem, w1gs_sem, w1gr_sem):
    rows = x_ref.shape[0]
    fin = x_ref.shape[1]
    unit = rows // UNITS
    hid = w1_ref.shape[1]
    cpad = w2b.shape[1]
    me = lax.axis_index("nodes")
    core = me % 2
    sib = me + 1 - 2 * core
    bit = [(me // v) % 2 for v in (2, 4, 8)]
    step = [v * (1 - 2 * b) for v, b in zip((2, 4, 8), bit)]
    own_d = [(1 - core) * step[r] + core * step[(r + 1) % 3] for r in range(3)]
    sib_d = [core * step[r] + (1 - core) * step[(r + 1) % 3] for r in range(3)]
    role_bit = [(1 - core) * bit[r] + core * bit[(r + 1) % 3] for r in range(3)]
    nbr = [me + d for d in own_d]

    def src_dev(base, deltas, hop, r):
        if hop == 0:
            return base + deltas[r]
        if hop == 1:
            return base + deltas[r] + deltas[(r + 2) % 3]
        return base + deltas[0] + deltas[1] + deltas[2]

    def remote(src, dst, ss, rs, dev):
        return pltpu.make_async_remote_copy(src_ref=src, dst_ref=dst, send_sem=ss, recv_sem=rs,
                                            device_id=(dev,), device_id_type=MESH)

    order = [me, sib]
    for hop in (0, 1):
        order += [src_dev(me, own_d, hop, r) for r in range(3)]
        order += [src_dev(sib, sib_d, hop, r) for r in range(3)]
    order += [src_dev(me, own_d, 2, 0), src_dev(sib, sib_d, 2, 0)]

    def a_cols(dev):
        return pl.ds(pl.multiple_of(dev * rows, rows), rows)

    def a_copy(i):
        return pltpu.make_async_copy(adj.at[:, a_cols(order[i])], a_v.at[:, a_cols(order[i])], a_sem.at[i])

    for i in range(DEVICES):
        a_copy(i).start()

    barrier = pltpu.get_barrier_semaphore()
    for i in range(1, DEVICES):
        pl.semaphore_signal(barrier, inc=1, device_id=((me + i) % DEVICES,), device_id_type=MESH)
    pl.semaphore_wait(barrier, DEVICES - 1)

    def rows_of(dev, q):
        return pl.ds(pl.multiple_of(dev * rows + q * unit, unit), unit)

    def block_of(dev):
        return pl.ds(pl.multiple_of(dev * rows, rows), rows)

    class Gather:
        def __init__(self, buf, width, par):
            self.buf, self.width, self.par = buf, width, par

        def view(self, dev, q):
            return self.buf.at[rows_of(dev, q), pl.ds(0, self.width)]

        def hop_copy(self, dev, q, r, sslot, rslot):
            v = self.view(dev, q)
            return remote(v, v, ssem.at[self.par, sslot], rsem.at[self.par, rslot], nbr[r])

        def sib_copy(self, dev, q, slot):
            v = self.view(dev, q)
            return remote(v, v, sib_ssem.at[self.par, slot], sib_rsem.at[self.par, slot], sib)

        def own_copies(self, q):
            return [self.hop_copy(me, q, r, r * 4 + q, r * 4 + q) for r in range(3)] + [self.sib_copy(me, q, 28 + q)]

        def start_own(self, q):
            for c in self.own_copies(q):
                c.start()

        def arrive(self, hop, q):
            if hop == 2:
                d = src_dev(me, own_d, 2, 0)
                self.hop_copy(d, q, 0, 24 + q, 24 + q).wait_recv()
                self.sib_copy(d, q, 24 + q).start()
                return
            for r in range(3):
                d = src_dev(me, own_d, hop, r)
                self.hop_copy(d, q, r, r * 4 + q, hop * 12 + r * 4 + q).wait_recv()
                nxt = (r + 1) % 3
                if hop == 0:
                    self.hop_copy(d, q, nxt, 12 + r * 4 + q, 12 + nxt * 4 + q).start()
                elif q % 3 == nxt:
                    self.hop_copy(d, q, nxt, 24 + q, 24 + q).start()
                self.sib_copy(d, q, hop * 12 + r * 4 + q).start()

        def sib_wait(self, hop, q):
            if hop == 2:
                self.sib_copy(src_dev(sib, sib_d, 2, 0), q, 24 + q).wait_recv()
            elif hop < 0:
                self.sib_copy(sib, q, 28 + q).wait_recv()
            else:
                for r in range(3):
                    self.sib_copy(src_dev(sib, sib_d, hop, r), q, hop * 12 + r * 4 + q).wait_recv()

        def wait_sends(self):
            for q in range(UNITS):
                for c in self.own_copies(q):
                    c.wait_send()
                for hop in (0, 1):
                    for r in range(3):
                        d = src_dev(me, own_d, hop, r)
                        nxt = (r + 1) % 3
                        if hop == 0:
                            self.hop_copy(d, q, nxt, 12 + r * 4 + q, 12 + nxt * 4 + q).wait_send()
                        elif q % 3 == nxt:
                            self.hop_copy(d, q, nxt, 24 + q, 24 + q).wait_send()
                        self.sib_copy(d, q, hop * 12 + r * 4 + q).wait_send()
                self.sib_copy(src_dev(me, own_d, 2, 0), q, 24 + q).wait_send()

    def mrows(m):
        return pl.ds(pl.multiple_of(m * unit, unit), unit)

    def for_m(fn):
        lax.fori_loop(0, UNITS, lambda m, c: (fn(mrows(m)), c)[1], 0)

    def phase(g, acc, n, prep, finish, hook, first):
        g_ = g

        def a_wait(lo, hi):
            if first:
                for i in range(lo, hi):
                    a_copy(i).wait()

        def add_block(dev, init):
            rhs = prep([block_of(dev)], rows)
            cols = a_cols(dev)

            def body(s):
                v = dot(a_v[s, cols], rhs(0))
                acc[s, :n] = v if init else acc[s, :n] + v
            for_m(body)

        def add_units(devs, q):
            rhs = prep([rows_of(d, q) for d in devs], unit)

            def body(s):
                v = acc[s, :n]
                for j, d in enumerate(devs):
                    v = v + dot(a_v[s, rows_of(d, q)], rhs(j))
                acc[s, :n] = v
            for_m(body)

        a_wait(0, 1)
        add_block(me, True)
        hook(-1)
        for q in range(UNITS):
            g_.sib_wait(-1, q)
        a_wait(1, 2)
        add_block(sib, False)
        groups = [(hop, q) for hop in (0, 1) for q in range(UNITS)]
        for i, (hop, q) in enumerate(groups):
            g_.arrive(hop, q)
            hook(i)
            if q == 0:
                a_wait(2 + 6 * hop, 5 + 6 * hop)
            add_units([src_dev(me, own_d, hop, r) for r in range(3)], q)
            if i > 0:
                ph, pq = groups[i - 1]
                g_.sib_wait(ph, pq)
                if pq == 0:
                    a_wait(5 + 6 * ph, 8 + 6 * ph)
                add_units([src_dev(sib, sib_d, ph, r) for r in range(3)], pq)
        for q in range(UNITS):
            g_.arrive(2, q)
        a_wait(14, 15)
        ph, pq = groups[-1]
        g_.sib_wait(ph, pq)
        add_units([src_dev(sib, sib_d, ph, r) for r in range(3)], pq)
        add_block(src_dev(me, own_d, 2, 0), False)
        for q in range(UNITS):
            g_.sib_wait(2, q)
        a_wait(15, 16)
        last = src_dev(sib, sib_d, 2, 0)
        rhs = prep([block_of(last)], rows)
        for m in range(UNITS):
            if m == UNITS - 1:
                g_.wait_sends()
            s = pl.ds(m * unit, unit)
            finish(m, s, acc[s, :n] + dot(a_v[s, a_cols(last)], rhs(0)))

    gx = Gather(gb, fin, 0)
    gh = Gather(hb, hid, 1)
    gg = Gather(gb, cpad, 0)
    gd = Gather(hb, hid, 1)

    def own_rows(q):
        return rows_of(me, q)

    for q in range(UNITS):
        gb[own_rows(q), :fin] = x_ref[q * unit:(q + 1) * unit, :]
    w1b[...] = w1_ref[...].astype(BF16)
    w2b[...] = jnp.zeros_like(w2b)
    for q in range(UNITS):
        gx.start_own(q)
    w2b[:, :classes] = w2_ref[...].astype(BF16)

    for i in range(rows // LANES):
        s = pl.ds(i * LANES, LANES)
        labb[s, :] = jnp.broadcast_to(lab_ref[i:i + 1, :].astype(F32), (LANES, LANES)).T
        mskb[s, :] = jnp.broadcast_to(msk_ref[i:i + 1, :].astype(F32), (LANES, LANES)).T

    partners = [sib] + nbr

    def cnt_copy(i):
        return remote(cnt_src.at[i], cnt_rcv.at[i], cs_sem.at[i], cr_sem.at[i], partners[i])

    local = jnp.sum(msk_ref[...].astype(F32), axis=1, keepdims=True)
    local = jnp.sum(local, axis=0, keepdims=True)
    cnt_src[0] = jnp.broadcast_to(local, (8, LANES))

    def prep1(slices, size):
        for j, s in enumerate(slices):
            ys[j * size:(j + 1) * size, :hid] = dot(gb[s, :fin], w1b[...]).astype(BF16)
        return lambda j: ys[j * size:(j + 1) * size, :hid]

    def finish1(m, s, z):
        acc1[s, :] = z
        h = jnp.maximum(z, 0.0).astype(BF16)
        hb[own_rows(m), :] = h
        hown[s, :] = h
        gh.start_own(m)

    def hook1(i):
        if i == 0:
            cnt_copy(0).start()
        if 1 <= i <= 4:
            cnt_copy(i - 1).wait_recv()
            cnt_src[i] = cnt_src[i - 1] + cnt_rcv[i - 1]
            if i <= 3:
                cnt_copy(i).start()
        if i == 7:
            for j in range(4):
                cnt_copy(j).wait_send()

    phase(gx, acc1, hid, prep1, finish1, hook1, True)

    def prep2(slices, size):
        for j, s in enumerate(slices):
            ys[j * size:(j + 1) * size, :] = dot(hb[s, :], w2b[...]).astype(BF16)
        return lambda j: ys[j * size:(j + 1) * size, :]

    loss_acc[...] = jnp.zeros_like(loss_acc)
    count = cnt_src[4][0:1, 0:1]

    def finish2(m, s, z):
        acc2[s, :] = z
        sub = 32

        def body(i, c):
            r = pl.ds(pl.multiple_of(m * unit + i * sub, sub), sub)
            zc = acc2[r, :]
            col = lax.broadcasted_iota(jnp.int32, (sub, cpad), 1).astype(F32)
            live = col < float(classes)
            zm = jnp.where(live, zc, -jnp.inf)
            top = jnp.max(zm, axis=1, keepdims=True)
            tot = jnp.sum(jnp.exp(zm - top), axis=1, keepdims=True)
            log_norm = top + jnp.log(tot)
            lab = labb[r, 0:1]
            msk = mskb[r, 0:1]
            hot = jnp.where(col == lab, 1.0, 0.0)
            picked = jnp.sum(zc * hot, axis=1, keepdims=True)
            per = mskb[r, :] * (log_norm - picked)
            loss_acc[...] += jnp.sum(per.reshape(sub // 8, 8, LANES), axis=0)
            gr = (jnp.exp(zm - log_norm) - hot) * (msk / count)
            gb[pl.ds(pl.multiple_of(me * rows + m * unit + i * sub, sub), sub), :] = gr.astype(BF16)
            return c
        lax.fori_loop(0, unit // sub, body, 0)
        gg.start_own(m)

    phase(gh, acc2, cpad, prep2, finish2, lambda i: None, False)

    def prep3(slices, size):
        return lambda j: gb[slices[j], :]

    def finish3(m, s, z):
        e = z.astype(BF16)
        e2own[s, :] = e
        gz = dot_nt(e, w2b[...])
        hb[own_rows(m), :] = jnp.where(acc1[s, :] > 0.0, gz, 0.0).astype(BF16)
        gd.start_own(m)

    phase(gg, acc2, cpad, prep3, finish3, lambda i: None, False)

    size = [hid // 2, hid // 4, hid // 8, hid // 16]
    bits = [core] + role_bit
    base = [0]
    for i in range(4):
        base.append(base[i] + bits[i] * size[i])
    roff = [0, size[0], size[0] + size[1], size[0] + size[1] + size[2]]

    def w2rows(start, n):
        return pl.ds(pl.multiple_of(start, 16), n)

    def w2_scatter(i):
        out = w2acc.at[w2rows(base[i] + (1 - bits[i]) * size[i], size[i])]
        return remote(out, w2rcv.at[pl.ds(roff[i], size[i])], w2s_sem.at[i], w2r_sem.at[i], partners[i])

    def w2_gather(i):
        out = w2f.at[w2rows(base[i + 1], size[i])]
        return remote(out, out, w2s_sem.at[4 + i], w2r_sem.at[4 + i], partners[i])

    def w2_gather_in(i):
        out = w2f.at[w2rows(base[i] + (1 - bits[i]) * size[i], size[i])]
        return remote(out, out, w2s_sem.at[4 + i], w2r_sem.at[4 + i], partners[i])

    def hook4(i):
        if i == -1:
            w2acc[...] = dot_tn(hown[...], e2own[...])
            lane = lax.broadcasted_iota(jnp.int32, (1, LANES), 1)
            total = jnp.sum(loss_acc[...], axis=0, keepdims=True)
            w2acc[0:1, cpad - LANES:] = jnp.where(lane == LANES - 1, total, w2acc[0:1, cpad - LANES:])
        elif i == 0:
            w2_scatter(0).start()
        elif i <= 4:
            w2_scatter(i - 1).wait_recv()
            mine = w2rows(base[i], size[i - 1])
            into = w2acc if i < 4 else w2f
            into[mine, :] = w2acc[mine, :] + w2rcv[roff[i - 1]:roff[i - 1] + size[i - 1], :]
            w2_scatter(i - 1).wait_send()
            if i < 4:
                w2_scatter(i).start()
            else:
                w2_gather(3).start()
        elif i <= 7:
            j = 8 - i
            w2_gather_in(j).wait_recv()
            w2_gather(j).wait_send()
            w2_gather(j - 1).start()

    def finish4(m, s, z):
        part = dot_tn(x_ref[s, :], z.astype(BF16))
        w1p[...] = part if m == 0 else w1p[...] + part

    phase(gd, acc1, hid, lambda sl, n: (lambda j: hb[sl[j], :]), finish4, hook4, False)

    sl = fin // DEVICES

    def w1rows(dev):
        return pl.ds(pl.multiple_of(dev * sl, sl), sl)

    def w1_scatter(i):
        dev = (me + i) % DEVICES
        return remote(w1p.at[w1rows(dev)], w1r.at[i], w1s_sem.at[i], w1r_sem.at[i], dev)

    def w1_gather(i):
        dev = (me + i) % DEVICES
        return remote(w1f.at[w1rows(me)], w1f.at[w1rows(me)], w1gs_sem.at[i], w1gr_sem.at[i], dev)

    def w1_gather_in(i):
        dev = (me + DEVICES - i) % DEVICES
        return remote(w1f.at[w1rows(dev)], w1f.at[w1rows(dev)], w1gs_sem.at[i], w1gr_sem.at[i], dev)

    for i in range(1, DEVICES):
        w1_scatter(i).start()
    w2_gather_in(0).wait_recv()
    w2_gather(0).wait_send()
    g2_out[...] = w2f[:, :classes]
    loss_out[0, 0] = jnp.sum(w2f[0:1, cpad - 1:] / cnt_src[4][0:1, 0:1])
    total = w1p[w1rows(me), :]
    for i in range(1, DEVICES):
        w1_scatter(i).wait_recv()
    for i in range(1, DEVICES):
        total = total + w1r[i]
    w1f[w1rows(me), :] = total
    for i in range(1, DEVICES):
        w1_scatter(i).wait_send()
    for i in range(1, DEVICES):
        w1_gather(i).start()
    for i in range(1, DEVICES):
        w1_gather_in(i).wait_recv()
    g1_out[...] = w1f[...]
    for i in range(1, DEVICES):
        w1_gather(i).wait_send()


def solution(mesh):
    axis = mesh.axis_names[0]

    def local_step(adj, x, w1, w2, labels, mask):
        rows, nodes = adj.shape
        fin, hid = w1.shape
        classes = w2.shape[1]
        cpad = -(-classes // LANES) * LANES
        if cpad == classes:
            cpad += LANES
        dma = pltpu.SemaphoreType.DMA
        vm = pl.BlockSpec(memory_space=pltpu.VMEM)
        loss, g1, g2 = pl.pallas_call(
            functools.partial(step_kernel, classes),
            out_shape=(jax.ShapeDtypeStruct((1, 1), F32),
                       jax.ShapeDtypeStruct((fin, hid), F32),
                       jax.ShapeDtypeStruct((hid, classes), F32)),
            in_specs=[pl.BlockSpec(memory_space=pl.ANY)] + [vm] * 5,
            out_specs=(pl.BlockSpec(memory_space=pltpu.SMEM), vm, vm),
            scratch_shapes=[
                pltpu.VMEM((rows, nodes), BF16),
                pltpu.VMEM((nodes, cpad), BF16),
                pltpu.VMEM((nodes, hid), BF16),
                pltpu.VMEM((rows, hid), F32),
                pltpu.VMEM((rows, cpad), F32),
                pltpu.VMEM((rows, cpad), BF16),
                pltpu.VMEM((rows, hid), BF16),
                pltpu.VMEM((rows, cpad), BF16),
                pltpu.VMEM((rows, LANES), F32),
                pltpu.VMEM((rows, LANES), F32),
                pltpu.VMEM((fin, hid), BF16),
                pltpu.VMEM((hid, cpad), BF16),
                pltpu.VMEM((hid, cpad), F32),
                pltpu.VMEM((hid, cpad), F32),
                pltpu.VMEM((hid, cpad), F32),
                pltpu.VMEM((fin, hid), F32),
                pltpu.VMEM((DEVICES, fin // DEVICES, hid), F32),
                pltpu.VMEM((fin, hid), F32),
                pltpu.VMEM((5, 8, LANES), F32),
                pltpu.VMEM((4, 8, LANES), F32),
                pltpu.VMEM((8, LANES), F32),
                dma((DEVICES,)),
                dma((2, 28)), dma((2, 28)), dma((2, 32)), dma((2, 32)),
                dma((4,)), dma((4,)), dma((8,)), dma((8,)),
                dma((DEVICES,)), dma((DEVICES,)), dma((DEVICES,)), dma((DEVICES,)),
            ],
            compiler_params=pltpu.CompilerParams(collective_id=0, has_side_effects=True,
                                                 vmem_limit_bytes=67043328),
            name="gcn_step",
        )(adj, x, w1, w2, labels.reshape(rows // LANES, LANES), mask.reshape(rows // LANES, LANES))
        return loss[0, 0], g1, g2

    return jax.shard_map(local_step, mesh=mesh,
                         in_specs=(P(axis, None), P(axis, None), P(None, None), P(None, None), P(axis), P(axis)),
                         out_specs=(P(), P(None, None), P(None, None)), check_vma=False)
```

```python
import functools

import jax
import jax.numpy as jnp
from jax import lax
from jax.experimental import pallas as pl
from jax.experimental.pallas import tpu as pltpu
from jax.sharding import PartitionSpec as P

F32 = jnp.float32
BF16 = jnp.bfloat16
MESH = pl.DeviceIdType.MESH
DEVICES = 16
UNITS = 4
LANES = 128
CHUNK = 512


def dot(a, b):
    return jnp.dot(a, b, preferred_element_type=F32)


def dot_tn(a, b):
    return lax.dot_general(a, b, (((0,), (0,)), ((), ())), preferred_element_type=F32)


def dot_nt(a, b):
    return lax.dot_general(a, b, (((1,), (1,)), ((), ())), preferred_element_type=F32)


def loop(n, fn):
    lax.fori_loop(0, n, lambda i, c: (fn(i), c)[1], 0)


def step_kernel(classes, adj, x_ref, w1_ref, w2_ref, lab_ref, msk_ref,
                loss_out, g1_out, g2_out,
                a_v, gb, hb, acc1, acc2, ys1, ys2, hown, e2own, w1b, w2b,
                w2acc, w2rcv, w2f, w1p, w1r, w1f, cnt_src, cnt_rcv, loss_acc,
                a_sem, rsem, ssem, sib_rsem, sib_ssem, cs_sem, cr_sem,
                w2s_sem, w2r_sem, w1s_sem, w1r_sem, w1gs_sem, w1gr_sem):
    rows = x_ref.shape[0]
    fin = x_ref.shape[1]
    unit = rows // UNITS
    hid = w1_ref.shape[1]
    cpad = w2b.shape[0]
    me = lax.axis_index("nodes")
    core = me % 2
    sib = me + 1 - 2 * core
    bit = [(me // v) % 2 for v in (2, 4, 8)]
    step = [v * (1 - 2 * b) for v, b in zip((2, 4, 8), bit)]
    own_d = [(1 - core) * step[r] + core * step[(r + 1) % 3] for r in range(3)]
    sib_d = [core * step[r] + (1 - core) * step[(r + 1) % 3] for r in range(3)]
    role_bit = [(1 - core) * bit[r] + core * bit[(r + 1) % 3] for r in range(3)]
    nbr = [me + d for d in own_d]

    def src_dev(base, deltas, hop, r):
        return base + deltas[r] + hop * deltas[(r + 2) % 3]

    anti = me + own_d[0] + own_d[1] + own_d[2]
    anti_sib = anti + 1 - 2 * core

    def remote(src, dst, ss, rs, dev):
        return pltpu.make_async_remote_copy(src_ref=src, dst_ref=dst, send_sem=ss, recv_sem=rs,
                                            device_id=(dev,), device_id_type=MESH)

    order = [me, sib]
    for hop in (0, 1):
        order += [src_dev(me, own_d, hop, r) for r in range(3)]
        order += [src_dev(sib, sib_d, hop, r) for r in range(3)]
    order += [anti, anti_sib]

    def a_cols(dev):
        return pl.ds(pl.multiple_of(dev * rows, rows), rows)

    def a_copy(i):
        return pltpu.make_async_copy(adj.at[:, a_cols(order[i])], a_v.at[:, a_cols(order[i])], a_sem.at[i])

    for i in range(DEVICES):
        a_copy(i).start()

    def rows_of(dev, q):
        return pl.ds(pl.multiple_of(dev * rows + q * unit, unit), unit)

    def uid(dev, q):
        return dev * UNITS + q

    for q in range(UNITS):
        gb[uid(me, q), :unit, :fin] = x_ref[q * unit:(q + 1) * unit, :]

    barrier = pltpu.get_barrier_semaphore()
    for i in range(1, DEVICES):
        pl.semaphore_signal(barrier, inc=1, device_id=((me + i) % DEVICES,), device_id_type=MESH)
    pl.semaphore_wait(barrier, DEVICES - 1)

    def pick(f, vals):
        return jnp.where(f == 0, vals[0], jnp.where(f == 1, vals[1], vals[2]))

    class Gather:
        def __init__(self, view, par):
            self.view, self.par = view, par

        def hop_copy(self, dev, q, to, sslot, rslot):
            v = self.view(dev, q)
            return remote(v, v, ssem.at[self.par, sslot], rsem.at[self.par, rslot], to)

        def sib_copy(self, dev, q, slot):
            v = self.view(dev, q)
            return remote(v, v, sib_ssem.at[self.par, slot], sib_rsem.at[self.par, slot], sib)

        def own_copies(self, q):
            return [self.hop_copy(me, q, nbr[r], r * 4 + q, r * 4 + q) for r in range(3)] + [self.sib_copy(me, q, 28 + q)]

        def start_own(self, q):
            for c in self.own_copies(q):
                c.start()

        def forward(self, q):
            return [self.hop_copy(src_dev(me, own_d, 0, r), q, nbr[(r + 1) % 3], 12 + r * 4 + q,
                                  12 + ((r + 1) % 3) * 4 + q) for r in range(3)]

        def last_forward(self, q):
            to = q % 3
            dev = pick((to + 2) % 3, [src_dev(me, own_d, 1, r) for r in range(3)])
            return self.hop_copy(dev, q, pick(to, nbr), 24 + q, 24 + q)

        def arrive(self, hop, q):
            for r in range(3):
                d = src_dev(me, own_d, hop, r)
                self.hop_copy(d, q, nbr[r], r * 4 + q, hop * 12 + r * 4 + q).wait_recv()

            @pl.when(hop == 0)
            def _():
                for c in self.forward(q):
                    c.start()

            @pl.when(hop == 1)
            def _():
                self.last_forward(q).start()
            for r in range(3):
                self.sib_copy(src_dev(me, own_d, hop, r), q, hop * 12 + r * 4 + q).start()

        def arrive_last(self, q):
            self.hop_copy(anti, q, nbr[0], 24 + q, 24 + q).wait_recv()
            self.sib_copy(anti, q, 24 + q).start()

        def sib_wait(self, hop, q):
            for r in range(3):
                self.sib_copy(src_dev(sib, sib_d, hop, r), q, hop * 12 + r * 4 + q).wait_recv()

        def sib_wait_own(self, q):
            self.sib_copy(sib, q, 28 + q).wait_recv()

        def sib_wait_last(self, q):
            self.sib_copy(anti_sib, q, 24 + q).wait_recv()

        def wait_sends(self):
            def body(q):
                for c in self.own_copies(q) + self.forward(q) + [self.last_forward(q)]:
                    c.wait_send()
                for slot in (q, 4 + q, 8 + q, 12 + q, 16 + q, 20 + q, 24 + q):
                    self.sib_copy(me, q, slot).wait_send()
            loop(UNITS, body)

    def phase(g, add, zero, finish, hook, first):
        def a_wait(lo, hi):
            if first:
                for i in range(lo, hi):
                    a_copy(i).wait()

        zero()

        def near(t):
            if first:
                @pl.when(t == 0)
                def _():
                    a_wait(0, 1)

            @pl.when(t == 1)
            def _():
                for q in range(UNITS):
                    g.sib_wait_own(q)
                a_wait(1, 2)
            dev = me + t * (sib - me)
            add([(dev, q) for q in range(UNITS)])
        loop(2, near)
        hook(-1, None)

        def group(i):
            hop, q, far = (i // 4) % 2, i % 4, i // 8

            @pl.when(far == 0)
            def _():
                g.arrive(hop, q)

            @pl.when(far == 1)
            def _():
                for j in range(3):
                    g.arrive_last(j)
            hook(None, i)

            def half(t):
                @pl.when(t == 1)
                def _():
                    @pl.when(far == 0)
                    def _():
                        g.sib_wait(hop, q)

                    @pl.when(far == 1)
                    def _():
                        for j in range(3):
                            g.sib_wait_last(j)
                if first:
                    for k, (lo, hi) in {(0, 0): (2, 5), (0, 1): (5, 8), (4, 0): (8, 11), (4, 1): (11, 14),
                                        (8, 0): (14, 15), (8, 1): (15, 16)}.items():
                        @pl.when((i == k[0]) & (t == k[1]))
                        def _(lo=lo, hi=hi):
                            a_wait(lo, hi)
                pairs = []
                for r in range(3):
                    o, s = src_dev(me, own_d, hop, r), src_dev(sib, sib_d, hop, r)
                    near_dev = o + t * (s - o)
                    far_dev = anti + t * (anti_sib - anti)
                    pairs.append((near_dev + far * (far_dev - near_dev), q + far * (r - q)))
                add(pairs)
            loop(2, half)
        loop(9, group)
        g.arrive_last(3)
        g.sib_wait_last(3)

        def last(m):
            @pl.when(m == UNITS - 1)
            def _():
                g.wait_sends()
            finish(m, [(anti, 3), (anti_sib, 3)])
        loop(UNITS, last)

    gx = Gather(lambda dev, q: gb.at[uid(dev, q), pl.ds(0, unit), pl.ds(0, fin)], 0)
    gh = Gather(lambda dev, q: hb.at[rows_of(dev, q)], 1)
    gg = Gather(lambda dev, q: gb.at[uid(dev, q)], 0)

    def mrows(m):
        return pl.ds(pl.multiple_of(m * unit, unit), unit)

    def chunk(c):
        return pl.ds(pl.multiple_of(c * CHUNK, CHUNK), CHUNK)

    for q in range(UNITS):
        gx.start_own(q)
    w1b[...] = w1_ref[...].astype(BF16)
    w2acc[...] = jnp.zeros_like(w2acc)
    w2acc[:classes, :] = w2_ref[...]
    w2b[...] = w2acc[:cpad, :].astype(BF16)

    partners = [sib] + nbr

    def cnt_copy(i):
        return remote(cnt_src.at[i], cnt_rcv.at[i], cs_sem.at[i], cr_sem.at[i], partners[i])

    local = jnp.sum(msk_ref[...].astype(F32), axis=1, keepdims=True)
    local = jnp.sum(local, axis=0, keepdims=True)
    cnt_src[0] = jnp.broadcast_to(local, (8, LANES))

    def hook1(pre, i):
        if i is None:
            cnt_copy(0).start()
            return
        for k in range(4):
            @pl.when(i == k + 1)
            def _(k=k):
                cnt_copy(k).wait_recv()
                cnt_src[k + 1] = cnt_src[k] + cnt_rcv[k]
                if k < 3:
                    cnt_copy(k + 1).start()

        @pl.when(i == 7)
        def _():
            for k in range(4):
                cnt_copy(k).wait_send()

    def zero1():
        acc1[...] = jnp.zeros_like(acc1)

    def y1(dev, q):
        return dot(gb[uid(dev, q), :unit, :fin], w1b[...]).astype(BF16)

    def add_rows(acc, pairs, operand):
        def body(c):
            s = chunk(c)
            v = acc[s, :]
            for j, (dev, q) in enumerate(pairs):
                v = v + dot(a_v[s, rows_of(dev, q)], operand(j))
            acc[s, :] = v
        loop(rows // CHUNK, body)

    def add1(pairs):
        for j, (dev, q) in enumerate(pairs):
            ys1[j] = y1(dev, q)
        add_rows(acc1, pairs, lambda j: ys1[j])

    def finish1(m, pairs):
        s = mrows(m)

        @pl.when(m == 0)
        def _():
            for j, (dev, q) in enumerate(pairs):
                ys1[j] = y1(dev, q)
        z = acc1[s, :]
        for j, (dev, q) in enumerate(pairs):
            z = z + dot(a_v[s, rows_of(dev, q)], ys1[j])
        acc1[s, :] = z
        h = jnp.maximum(z, 0.0).astype(BF16)
        hb[rows_of(me, m), :] = h
        hown[s, :] = h
        gh.start_own(m)

    phase(gx, add1, zero1, finish1, hook1, True)

    def zero2():
        acc2[...] = jnp.zeros_like(acc2)

    def y2(dev, q):
        return dot_nt(w2b[...], hb[rows_of(dev, q), :]).astype(BF16)

    def add_cols(acc, pairs, operand):
        def body(c):
            s = chunk(c)
            v = acc[:, s]
            for j, (dev, q) in enumerate(pairs):
                v = v + dot_nt(operand(j), a_v[s, rows_of(dev, q)])
            acc[:, s] = v
        loop(rows // CHUNK, body)

    def add2(pairs):
        for j, (dev, q) in enumerate(pairs):
            ys2[j] = y2(dev, q)
        add_cols(acc2, pairs, lambda j: ys2[j])

    loss_acc[...] = jnp.zeros_like(loss_acc)
    count = cnt_src[4][0:1, :]

    def finish2(m, pairs):
        s = mrows(m)

        @pl.when(m == 0)
        def _():
            for j, (dev, q) in enumerate(pairs):
                ys2[j] = y2(dev, q)
        z = acc2[:, s]
        for j, (dev, q) in enumerate(pairs):
            z = z + dot_nt(ys2[j], a_v[s, rows_of(dev, q)])
        acc2[:, s] = z
        for h in range(unit // LANES):
            at = pl.ds(pl.multiple_of(m * unit + h * LANES, LANES), LANES)
            zc = acc2[:, at]
            row = lax.broadcasted_iota(jnp.int32, (cpad, LANES), 0)
            zm = jnp.where(row < classes, zc, -jnp.inf)
            top = jnp.max(zm, axis=0, keepdims=True)
            log_norm = top + jnp.log(jnp.sum(jnp.exp(zm - top), axis=0, keepdims=True))
            which = m * (unit // LANES) + h
            hot = row == lab_ref[pl.ds(which, 1), :]
            mask = msk_ref[pl.ds(which, 1), :].astype(F32)
            picked = jnp.sum(jnp.where(hot, zc, 0.0), axis=0, keepdims=True)
            loss_acc[...] = loss_acc[...] + mask * (log_norm - picked)
            gr = (jnp.exp(zm - log_norm) - jnp.where(hot, 1.0, 0.0)) * (mask / count)
            gb[uid(me, m), :, h * LANES:(h + 1) * LANES] = gr.astype(BF16)
        gg.start_own(m)

    phase(gh, add2, zero2, finish2, lambda pre, i: None, False)

    def finish3(m, pairs):
        s = mrows(m)
        z = acc2[:, s]
        for dev, q in pairs:
            z = z + dot_nt(gb[uid(dev, q)], a_v[s, rows_of(dev, q)])
        e = z.astype(BF16)
        e2own[:, s] = e
        gz = dot_tn(e, w2b[...])
        hb[rows_of(me, m), :] = jnp.where(acc1[s, :] > 0.0, gz, 0.0).astype(BF16)
        gh.start_own(m)

    phase(gg, lambda pairs: add_cols(acc2, pairs, lambda j: gb[uid(*pairs[j])]), zero2, finish3,
          lambda pre, i: None, False)

    total_rows = w2acc.shape[0]
    size = [total_rows // 2, total_rows // 4, total_rows // 8, total_rows // 16]
    bits = [core] + role_bit
    base = [0]
    for i in range(4):
        base.append(base[i] + bits[i] * size[i])
    roff = [0, size[0], size[0] + size[1], size[0] + size[1] + size[2]]

    def w2rows(start, n):
        return pl.ds(pl.multiple_of(start, 8), n)

    def w2_scatter(i):
        out = w2acc.at[w2rows(base[i] + (1 - bits[i]) * size[i], size[i])]
        return remote(out, w2rcv.at[pl.ds(roff[i], size[i])], w2s_sem.at[i], w2r_sem.at[i], partners[i])

    def w2_gather(i):
        out = w2f.at[w2rows(base[i + 1], size[i])]
        return remote(out, out, w2s_sem.at[4 + i], w2r_sem.at[4 + i], partners[i])

    def w2_gather_in(i):
        out = w2f.at[w2rows(base[i] + (1 - bits[i]) * size[i], size[i])]
        return remote(out, out, w2s_sem.at[4 + i], w2r_sem.at[4 + i], partners[i])

    def hook4(pre, i):
        if i is None:
            w2acc[...] = jnp.zeros_like(w2acc)
            w2acc[:cpad, :] = dot(e2own[...], hown[...])
            w2acc[total_rows - 1:, :LANES] = loss_acc[...]
            return

        @pl.when(i == 0)
        def _():
            w2_scatter(0).start()
        for k in range(4):
            @pl.when(i == k + 1)
            def _(k=k):
                w2_scatter(k).wait_recv()
                mine = w2rows(base[k + 1], size[k])
                into = w2acc if k < 3 else w2f
                into[mine, :] = w2acc[mine, :] + w2rcv[roff[k]:roff[k] + size[k], :]
                w2_scatter(k).wait_send()
                (w2_scatter(k + 1) if k < 3 else w2_gather(3)).start()
        for k in range(3):
            @pl.when(i == k + 5)
            def _(j=3 - k):
                w2_gather_in(j).wait_recv()
                w2_gather(j).wait_send()
                w2_gather(j - 1).start()

    def finish4(m, pairs):
        s = mrows(m)
        z = acc1[s, :]
        for dev, q in pairs:
            z = z + dot(a_v[s, rows_of(dev, q)], hb[rows_of(dev, q), :])
        part = dot_tn(x_ref[s, :], z.astype(BF16))
        w1p[...] = w1p[...] + part

    w1p[...] = jnp.zeros_like(w1p)
    phase(gh, lambda pairs: add_rows(acc1, pairs, lambda j: hb[rows_of(*pairs[j]), :]), zero1, finish4, hook4, False)

    sl = fin // DEVICES

    def w1rows(dev):
        return pl.ds(pl.multiple_of(dev * sl, sl), sl)

    def w1_scatter(i):
        dev = (me + i) % DEVICES
        return remote(w1p.at[w1rows(dev)], w1r.at[i], w1s_sem.at[i], w1r_sem.at[i], dev)

    def w1_gather(i):
        dev = (me + i) % DEVICES
        return remote(w1f.at[w1rows(me)], w1f.at[w1rows(me)], w1gs_sem.at[i], w1gr_sem.at[i], dev)

    def w1_gather_in(i):
        dev = (me + DEVICES - i) % DEVICES
        return remote(w1f.at[w1rows(dev)], w1f.at[w1rows(dev)], w1gs_sem.at[i], w1gr_sem.at[i], dev)

    for i in range(1, DEVICES):
        w1_scatter(i).start()
    w2_gather_in(0).wait_recv()
    w2_gather(0).wait_send()
    g2_out[...] = w2f[:classes, :]
    loss_out[0, 0] = jnp.sum(w2f[total_rows - 1:, :LANES] / cnt_src[4][0:1, :])
    total = w1p[w1rows(me), :]
    for i in range(1, DEVICES):
        w1_scatter(i).wait_recv()
    for i in range(1, DEVICES):
        total = total + w1r[i]
    w1f[w1rows(me), :] = total
    for i in range(1, DEVICES):
        w1_scatter(i).wait_send()
    for i in range(1, DEVICES):
        w1_gather(i).start()
    for i in range(1, DEVICES):
        w1_gather_in(i).wait_recv()
    g1_out[...] = w1f[...]
    for i in range(1, DEVICES):
        w1_gather(i).wait_send()


def solution(mesh):
    axis = mesh.axis_names[0]

    def local_step(adj, x, w1, w2, labels, mask):
        rows, nodes = adj.shape
        fin, hid = w1.shape
        classes = w2.shape[1]
        unit = rows // UNITS
        cpad = -(-classes // 16) * 16
        total_rows = -(-(cpad + 1) // LANES) * LANES
        dma = pltpu.SemaphoreType.DMA
        vm = pl.BlockSpec(memory_space=pltpu.VMEM)
        loss, g1, g2 = pl.pallas_call(
            functools.partial(step_kernel, classes),
            out_shape=(jax.ShapeDtypeStruct((1, 1), F32),
                       jax.ShapeDtypeStruct((fin, hid), F32),
                       jax.ShapeDtypeStruct((classes, hid), F32)),
            in_specs=[pl.BlockSpec(memory_space=pl.ANY)] + [vm] * 5,
            out_specs=(pl.BlockSpec(memory_space=pltpu.SMEM), vm, vm),
            scratch_shapes=[
                pltpu.VMEM((rows, nodes), BF16),
                pltpu.VMEM((nodes // unit, cpad, unit), BF16),
                pltpu.VMEM((nodes, hid), BF16),
                pltpu.VMEM((rows, hid), F32),
                pltpu.VMEM((cpad, rows), F32),
                pltpu.VMEM((UNITS, unit, hid), BF16),
                pltpu.VMEM((UNITS, cpad, unit), BF16),
                pltpu.VMEM((rows, hid), BF16),
                pltpu.VMEM((cpad, rows), BF16),
                pltpu.VMEM((fin, hid), BF16),
                pltpu.VMEM((cpad, hid), BF16),
                pltpu.VMEM((total_rows, hid), F32),
                pltpu.VMEM((total_rows, hid), F32),
                pltpu.VMEM((total_rows, hid), F32),
                pltpu.VMEM((fin, hid), F32),
                pltpu.VMEM((DEVICES, fin // DEVICES, hid), F32),
                pltpu.VMEM((fin, hid), F32),
                pltpu.VMEM((5, 8, LANES), F32),
                pltpu.VMEM((4, 8, LANES), F32),
                pltpu.VMEM((1, LANES), F32),
                dma((DEVICES,)),
                dma((2, 28)), dma((2, 28)), dma((2, 32)), dma((2, 32)),
                dma((4,)), dma((4,)), dma((8,)), dma((8,)),
                dma((DEVICES,)), dma((DEVICES,)), dma((DEVICES,)), dma((DEVICES,)),
            ],
            compiler_params=pltpu.CompilerParams(collective_id=0, has_side_effects=True,
                                                 vmem_limit_bytes=67043328),
            name="gcn_step",
        )(adj, x, w1, w2.T, labels.reshape(rows // LANES, LANES), mask.reshape(rows // LANES, LANES))
        return loss[0, 0], g1, g2.T

    return jax.shard_map(local_step, mesh=mesh,
                         in_specs=(P(axis, None), P(axis, None), P(None, None), P(None, None), P(axis), P(axis)),
                         out_specs=(P(), P(None, None), P(None, None)), check_vma=False)
```

```python
import functools

import jax
import jax.numpy as jnp
from jax import lax
from jax.experimental import pallas as pl
from jax.experimental.pallas import tpu as pltpu
from jax.sharding import PartitionSpec as P

F32 = jnp.float32
BF16 = jnp.bfloat16
MESH = pl.DeviceIdType.MESH
DEVICES = 16
UNITS = 4
LANES = 128
CHUNK = 1024


def dot(a, b):
    return jnp.dot(a, b, preferred_element_type=F32)


def dot_tn(a, b):
    return lax.dot_general(a, b, (((0,), (0,)), ((), ())), preferred_element_type=F32)


def dot_nt(a, b):
    return lax.dot_general(a, b, (((1,), (1,)), ((), ())), preferred_element_type=F32)


def loop(n, fn):
    lax.fori_loop(0, n, lambda i, c: (fn(i), c)[1], 0)


def step_kernel(classes, adj, x_ref, w1_ref, w2_ref, lab_ref, msk_ref,
                loss_out, g1_out, g2_out,
                a_v, gb, hb, acc1, acc2, ys1, ys2, hown, e2own, w1b, w2b,
                w2acc, w2rcv, w2f, w1p, w1r, w1f, cnt_src, cnt_rcv, loss_acc,
                a_sem, rsem, ssem, sib_rsem, sib_ssem, cs_sem, cr_sem,
                w2s_sem, w2r_sem, w1s_sem, w1r_sem, w1gs_sem, w1gr_sem):
    rows = x_ref.shape[0]
    fin = x_ref.shape[1]
    unit = rows // UNITS
    hid = w1_ref.shape[1]
    cpad = w2b.shape[0]
    me = lax.axis_index("nodes")
    core = me % 2
    sib = me + 1 - 2 * core
    bit = [(me // v) % 2 for v in (2, 4, 8)]
    step = [v * (1 - 2 * b) for v, b in zip((2, 4, 8), bit)]
    own_d = [(1 - core) * step[r] + core * step[(r + 1) % 3] for r in range(3)]
    sib_d = [core * step[r] + (1 - core) * step[(r + 1) % 3] for r in range(3)]
    role_bit = [(1 - core) * bit[r] + core * bit[(r + 1) % 3] for r in range(3)]
    nbr = [me + d for d in own_d]

    def src_dev(base, deltas, hop, r):
        return base + deltas[r] + hop * deltas[(r + 2) % 3]

    anti = me + own_d[0] + own_d[1] + own_d[2]
    anti_sib = anti + 1 - 2 * core

    def remote(src, dst, ss, rs, dev):
        return pltpu.make_async_remote_copy(src_ref=src, dst_ref=dst, send_sem=ss, recv_sem=rs,
                                            device_id=(dev,), device_id_type=MESH)

    order = [me, sib]
    for hop in (0, 1):
        order += [src_dev(me, own_d, hop, r) for r in range(3)]
        order += [src_dev(sib, sib_d, hop, r) for r in range(3)]
    order += [anti, anti_sib]

    def a_cols(dev):
        return pl.ds(pl.multiple_of(dev * rows, rows), rows)

    def a_copy(i):
        return pltpu.make_async_copy(adj.at[:, a_cols(order[i])], a_v.at[:, a_cols(order[i])], a_sem.at[i])

    for i in range(2):
        a_copy(i).start()

    def rows_of(dev, q):
        return pl.ds(pl.multiple_of(dev * rows + q * unit, unit), unit)

    def uid(dev, q):
        return dev * UNITS + q

    for q in range(UNITS):
        gb[uid(me, q), :unit, :fin] = x_ref[q * unit:(q + 1) * unit, :]

    barrier = pltpu.get_barrier_semaphore()
    for dev in [sib] + nbr:
        pl.semaphore_signal(barrier, inc=1, device_id=(dev,), device_id_type=MESH)
    pl.semaphore_wait(barrier, 4)

    def pick(f, vals):
        return jnp.where(f == 0, vals[0], jnp.where(f == 1, vals[1], vals[2]))

    class Gather:
        def __init__(self, view, par):
            self.view, self.par = view, par

        def hop_copy(self, dev, q, to, sslot, rslot):
            v = self.view(dev, q)
            return remote(v, v, ssem.at[self.par, sslot], rsem.at[self.par, rslot], to)

        def sib_copy(self, dev, q, slot):
            v = self.view(dev, q)
            return remote(v, v, sib_ssem.at[self.par, slot], sib_rsem.at[self.par, slot], sib)

        def own_copies(self, q):
            return [self.hop_copy(me, q, nbr[r], r * 4 + q, r * 4 + q) for r in range(3)] + [self.sib_copy(me, q, 28 + q)]

        def start_own(self, q):
            for c in self.own_copies(q):
                c.start()

        def forward(self, q):
            return [self.hop_copy(src_dev(me, own_d, 0, r), q, nbr[(r + 1) % 3], 12 + r * 4 + q,
                                  12 + ((r + 1) % 3) * 4 + q) for r in range(3)]

        def last_forward(self, q):
            to = q % 3
            dev = pick((to + 2) % 3, [src_dev(me, own_d, 1, r) for r in range(3)])
            return self.hop_copy(dev, q, pick(to, nbr), 24 + q, 24 + q)

        def arrive(self, hop, q):
            for r in range(3):
                d = src_dev(me, own_d, hop, r)
                self.hop_copy(d, q, nbr[r], r * 4 + q, hop * 12 + r * 4 + q).wait_recv()

            @pl.when(hop == 0)
            def _():
                for c in self.forward(q):
                    c.start()

            @pl.when(hop == 1)
            def _():
                self.last_forward(q).start()
            for r in range(3):
                self.sib_copy(src_dev(me, own_d, hop, r), q, hop * 12 + r * 4 + q).start()

        def arrive_last(self, q):
            self.hop_copy(anti, q, nbr[0], 24 + q, 24 + q).wait_recv()
            self.sib_copy(anti, q, 24 + q).start()

        def sib_wait(self, hop, q):
            for r in range(3):
                self.sib_copy(src_dev(sib, sib_d, hop, r), q, hop * 12 + r * 4 + q).wait_recv()

        def sib_wait_own(self, q):
            self.sib_copy(sib, q, 28 + q).wait_recv()

        def sib_wait_last(self, q):
            self.sib_copy(anti_sib, q, 24 + q).wait_recv()

        def wait_sends(self):
            def body(q):
                for c in self.own_copies(q) + self.forward(q) + [self.last_forward(q)]:
                    c.wait_send()
                for slot in (q, 4 + q, 8 + q, 12 + q, 16 + q, 20 + q, 24 + q):
                    self.sib_copy(me, q, slot).wait_send()
            loop(UNITS, body)

    def phase(g, add, zero, finish, hook, first):
        def a_wait(lo, hi):
            if first:
                for i in range(lo, hi):
                    a_copy(i).wait()

        zero()

        def near(t):
            if first:
                @pl.when(t == 0)
                def _():
                    a_wait(0, 1)

            @pl.when(t == 1)
            def _():
                for q in range(UNITS):
                    g.sib_wait_own(q)
                a_wait(1, 2)
            dev = me + t * (sib - me)
            add([(dev, q) for q in range(UNITS)])
        loop(2, near)
        hook(-1, None)

        def group(i):
            @pl.when(i < 8)
            def _():
                g.arrive(i // 4, i % 4)

            @pl.when(i == 8)
            def _():
                for j in range(3):
                    g.arrive_last(j)

            @pl.when(i == 9)
            def _():
                g.arrive_last(3)
            hook(None, i)

            def half(t):
                k = i - t
                hop, q, far = (k // 4) % 2, k % 4, k // 8

                @pl.when((k >= 0) & (k <= 8))
                def _():
                    @pl.when((t == 1) & (k < 8))
                    def _():
                        g.sib_wait(hop, q)

                    @pl.when((t == 1) & (k == 8))
                    def _():
                        for j in range(3):
                            g.sib_wait_last(j)
                    if first:
                        for key, (lo, hi) in {(0, 0): (2, 5), (0, 1): (5, 8), (4, 0): (8, 11), (4, 1): (11, 14),
                                              (8, 0): (14, 15), (8, 1): (15, 16)}.items():
                            @pl.when((k == key[0]) & (t == key[1]))
                            def _(lo=lo, hi=hi):
                                a_wait(lo, hi)
                    pairs = []
                    for r in range(3):
                        o, s = src_dev(me, own_d, hop, r), src_dev(sib, sib_d, hop, r)
                        near_dev = o + t * (s - o)
                        far_dev = anti + t * (anti_sib - anti)
                        pairs.append((near_dev + far * (far_dev - near_dev), q + far * (r - q)))
                    add(pairs)
            loop(2, half)
        loop(10, group)
        g.sib_wait_last(3)

        def last(m):
            @pl.when(m == UNITS - 1)
            def _():
                g.wait_sends()
            finish(m, [(anti, 3), (anti_sib, 3)])
        loop(UNITS, last)

    gx = Gather(lambda dev, q: gb.at[uid(dev, q), pl.ds(0, unit), pl.ds(0, fin)], 0)
    gh = Gather(lambda dev, q: hb.at[rows_of(dev, q)], 1)
    gg = Gather(lambda dev, q: gb.at[uid(dev, q)], 0)

    def mrows(m):
        return pl.ds(pl.multiple_of(m * unit, unit), unit)

    def chunk(c):
        return pl.ds(pl.multiple_of(c * CHUNK, CHUNK), CHUNK)

    for q in range(UNITS):
        gx.start_own(q)
    for i in range(2, 8):
        a_copy(i).start()
    w1b[...] = w1_ref[...].astype(BF16)
    w2acc[...] = jnp.zeros_like(w2acc)
    w2acc[:classes, :] = w2_ref[...]
    w2b[...] = w2acc[:cpad, :].astype(BF16)

    partners = [sib] + nbr

    def cnt_copy(i):
        return remote(cnt_src.at[i], cnt_rcv.at[i], cs_sem.at[i], cr_sem.at[i], partners[i])

    local = jnp.sum(msk_ref[...].astype(F32), axis=1, keepdims=True)
    local = jnp.sum(local, axis=0, keepdims=True)
    cnt_src[0] = jnp.broadcast_to(local, (8, LANES))

    def hook1(pre, i):
        if i is None:
            cnt_copy(0).start()
            for j in range(8, DEVICES):
                a_copy(j).start()
            return
        for k in range(4):
            @pl.when(i == k + 1)
            def _(k=k):
                cnt_copy(k).wait_recv()
                cnt_src[k + 1] = cnt_src[k] + cnt_rcv[k]
                if k < 3:
                    cnt_copy(k + 1).start()

        @pl.when(i == 7)
        def _():
            for k in range(4):
                cnt_copy(k).wait_send()

    def zero1():
        acc1[...] = jnp.zeros_like(acc1)

    def y1(dev, q):
        return dot(gb[uid(dev, q), :unit, :fin], w1b[...]).astype(BF16)

    def add_rows(acc, pairs, operand):
        def body(c):
            s = chunk(c)
            v = acc[s, :]
            for j, (dev, q) in enumerate(pairs):
                v = v + dot(a_v[s, rows_of(dev, q)], operand(j))
            acc[s, :] = v
        loop(rows // CHUNK, body)

    def add1(pairs):
        for j, (dev, q) in enumerate(pairs):
            ys1[j] = y1(dev, q)
        add_rows(acc1, pairs, lambda j: ys1[j])

    def finish1(m, pairs):
        s = mrows(m)

        @pl.when(m == 0)
        def _():
            for j, (dev, q) in enumerate(pairs):
                ys1[j] = y1(dev, q)
        z = acc1[s, :]
        for j, (dev, q) in enumerate(pairs):
            z = z + dot(a_v[s, rows_of(dev, q)], ys1[j])
        acc1[s, :] = z
        h = jnp.maximum(z, 0.0).astype(BF16)
        hb[rows_of(me, m), :] = h
        hown[s, :] = h
        gh.start_own(m)

    phase(gx, add1, zero1, finish1, hook1, True)

    def zero2():
        acc2[...] = jnp.zeros_like(acc2)

    def y2(dev, q):
        return dot_nt(w2b[...], hb[rows_of(dev, q), :]).astype(BF16)

    def add_cols(acc, pairs, operand):
        def body(c):
            s = chunk(c)
            v = acc[:, s]
            for j, (dev, q) in enumerate(pairs):
                v = v + dot_nt(operand(j), a_v[s, rows_of(dev, q)])
            acc[:, s] = v
        loop(rows // CHUNK, body)

    def add2(pairs):
        for j, (dev, q) in enumerate(pairs):
            ys2[j] = y2(dev, q)
        add_cols(acc2, pairs, lambda j: ys2[j])

    loss_acc[...] = jnp.zeros_like(loss_acc)
    count = cnt_src[4][0:1, :]

    def finish2(m, pairs):
        s = mrows(m)

        @pl.when(m == 0)
        def _():
            for j, (dev, q) in enumerate(pairs):
                ys2[j] = y2(dev, q)
        z = acc2[:, s]
        for j, (dev, q) in enumerate(pairs):
            z = z + dot_nt(ys2[j], a_v[s, rows_of(dev, q)])
        acc2[:, s] = z
        for h in range(unit // LANES):
            at = pl.ds(pl.multiple_of(m * unit + h * LANES, LANES), LANES)
            zc = acc2[:, at]
            row = lax.broadcasted_iota(jnp.int32, (cpad, LANES), 0)
            zm = jnp.where(row < classes, zc, -jnp.inf)
            top = jnp.max(zm, axis=0, keepdims=True)
            log_norm = top + jnp.log(jnp.sum(jnp.exp(zm - top), axis=0, keepdims=True))
            which = m * (unit // LANES) + h
            hot = row == lab_ref[pl.ds(which, 1), :]
            mask = msk_ref[pl.ds(which, 1), :].astype(F32)
            picked = jnp.sum(jnp.where(hot, zc, 0.0), axis=0, keepdims=True)
            loss_acc[...] = loss_acc[...] + mask * (log_norm - picked)
            gr = (jnp.exp(zm - log_norm) - jnp.where(hot, 1.0, 0.0)) * (mask / count)
            gb[uid(me, m), :, h * LANES:(h + 1) * LANES] = gr.astype(BF16)
        gg.start_own(m)

    phase(gh, add2, zero2, finish2, lambda pre, i: None, False)

    def finish3(m, pairs):
        s = mrows(m)
        z = acc2[:, s]
        for dev, q in pairs:
            z = z + dot_nt(gb[uid(dev, q)], a_v[s, rows_of(dev, q)])
        e = z.astype(BF16)
        e2own[:, s] = e
        gz = dot_tn(e, w2b[...])
        hb[rows_of(me, m), :] = jnp.where(acc1[s, :] > 0.0, gz, 0.0).astype(BF16)
        gh.start_own(m)

    phase(gg, lambda pairs: add_cols(acc2, pairs, lambda j: gb[uid(*pairs[j])]), zero2, finish3,
          lambda pre, i: None, False)

    total_rows = w2acc.shape[0]
    size = [total_rows // 2, total_rows // 4, total_rows // 8, total_rows // 16]
    bits = [core] + role_bit
    base = [0]
    for i in range(4):
        base.append(base[i] + bits[i] * size[i])
    roff = [0, size[0], size[0] + size[1], size[0] + size[1] + size[2]]

    def w2rows(start, n):
        return pl.ds(pl.multiple_of(start, 8), n)

    def w2_scatter(i):
        out = w2acc.at[w2rows(base[i] + (1 - bits[i]) * size[i], size[i])]
        return remote(out, w2rcv.at[pl.ds(roff[i], size[i])], w2s_sem.at[i], w2r_sem.at[i], partners[i])

    def w2_gather(i):
        out = w2f.at[w2rows(base[i + 1], size[i])]
        return remote(out, out, w2s_sem.at[4 + i], w2r_sem.at[4 + i], partners[i])

    def w2_gather_in(i):
        out = w2f.at[w2rows(base[i] + (1 - bits[i]) * size[i], size[i])]
        return remote(out, out, w2s_sem.at[4 + i], w2r_sem.at[4 + i], partners[i])

    def hook4(pre, i):
        if i is None:
            w2acc[...] = jnp.zeros_like(w2acc)
            w2acc[:cpad, :] = dot(e2own[...], hown[...])
            w2acc[total_rows - 1:, :LANES] = loss_acc[...]
            return

        @pl.when(i == 0)
        def _():
            w2_scatter(0).start()
        for k in range(4):
            @pl.when(i == k + 1)
            def _(k=k):
                w2_scatter(k).wait_recv()
                mine = w2rows(base[k + 1], size[k])
                into = w2acc if k < 3 else w2f
                into[mine, :] = w2acc[mine, :] + w2rcv[roff[k]:roff[k] + size[k], :]
                w2_scatter(k).wait_send()
                (w2_scatter(k + 1) if k < 3 else w2_gather(3)).start()
        for k in range(3):
            @pl.when(i == k + 5)
            def _(j=3 - k):
                w2_gather_in(j).wait_recv()
                w2_gather(j).wait_send()
                w2_gather(j - 1).start()

    def finish4(m, pairs):
        s = mrows(m)
        z = acc1[s, :]
        for dev, q in pairs:
            z = z + dot(a_v[s, rows_of(dev, q)], hb[rows_of(dev, q), :])
        part = dot_tn(x_ref[s, :], z.astype(BF16))
        w1p[...] = w1p[...] + part

    w1p[...] = jnp.zeros_like(w1p)
    phase(gh, lambda pairs: add_rows(acc1, pairs, lambda j: hb[rows_of(*pairs[j]), :]), zero1, finish4, hook4, False)

    sl = fin // DEVICES

    def w1rows(dev):
        return pl.ds(pl.multiple_of(dev * sl, sl), sl)

    def w1_scatter(i):
        dev = (me + i) % DEVICES
        return remote(w1p.at[w1rows(dev)], w1r.at[i], w1s_sem.at[i], w1r_sem.at[i], dev)

    def w1_gather(i):
        dev = (me + i) % DEVICES
        return remote(w1f.at[w1rows(me)], w1f.at[w1rows(me)], w1gs_sem.at[i], w1gr_sem.at[i], dev)

    def w1_gather_in(i):
        dev = (me + DEVICES - i) % DEVICES
        return remote(w1f.at[w1rows(dev)], w1f.at[w1rows(dev)], w1gs_sem.at[i], w1gr_sem.at[i], dev)

    for i in range(1, DEVICES):
        w1_scatter(i).start()
    w2_gather_in(0).wait_recv()
    w2_gather(0).wait_send()
    g2_out[...] = w2f[:classes, :]
    loss_out[0, 0] = jnp.sum(w2f[total_rows - 1:, :LANES] / cnt_src[4][0:1, :])
    total = w1p[w1rows(me), :]
    for i in range(1, DEVICES):
        w1_scatter(i).wait_recv()
    for i in range(1, DEVICES):
        total = total + w1r[i]
    w1f[w1rows(me), :] = total
    for i in range(1, DEVICES):
        w1_scatter(i).wait_send()
    for i in range(1, DEVICES):
        w1_gather(i).start()
    for i in range(1, DEVICES):
        w1_gather_in(i).wait_recv()
    g1_out[...] = w1f[...]
    for i in range(1, DEVICES):
        w1_gather(i).wait_send()


def solution(mesh):
    axis = mesh.axis_names[0]

    def local_step(adj, x, w1, w2, labels, mask):
        rows, nodes = adj.shape
        fin, hid = w1.shape
        classes = w2.shape[1]
        unit = rows // UNITS
        cpad = -(-classes // 16) * 16
        total_rows = -(-(cpad + 1) // LANES) * LANES
        dma = pltpu.SemaphoreType.DMA
        vm = pl.BlockSpec(memory_space=pltpu.VMEM)
        loss, g1, g2 = pl.pallas_call(
            functools.partial(step_kernel, classes),
            out_shape=(jax.ShapeDtypeStruct((1, 1), F32),
                       jax.ShapeDtypeStruct((fin, hid), F32),
                       jax.ShapeDtypeStruct((classes, hid), F32)),
            in_specs=[pl.BlockSpec(memory_space=pl.ANY)] + [vm] * 5,
            out_specs=(pl.BlockSpec(memory_space=pltpu.SMEM), vm, vm),
            scratch_shapes=[
                pltpu.VMEM((rows, nodes), BF16),
                pltpu.VMEM((nodes // unit, cpad, unit), BF16),
                pltpu.VMEM((nodes, hid), BF16),
                pltpu.VMEM((rows, hid), F32),
                pltpu.VMEM((cpad, rows), F32),
                pltpu.VMEM((UNITS, unit, hid), BF16),
                pltpu.VMEM((UNITS, cpad, unit), BF16),
                pltpu.VMEM((rows, hid), BF16),
                pltpu.VMEM((cpad, rows), BF16),
                pltpu.VMEM((fin, hid), BF16),
                pltpu.VMEM((cpad, hid), BF16),
                pltpu.VMEM((total_rows, hid), F32),
                pltpu.VMEM((total_rows, hid), F32),
                pltpu.VMEM((total_rows, hid), F32),
                pltpu.VMEM((fin, hid), F32),
                pltpu.VMEM((DEVICES, fin // DEVICES, hid), F32),
                pltpu.VMEM((fin, hid), F32),
                pltpu.VMEM((5, 8, LANES), F32),
                pltpu.VMEM((4, 8, LANES), F32),
                pltpu.VMEM((1, LANES), F32),
                dma((DEVICES,)),
                dma((2, 28)), dma((2, 28)), dma((2, 32)), dma((2, 32)),
                dma((4,)), dma((4,)), dma((8,)), dma((8,)),
                dma((DEVICES,)), dma((DEVICES,)), dma((DEVICES,)), dma((DEVICES,)),
            ],
            compiler_params=pltpu.CompilerParams(collective_id=0, has_side_effects=True,
                                                 vmem_limit_bytes=67043328),
            name="gcn_step",
        )(adj, x, w1, w2.T, labels.reshape(rows // LANES, LANES), mask.reshape(rows // LANES, LANES))
        return loss[0, 0], g1, g2.T

    return jax.shard_map(local_step, mesh=mesh,
                         in_specs=(P(axis, None), P(axis, None), P(None, None), P(None, None), P(axis), P(axis)),
                         out_specs=(P(), P(None, None), P(None, None)), check_vma=False)
```

```python
import functools

import jax
import jax.numpy as jnp
from jax import lax
from jax.experimental import pallas as pl
from jax.experimental.pallas import tpu as pltpu
from jax.sharding import PartitionSpec as P

F32 = jnp.float32
BF16 = jnp.bfloat16
MESH = pl.DeviceIdType.MESH
DEVICES = 16
UNITS = 4
LANES = 128
CHUNK = 1024


def dot(a, b):
    return jnp.dot(a, b, preferred_element_type=F32)


def dot_tn(a, b):
    return lax.dot_general(a, b, (((0,), (0,)), ((), ())), preferred_element_type=F32)


def dot_nt(a, b):
    return lax.dot_general(a, b, (((1,), (1,)), ((), ())), preferred_element_type=F32)


def loop(n, fn):
    lax.fori_loop(0, n, lambda i, c: (fn(i), c)[1], 0)


def step_kernel(classes, adj, x_ref, w1_ref, w2_ref, lab_ref, msk_ref,
                loss_out, g1_out, g2_out,
                a_v, gb, hb, acc1, acc2, ys1, ys2, hown, e2own, w1b, w2b,
                w2acc, w2rcv, w2part, w2f, w1p, w1r, w1f, cnt_own, cnt_rcv, cnt, loss_acc,
                a_sem, rsem, ssem, sib_rsem, sib_ssem, cs_sem, cr_sem,
                w2s_sem, w2r_sem, w1s_sem, w1r_sem, w1gs_sem, w1gr_sem):
    rows = x_ref.shape[0]
    fin = x_ref.shape[1]
    unit = rows // UNITS
    hid = w1_ref.shape[1]
    cpad = w2b.shape[0]
    me = lax.axis_index("nodes")
    core = me % 2
    sib = me + 1 - 2 * core
    bit = [(me // v) % 2 for v in (2, 4, 8)]
    step = [v * (1 - 2 * b) for v, b in zip((2, 4, 8), bit)]
    own_d = [(1 - core) * step[r] + core * step[(r + 1) % 3] for r in range(3)]
    sib_d = [core * step[r] + (1 - core) * step[(r + 1) % 3] for r in range(3)]
    role_bit = [(1 - core) * bit[r] + core * bit[(r + 1) % 3] for r in range(3)]
    nbr = [me + d for d in own_d]

    def src_dev(base, deltas, hop, r):
        return base + deltas[r] + hop * deltas[(r + 2) % 3]

    anti = me + own_d[0] + own_d[1] + own_d[2]
    anti_sib = anti + 1 - 2 * core

    def remote(src, dst, ss, rs, dev):
        return pltpu.make_async_remote_copy(src_ref=src, dst_ref=dst, send_sem=ss, recv_sem=rs,
                                            device_id=(dev,), device_id_type=MESH)

    order = [me, sib]
    for hop in (0, 1):
        order += [src_dev(me, own_d, hop, r) for r in range(3)]
        order += [src_dev(sib, sib_d, hop, r) for r in range(3)]
    order += [anti, anti_sib]

    def a_cols(dev):
        return pl.ds(pl.multiple_of(dev * rows, rows), rows)

    def a_copy(i):
        return pltpu.make_async_copy(adj.at[:, a_cols(order[i])], a_v.at[:, a_cols(order[i])], a_sem.at[i])

    for i in range(2):
        a_copy(i).start()

    def rows_of(dev, q):
        return pl.ds(pl.multiple_of(dev * rows + q * unit, unit), unit)

    def uid(dev, q):
        return dev * UNITS + q

    for q in range(UNITS):
        gb[uid(me, q), :unit, :fin] = x_ref[q * unit:(q + 1) * unit, :]

    barrier = pltpu.get_barrier_semaphore()
    for dev in [sib] + nbr:
        pl.semaphore_signal(barrier, inc=1, device_id=(dev,), device_id_type=MESH)
    pl.semaphore_wait(barrier, 4)

    def pick(f, vals):
        return jnp.where(f == 0, vals[0], jnp.where(f == 1, vals[1], vals[2]))

    class Gather:
        def __init__(self, view, par):
            self.view, self.par = view, par

        def hop_copy(self, dev, q, to, sslot, rslot):
            v = self.view(dev, q)
            return remote(v, v, ssem.at[self.par, sslot], rsem.at[self.par, rslot], to)

        def sib_copy(self, dev, q, slot):
            v = self.view(dev, q)
            return remote(v, v, sib_ssem.at[self.par, slot], sib_rsem.at[self.par, slot], sib)

        def own_copies(self, q):
            return [self.hop_copy(me, q, nbr[r], r * 4 + q, r * 4 + q) for r in range(3)] + [self.sib_copy(me, q, 28 + q)]

        def start_own(self, q):
            for c in self.own_copies(q):
                c.start()

        def forward(self, q):
            return [self.hop_copy(src_dev(me, own_d, 0, r), q, nbr[(r + 1) % 3], 12 + r * 4 + q,
                                  12 + ((r + 1) % 3) * 4 + q) for r in range(3)]

        def last_forward(self, q):
            to = q % 3
            dev = pick((to + 2) % 3, [src_dev(me, own_d, 1, r) for r in range(3)])
            return self.hop_copy(dev, q, pick(to, nbr), 24 + q, 24 + q)

        def arrive(self, hop, q):
            for r in range(3):
                d = src_dev(me, own_d, hop, r)
                self.hop_copy(d, q, nbr[r], r * 4 + q, hop * 12 + r * 4 + q).wait_recv()

            @pl.when(hop == 0)
            def _():
                for c in self.forward(q):
                    c.start()

            @pl.when(hop == 1)
            def _():
                self.last_forward(q).start()
            for r in range(3):
                self.sib_copy(src_dev(me, own_d, hop, r), q, hop * 12 + r * 4 + q).start()

        def arrive_last(self, q):
            self.hop_copy(anti, q, nbr[0], 24 + q, 24 + q).wait_recv()
            self.sib_copy(anti, q, 24 + q).start()

        def sib_wait(self, hop, q):
            for r in range(3):
                self.sib_copy(src_dev(sib, sib_d, hop, r), q, hop * 12 + r * 4 + q).wait_recv()

        def sib_wait_own(self, q):
            self.sib_copy(sib, q, 28 + q).wait_recv()

        def sib_wait_last(self, q):
            self.sib_copy(anti_sib, q, 24 + q).wait_recv()

        def wait_sends(self):
            def body(q):
                for c in self.own_copies(q) + self.forward(q) + [self.last_forward(q)]:
                    c.wait_send()
                for slot in (q, 4 + q, 8 + q, 12 + q, 16 + q, 20 + q, 24 + q):
                    self.sib_copy(me, q, slot).wait_send()
            loop(UNITS, body)

    def phase(g, add, zero, finish, hook, first):
        def a_wait(lo, hi):
            if first:
                for i in range(lo, hi):
                    a_copy(i).wait()

        zero()

        def near(t):
            if first:
                @pl.when(t == 0)
                def _():
                    a_wait(0, 1)

            @pl.when(t == 1)
            def _():
                for q in range(UNITS):
                    g.sib_wait_own(q)
                a_wait(1, 2)
            dev = me + t * (sib - me)
            add([(dev, q) for q in range(UNITS)])
        loop(2, near)
        hook(-1, None)

        def group(i):
            @pl.when(i < 8)
            def _():
                g.arrive(i // 4, i % 4)

            @pl.when(i == 8)
            def _():
                for j in range(3):
                    g.arrive_last(j)

            @pl.when(i == 9)
            def _():
                g.arrive_last(3)
            hook(None, i)

            def half(t):
                k = i - t
                hop, q, far = (k // 4) % 2, k % 4, k // 8

                @pl.when((k >= 0) & (k <= 8))
                def _():
                    @pl.when((t == 1) & (k < 8))
                    def _():
                        g.sib_wait(hop, q)

                    @pl.when((t == 1) & (k == 8))
                    def _():
                        for j in range(3):
                            g.sib_wait_last(j)
                    if first:
                        for key, (lo, hi) in {(0, 0): (2, 5), (0, 1): (5, 8), (4, 0): (8, 11), (4, 1): (11, 14),
                                              (8, 0): (14, 15), (8, 1): (15, 16)}.items():
                            @pl.when((k == key[0]) & (t == key[1]))
                            def _(lo=lo, hi=hi):
                                a_wait(lo, hi)
                    pairs = []
                    for r in range(3):
                        o, s = src_dev(me, own_d, hop, r), src_dev(sib, sib_d, hop, r)
                        near_dev = o + t * (s - o)
                        far_dev = anti + t * (anti_sib - anti)
                        pairs.append((near_dev + far * (far_dev - near_dev), q + far * (r - q)))
                    add(pairs)
            loop(2, half)
        loop(10, group)
        g.sib_wait_last(3)

        def last(m):
            @pl.when(m == UNITS - 1)
            def _():
                g.wait_sends()
            finish(m, [(anti, 3), (anti_sib, 3)])
        loop(UNITS, last)

    gx = Gather(lambda dev, q: gb.at[uid(dev, q), pl.ds(0, unit), pl.ds(0, fin)], 0)
    gh = Gather(lambda dev, q: hb.at[rows_of(dev, q)], 1)
    gg = Gather(lambda dev, q: gb.at[uid(dev, q)], 0)

    def mrows(m):
        return pl.ds(pl.multiple_of(m * unit, unit), unit)

    def chunk(c):
        return pl.ds(pl.multiple_of(c * CHUNK, CHUNK), CHUNK)

    for q in range(UNITS):
        gx.start_own(q)
    for i in range(2, 8):
        a_copy(i).start()
    w1b[...] = w1_ref[...].astype(BF16)
    w2acc[...] = jnp.zeros_like(w2acc)
    w2acc[:classes, :] = w2_ref[...]
    w2b[...] = w2acc[:cpad, :].astype(BF16)

    def cnt_copy(i):
        return remote(cnt_own, cnt_rcv.at[i], cs_sem.at[i], cr_sem.at[i], (me + i) % DEVICES)

    local = jnp.sum(msk_ref[...].astype(F32), axis=1, keepdims=True)
    local = jnp.sum(local, axis=0, keepdims=True)
    cnt_own[...] = jnp.broadcast_to(local, (8, LANES))

    def hook1(pre, i):
        if i is None:
            for j in range(8, DEVICES):
                a_copy(j).start()

    def zero1():
        acc1[...] = jnp.zeros_like(acc1)

    def y1(dev, q):
        return dot(gb[uid(dev, q), :unit, :fin], w1b[...]).astype(BF16)

    def add_rows(acc, pairs, operand):
        def body(c):
            s = chunk(c)
            v = acc[s, :]
            for j, (dev, q) in enumerate(pairs):
                v = v + dot(a_v[s, rows_of(dev, q)], operand(j))
            acc[s, :] = v
        loop(rows // CHUNK, body)

    def add1(pairs):
        for j, (dev, q) in enumerate(pairs):
            ys1[j] = y1(dev, q)
        add_rows(acc1, pairs, lambda j: ys1[j])

    def finish1(m, pairs):
        s = mrows(m)

        @pl.when(m == 0)
        def _():
            for j, (dev, q) in enumerate(pairs):
                ys1[j] = y1(dev, q)
        z = acc1[s, :]
        for j, (dev, q) in enumerate(pairs):
            z = z + dot(a_v[s, rows_of(dev, q)], ys1[j])
        acc1[s, :] = z
        h = jnp.maximum(z, 0.0).astype(BF16)
        hb[rows_of(me, m), :] = h
        hown[s, :] = h
        gh.start_own(m)

    phase(gx, add1, zero1, finish1, hook1, True)

    def zero2():
        acc2[...] = jnp.zeros_like(acc2)

    def y2(dev, q):
        return dot_nt(w2b[...], hb[rows_of(dev, q), :]).astype(BF16)

    def add_cols(acc, pairs, operand):
        def body(c):
            s = chunk(c)
            v = acc[:, s]
            for j, (dev, q) in enumerate(pairs):
                v = v + dot_nt(operand(j), a_v[s, rows_of(dev, q)])
            acc[:, s] = v
        loop(rows // CHUNK, body)

    def add2(pairs):
        for j, (dev, q) in enumerate(pairs):
            ys2[j] = y2(dev, q)
        add_cols(acc2, pairs, lambda j: ys2[j])

    loss_acc[...] = jnp.zeros_like(loss_acc)

    def hook2(pre, i):
        if i is None:
            for j in range(1, DEVICES):
                cnt_copy(j).start()
            return

        @pl.when(i == 9)
        def _():
            for j in range(1, DEVICES):
                cnt_copy(j).wait_recv()
            total = cnt_own[...]
            for j in range(1, DEVICES):
                total = total + cnt_rcv[j]
            cnt[...] = total
            for j in range(1, DEVICES):
                cnt_copy(j).wait_send()

    def finish2(m, pairs):
        s = mrows(m)

        @pl.when(m == 0)
        def _():
            for j, (dev, q) in enumerate(pairs):
                ys2[j] = y2(dev, q)
        z = acc2[:, s]
        for j, (dev, q) in enumerate(pairs):
            z = z + dot_nt(ys2[j], a_v[s, rows_of(dev, q)])
        acc2[:, s] = z
        for h in range(unit // LANES):
            at = pl.ds(pl.multiple_of(m * unit + h * LANES, LANES), LANES)
            zc = acc2[:, at]
            row = lax.broadcasted_iota(jnp.int32, (cpad, LANES), 0)
            zm = jnp.where(row < classes, zc, -jnp.inf)
            top = jnp.max(zm, axis=0, keepdims=True)
            log_norm = top + jnp.log(jnp.sum(jnp.exp(zm - top), axis=0, keepdims=True))
            which = m * (unit // LANES) + h
            hot = row == lab_ref[pl.ds(which, 1), :]
            mask = msk_ref[pl.ds(which, 1), :].astype(F32)
            picked = jnp.sum(jnp.where(hot, zc, 0.0), axis=0, keepdims=True)
            loss_acc[...] = loss_acc[...] + mask * (log_norm - picked)
            gr = (jnp.exp(zm - log_norm) - jnp.where(hot, 1.0, 0.0)) * (mask / cnt[0:1, :])
            gb[uid(me, m), :, h * LANES:(h + 1) * LANES] = gr.astype(BF16)
        gg.start_own(m)

    phase(gh, add2, zero2, finish2, hook2, False)

    def finish3(m, pairs):
        s = mrows(m)
        z = acc2[:, s]
        for dev, q in pairs:
            z = z + dot_nt(gb[uid(dev, q)], a_v[s, rows_of(dev, q)])
        e = z.astype(BF16)
        e2own[:, s] = e
        gz = dot_tn(e, w2b[...])
        hb[rows_of(me, m), :] = jnp.where(acc1[s, :] > 0.0, gz, 0.0).astype(BF16)
        gh.start_own(m)

    phase(gg, lambda pairs: add_cols(acc2, pairs, lambda j: gb[uid(*pairs[j])]), zero2, finish3,
          lambda pre, i: None, False)

    total_rows = w2acc.shape[0]
    half_rows = total_rows // 2
    piece = half_rows // 8
    chips = DEVICES // 2
    chip = me // 2

    def w2rows(start, n):
        return pl.ds(pl.multiple_of(start, 8), n)

    mine = w2rows(core * half_rows, half_rows)

    def w2_sib():
        out = w2acc.at[w2rows((1 - core) * half_rows, half_rows)]
        return remote(out, w2rcv, w2s_sem.at[0], w2r_sem.at[0], sib)

    def w2_scatter(j):
        to = (chip + j) % chips
        out = w2acc.at[w2rows(core * half_rows + to * piece, piece)]
        return remote(out, w2part.at[j], w2s_sem.at[j], w2r_sem.at[j], to * 2 + core)

    def w2_gather(j, frm):
        to = (chip + j) % chips
        out = w2f.at[w2rows(core * half_rows + frm * piece, piece)]
        return remote(out, out, w2s_sem.at[chips + j], w2r_sem.at[chips + j], to * 2 + core)

    def w2_sib_gather(c):
        out = w2f.at[w2rows(c * half_rows, half_rows)]
        return remote(out, out, w2s_sem.at[chips], w2r_sem.at[chips], sib)

    def hook4(pre, i):
        if i is None:
            w2acc[...] = jnp.zeros_like(w2acc)
            w2acc[:cpad, :] = dot(e2own[...], hown[...])
            w2acc[total_rows - 1:, :LANES] = loss_acc[...]
            return

        @pl.when(i == 0)
        def _():
            w2_sib().start()

        @pl.when(i == 1)
        def _():
            w2_sib().wait_recv()
            w2acc[mine, :] = w2acc[mine, :] + w2rcv[...]

        @pl.when(i == 2)
        def _():
            w2_sib().wait_send()
            for j in range(1, chips):
                w2_scatter(j).start()

        @pl.when(i == 8)
        def _():
            own = w2rows(core * half_rows + chip * piece, piece)
            total = w2acc[own, :]
            for j in range(1, chips):
                w2_scatter(j).wait_recv()
            for j in range(1, chips):
                total = total + w2part[j]
            w2f[own, :] = total
            for j in range(1, chips):
                w2_scatter(j).wait_send()

        @pl.when(i == 9)
        def _():
            for j in range(1, chips):
                w2_gather(j, chip).start()

    def finish4(m, pairs):
        s = mrows(m)
        z = acc1[s, :]
        for dev, q in pairs:
            z = z + dot(a_v[s, rows_of(dev, q)], hb[rows_of(dev, q), :])
        part = dot_tn(x_ref[s, :], z.astype(BF16))
        w1p[...] = w1p[...] + part

    w1p[...] = jnp.zeros_like(w1p)
    phase(gh, lambda pairs: add_rows(acc1, pairs, lambda j: hb[rows_of(*pairs[j]), :]), zero1, finish4, hook4, False)

    sl = fin // DEVICES

    def w1rows(dev):
        return pl.ds(pl.multiple_of(dev * sl, sl), sl)

    def w1_scatter(i):
        dev = (me + i) % DEVICES
        return remote(w1p.at[w1rows(dev)], w1r.at[i], w1s_sem.at[i], w1r_sem.at[i], dev)

    def w1_gather(i):
        dev = (me + i) % DEVICES
        return remote(w1f.at[w1rows(me)], w1f.at[w1rows(me)], w1gs_sem.at[i], w1gr_sem.at[i], dev)

    def w1_gather_in(i):
        dev = (me + DEVICES - i) % DEVICES
        return remote(w1f.at[w1rows(dev)], w1f.at[w1rows(dev)], w1gs_sem.at[i], w1gr_sem.at[i], dev)

    for i in range(1, DEVICES):
        w1_scatter(i).start()
    total = w1p[w1rows(me), :]
    for j in range(1, chips):
        w2_gather(j, (chip + chips - j) % chips).wait_recv()
    w2_sib_gather(core).start()
    for j in range(1, chips):
        w2_gather(j, chip).wait_send()
    for i in range(1, DEVICES):
        w1_scatter(i).wait_recv()
    for i in range(1, DEVICES):
        total = total + w1r[i]
    w1f[w1rows(me), :] = total
    for i in range(1, DEVICES):
        w1_scatter(i).wait_send()
    for i in range(1, DEVICES):
        w1_gather(i).start()
    w2_sib_gather(1 - core).wait_recv()
    w2_sib_gather(core).wait_send()
    g2_out[...] = w2f[:classes, :]
    loss_out[0, 0] = jnp.sum(w2f[total_rows - 1:, :LANES] / cnt[0:1, :])
    for i in range(1, DEVICES):
        w1_gather_in(i).wait_recv()
    g1_out[...] = w1f[...]
    for i in range(1, DEVICES):
        w1_gather(i).wait_send()


def solution(mesh):
    axis = mesh.axis_names[0]

    def local_step(adj, x, w1, w2, labels, mask):
        rows, nodes = adj.shape
        fin, hid = w1.shape
        classes = w2.shape[1]
        unit = rows // UNITS
        cpad = -(-classes // 16) * 16
        total_rows = -(-(cpad + 1) // LANES) * LANES
        dma = pltpu.SemaphoreType.DMA
        vm = pl.BlockSpec(memory_space=pltpu.VMEM)
        loss, g1, g2 = pl.pallas_call(
            functools.partial(step_kernel, classes),
            out_shape=(jax.ShapeDtypeStruct((1, 1), F32),
                       jax.ShapeDtypeStruct((fin, hid), F32),
                       jax.ShapeDtypeStruct((classes, hid), F32)),
            in_specs=[pl.BlockSpec(memory_space=pl.ANY)] + [vm] * 5,
            out_specs=(pl.BlockSpec(memory_space=pltpu.SMEM), vm, vm),
            scratch_shapes=[
                pltpu.VMEM((rows, nodes), BF16),
                pltpu.VMEM((nodes // unit, cpad, unit), BF16),
                pltpu.VMEM((nodes, hid), BF16),
                pltpu.VMEM((rows, hid), F32),
                pltpu.VMEM((cpad, rows), F32),
                pltpu.VMEM((UNITS, unit, hid), BF16),
                pltpu.VMEM((UNITS, cpad, unit), BF16),
                pltpu.VMEM((rows, hid), BF16),
                pltpu.VMEM((cpad, rows), BF16),
                pltpu.VMEM((fin, hid), BF16),
                pltpu.VMEM((cpad, hid), BF16),
                pltpu.VMEM((total_rows, hid), F32),
                pltpu.VMEM((total_rows // 2, hid), F32),
                pltpu.VMEM((8, total_rows // 16, hid), F32),
                pltpu.VMEM((total_rows, hid), F32),
                pltpu.VMEM((fin, hid), F32),
                pltpu.VMEM((DEVICES, fin // DEVICES, hid), F32),
                pltpu.VMEM((fin, hid), F32),
                pltpu.VMEM((8, LANES), F32),
                pltpu.VMEM((DEVICES, 8, LANES), F32),
                pltpu.VMEM((8, LANES), F32),
                pltpu.VMEM((1, LANES), F32),
                dma((DEVICES,)),
                dma((2, 28)), dma((2, 28)), dma((2, 32)), dma((2, 32)),
                dma((DEVICES,)), dma((DEVICES,)), dma((DEVICES,)), dma((DEVICES,)),
                dma((DEVICES,)), dma((DEVICES,)), dma((DEVICES,)), dma((DEVICES,)),
            ],
            compiler_params=pltpu.CompilerParams(collective_id=0, has_side_effects=True,
                                                 vmem_limit_bytes=67043328),
            name="gcn_step",
        )(adj, x, w1, w2.T, labels.reshape(rows // LANES, LANES), mask.reshape(rows // LANES, LANES))
        return loss[0, 0], g1, g2.T

    return jax.shard_map(local_step, mesh=mesh,
                         in_specs=(P(axis, None), P(axis, None), P(None, None), P(None, None), P(axis), P(axis)),
                         out_specs=(P(), P(None, None), P(None, None)), check_vma=False)
```

```python
import functools

import jax
import jax.numpy as jnp
from jax import lax
from jax.experimental import pallas as pl
from jax.experimental.pallas import tpu as pltpu
from jax.sharding import PartitionSpec as P

F32 = jnp.float32
BF16 = jnp.bfloat16
MESH = pl.DeviceIdType.MESH
DEVICES = 16
UNITS = 4
LANES = 128
CHUNK = 1024


def dot(a, b):
    return jnp.dot(a, b, preferred_element_type=F32)


def dot_tn(a, b):
    return lax.dot_general(a, b, (((0,), (0,)), ((), ())), preferred_element_type=F32)


def dot_nt(a, b):
    return lax.dot_general(a, b, (((1,), (1,)), ((), ())), preferred_element_type=F32)


def loop(n, fn):
    lax.fori_loop(0, n, lambda i, c: (fn(i), c)[1], 0)


def step_kernel(classes, adj, x_hbm, w1_hbm, w2_hbm, lab_hbm, msk_hbm,
                loss_out, g1_out, g2_out,
                x_ref, w1_ref, w2_ref, lab_ref, msk_ref, in_sem,
                a_v, gb, hb, acc1, acc2, ys1, ys2, hown, e2own, w1b, w2b,
                w2acc, w2rcv, w2part, w2f, w1p, w1r, w1f, cnt_own, cnt_rcv, cnt, loss_acc,
                a_sem, rsem, ssem, sib_rsem, sib_ssem, cs_sem, cr_sem,
                w2s_sem, w2r_sem, w1s_sem, w1r_sem, w1gs_sem, w1gr_sem):
    rows = x_ref.shape[0]
    fin = x_ref.shape[1]
    unit = rows // UNITS
    hid = w1_ref.shape[1]
    cpad = w2b.shape[0]
    me = lax.axis_index("nodes")
    core = me % 2
    sib = me + 1 - 2 * core
    bit = [(me // v) % 2 for v in (2, 4, 8)]
    step = [v * (1 - 2 * b) for v, b in zip((2, 4, 8), bit)]
    own_d = [(1 - core) * step[r] + core * step[(r + 1) % 3] for r in range(3)]
    sib_d = [core * step[r] + (1 - core) * step[(r + 1) % 3] for r in range(3)]
    role_bit = [(1 - core) * bit[r] + core * bit[(r + 1) % 3] for r in range(3)]
    nbr = [me + d for d in own_d]

    def src_dev(base, deltas, hop, r):
        return base + deltas[r] + hop * deltas[(r + 2) % 3]

    anti = me + own_d[0] + own_d[1] + own_d[2]
    anti_sib = anti + 1 - 2 * core

    def remote(src, dst, ss, rs, dev):
        return pltpu.make_async_remote_copy(src_ref=src, dst_ref=dst, send_sem=ss, recv_sem=rs,
                                            device_id=(dev,), device_id_type=MESH)

    barrier = pltpu.get_barrier_semaphore()
    for dev in [sib] + nbr:
        pl.semaphore_signal(barrier, inc=1, device_id=(dev,), device_id_type=MESH)

    def uid(dev, q):
        return dev * UNITS + q

    order = [me, sib]
    for hop in (0, 1):
        order += [src_dev(me, own_d, hop, r) for r in range(3)]
        order += [src_dev(sib, sib_d, hop, r) for r in range(3)]
    order += [anti, anti_sib]

    def a_cols(dev):
        return pl.ds(pl.multiple_of(dev * rows, rows), rows)

    def a_copy(i):
        return pltpu.make_async_copy(adj.at[:, a_cols(order[i])], a_v.at[:, a_cols(order[i])], a_sem.at[i])

    x_units = [pltpu.make_async_copy(x_hbm.at[pl.ds(q * unit, unit)], gb.at[uid(me, q), pl.ds(0, unit), pl.ds(0, fin)],
                                     in_sem.at[q]) for q in range(UNITS)]
    inputs = [pltpu.make_async_copy(src, dst, in_sem.at[UNITS + i]) for i, (src, dst) in enumerate(
        [(w1_hbm, w1_ref), (w2_hbm, w2_ref), (msk_hbm, msk_ref), (lab_hbm, lab_ref), (x_hbm, x_ref)])]
    for c in x_units + inputs:
        c.start()
    for i in range(2):
        a_copy(i).start()

    def rows_of(dev, q):
        return pl.ds(pl.multiple_of(dev * rows + q * unit, unit), unit)

    pl.semaphore_wait(barrier, 4)

    def pick(f, vals):
        return jnp.where(f == 0, vals[0], jnp.where(f == 1, vals[1], vals[2]))

    class Gather:
        def __init__(self, view, height, par):
            self.view, self.height, self.par = view, height, par

        def hop_copy(self, dev, q, to, sslot, rslot):
            v = self.view(dev, q)
            return remote(v, v, ssem.at[self.par, sslot], rsem.at[self.par, rslot], to)

        def sib_copy(self, dev, q, slot):
            v = self.view(dev, q)
            return remote(v, v, sib_ssem.at[self.par, slot], sib_rsem.at[self.par, slot], sib)

        def own_copies(self, q):
            return [self.hop_copy(me, q, nbr[r], r * 4 + q, r * 4 + q) for r in range(3)] + [self.sib_copy(me, q, 28 + q)]

        def start_own(self, q):
            for c in self.own_copies(q):
                c.start()

        def forward(self, q):
            return [self.hop_copy(src_dev(me, own_d, 0, r), q, nbr[(r + 1) % 3], 12 + r * 4 + q,
                                  12 + ((r + 1) % 3) * 4 + q) for r in range(3)]

        def last_forward(self, q):
            to = q % 3
            dev = pick((to + 2) % 3, [src_dev(me, own_d, 1, r) for r in range(3)])
            return self.hop_copy(dev, q, pick(to, nbr), 24 + q, 24 + q)

        def thirds(self, dev):
            tiles = self.height // 16
            at = [0, tiles // 3 * 16, 2 * (tiles // 3) * 16, self.height]
            return [self.view(dev, 3).at[pl.ds(at[t], at[t + 1] - at[t])] for t in range(3)]

        def third_copy(self, t):
            v = self.thirds(src_dev(me, own_d, 1, (t + 2) % 3))[t]
            return remote(v, v, ssem.at[self.par, 27 + t], rsem.at[self.par, 27 + t], nbr[t])

        def third_in(self, t):
            v = self.thirds(anti)[t]
            return remote(v, v, ssem.at[self.par, 27 + t], rsem.at[self.par, 27 + t], nbr[t])

        def arrive(self, hop, q):
            for r in range(3):
                d = src_dev(me, own_d, hop, r)
                self.hop_copy(d, q, nbr[r], r * 4 + q, hop * 12 + r * 4 + q).wait_recv()

            @pl.when(hop == 0)
            def _():
                for c in self.forward(q):
                    c.start()

            @pl.when((hop == 1) & (q < 3))
            def _():
                self.last_forward(q).start()

            @pl.when((hop == 1) & (q == 3))
            def _():
                for t in range(3):
                    self.third_copy(t).start()
            for r in range(3):
                self.sib_copy(src_dev(me, own_d, hop, r), q, hop * 12 + r * 4 + q).start()

        def arrive_last(self, q):
            if q < 3:
                self.hop_copy(anti, q, nbr[0], 24 + q, 24 + q).wait_recv()
            else:
                for t in range(3):
                    self.third_in(t).wait_recv()
            self.sib_copy(anti, q, 24 + q).start()

        def sib_wait(self, hop, q):
            for r in range(3):
                self.sib_copy(src_dev(sib, sib_d, hop, r), q, hop * 12 + r * 4 + q).wait_recv()

        def sib_wait_own(self, q):
            self.sib_copy(sib, q, 28 + q).wait_recv()

        def sib_wait_last(self, q):
            self.sib_copy(anti_sib, q, 24 + q).wait_recv()

        def wait_sends(self):
            def body(q):
                for c in self.own_copies(q) + self.forward(q):
                    c.wait_send()
                for slot in (q, 4 + q, 8 + q, 12 + q, 16 + q, 20 + q, 24 + q):
                    self.sib_copy(me, q, slot).wait_send()
            loop(UNITS, body)
            for q in range(3):
                self.last_forward(q).wait_send()
            for t in range(3):
                self.third_copy(t).wait_send()

    def phase(g, add, zero, finish, hook, first):
        def a_wait(lo, hi):
            if first:
                for i in range(lo, hi):
                    a_copy(i).wait()

        zero()

        def near(t):
            if first:
                @pl.when(t == 0)
                def _():
                    a_wait(0, 1)

            @pl.when(t == 1)
            def _():
                for q in range(UNITS):
                    g.sib_wait_own(q)
                a_wait(1, 2)
            dev = me + t * (sib - me)
            add([(dev, q) for q in range(UNITS)])
        loop(2, near)
        hook(-1, None)

        def group(i):
            @pl.when(i < 8)
            def _():
                g.arrive(i // 4, i % 4)

            @pl.when(i == 8)
            def _():
                for j in range(3):
                    g.arrive_last(j)

            @pl.when(i == 9)
            def _():
                g.arrive_last(3)
            hook(None, i)

            def half(t):
                k = i - t
                hop, q, far = (k // 4) % 2, k % 4, k // 8

                @pl.when((k >= 0) & (k <= 8))
                def _():
                    @pl.when((t == 1) & (k < 8))
                    def _():
                        g.sib_wait(hop, q)

                    @pl.when((t == 1) & (k == 8))
                    def _():
                        for j in range(3):
                            g.sib_wait_last(j)
                    if first:
                        for key, (lo, hi) in {(0, 0): (2, 5), (0, 1): (5, 8), (4, 0): (8, 11), (4, 1): (11, 14),
                                              (8, 0): (14, 15), (8, 1): (15, 16)}.items():
                            @pl.when((k == key[0]) & (t == key[1]))
                            def _(lo=lo, hi=hi):
                                a_wait(lo, hi)
                    pairs = []
                    for r in range(3):
                        o, s = src_dev(me, own_d, hop, r), src_dev(sib, sib_d, hop, r)
                        near_dev = o + t * (s - o)
                        far_dev = anti + t * (anti_sib - anti)
                        pairs.append((near_dev + far * (far_dev - near_dev), q + far * (r - q)))
                    add(pairs)
            loop(2, half)
        loop(10, group)
        add([(anti, 3)])
        g.sib_wait_last(3)

        def last(m):
            @pl.when(m == UNITS - 1)
            def _():
                g.wait_sends()
            finish(m, [(anti_sib, 3)])
        loop(UNITS, last)

    gx = Gather(lambda dev, q: gb.at[uid(dev, q), pl.ds(0, unit), pl.ds(0, fin)], unit, 0)
    gh = Gather(lambda dev, q: hb.at[rows_of(dev, q)], unit, 1)
    gg = Gather(lambda dev, q: gb.at[uid(dev, q)], cpad, 0)

    def mrows(m):
        return pl.ds(pl.multiple_of(m * unit, unit), unit)

    def chunk(c):
        return pl.ds(pl.multiple_of(c * CHUNK, CHUNK), CHUNK)

    for q in range(UNITS):
        x_units[q].wait()
        gx.start_own(q)
    for i in range(2, 8):
        a_copy(i).start()
    for c in inputs:
        c.wait()
    w1b[...] = w1_ref[...].astype(BF16)
    w2acc[...] = jnp.zeros_like(w2acc)
    w2acc[:classes, :] = w2_ref[...]
    w2b[...] = w2acc[:cpad, :].astype(BF16)

    def cnt_copy(i):
        return remote(cnt_own, cnt_rcv.at[i], cs_sem.at[i], cr_sem.at[i], (me + i) % DEVICES)

    local = jnp.sum(msk_ref[...].astype(F32), axis=1, keepdims=True)
    local = jnp.sum(local, axis=0, keepdims=True)
    cnt_own[...] = jnp.broadcast_to(local, (8, LANES))

    def hook1(pre, i):
        if i is None:
            for j in range(8, DEVICES):
                a_copy(j).start()

    def zero1():
        acc1[...] = jnp.zeros_like(acc1)

    def y1(dev, q):
        return dot(gb[uid(dev, q), :unit, :fin], w1b[...]).astype(BF16)

    def add_rows(acc, pairs, operand):
        def body(c):
            s = chunk(c)
            v = acc[s, :]
            for j, (dev, q) in enumerate(pairs):
                v = v + dot(a_v[s, rows_of(dev, q)], operand(j))
            acc[s, :] = v
        loop(rows // CHUNK, body)

    def add1(pairs):
        for j, (dev, q) in enumerate(pairs):
            ys1[j] = y1(dev, q)
        add_rows(acc1, pairs, lambda j: ys1[j])

    def finish1(m, pairs):
        s = mrows(m)

        @pl.when(m == 0)
        def _():
            for j, (dev, q) in enumerate(pairs):
                ys1[j] = y1(dev, q)
        z = acc1[s, :]
        for j, (dev, q) in enumerate(pairs):
            z = z + dot(a_v[s, rows_of(dev, q)], ys1[j])
        acc1[s, :] = z
        h = jnp.maximum(z, 0.0).astype(BF16)
        hb[rows_of(me, m), :] = h
        hown[s, :] = h
        gh.start_own(m)

    phase(gx, add1, zero1, finish1, hook1, True)

    def zero2():
        acc2[...] = jnp.zeros_like(acc2)

    def y2(dev, q):
        return dot_nt(w2b[...], hb[rows_of(dev, q), :]).astype(BF16)

    def add_cols(acc, pairs, operand):
        def body(c):
            s = chunk(c)
            v = acc[:, s]
            for j, (dev, q) in enumerate(pairs):
                v = v + dot_nt(operand(j), a_v[s, rows_of(dev, q)])
            acc[:, s] = v
        loop(rows // CHUNK, body)

    def add2(pairs):
        for j, (dev, q) in enumerate(pairs):
            ys2[j] = y2(dev, q)
        add_cols(acc2, pairs, lambda j: ys2[j])

    loss_acc[...] = jnp.zeros_like(loss_acc)

    def hook2(pre, i):
        if i is None:
            for j in range(1, DEVICES):
                cnt_copy(j).start()
            return

        @pl.when(i == 9)
        def _():
            for j in range(1, DEVICES):
                cnt_copy(j).wait_recv()
            total = cnt_own[...]
            for j in range(1, DEVICES):
                total = total + cnt_rcv[j]
            cnt[...] = total
            for j in range(1, DEVICES):
                cnt_copy(j).wait_send()

    def finish2(m, pairs):
        s = mrows(m)

        @pl.when(m == 0)
        def _():
            for j, (dev, q) in enumerate(pairs):
                ys2[j] = y2(dev, q)
        z = acc2[:, s]
        for j, (dev, q) in enumerate(pairs):
            z = z + dot_nt(ys2[j], a_v[s, rows_of(dev, q)])
        acc2[:, s] = z
        for h in range(unit // LANES):
            at = pl.ds(pl.multiple_of(m * unit + h * LANES, LANES), LANES)
            zc = acc2[:, at]
            row = lax.broadcasted_iota(jnp.int32, (cpad, LANES), 0)
            zm = jnp.where(row < classes, zc, -jnp.inf)
            top = jnp.max(zm, axis=0, keepdims=True)
            log_norm = top + jnp.log(jnp.sum(jnp.exp(zm - top), axis=0, keepdims=True))
            which = m * (unit // LANES) + h
            hot = row == lab_ref[pl.ds(which, 1), :]
            mask = msk_ref[pl.ds(which, 1), :].astype(F32)
            picked = jnp.sum(jnp.where(hot, zc, 0.0), axis=0, keepdims=True)
            loss_acc[...] = loss_acc[...] + mask * (log_norm - picked)
            gr = (jnp.exp(zm - log_norm) - jnp.where(hot, 1.0, 0.0)) * (mask / cnt[0:1, :])
            gb[uid(me, m), :, h * LANES:(h + 1) * LANES] = gr.astype(BF16)
        gg.start_own(m)

    phase(gh, add2, zero2, finish2, hook2, False)

    def finish3(m, pairs):
        s = mrows(m)
        z = acc2[:, s]
        for dev, q in pairs:
            z = z + dot_nt(gb[uid(dev, q)], a_v[s, rows_of(dev, q)])
        e = z.astype(BF16)
        e2own[:, s] = e
        gz = dot_tn(e, w2b[...])
        hb[rows_of(me, m), :] = jnp.where(acc1[s, :] > 0.0, gz, 0.0).astype(BF16)
        gh.start_own(m)

    phase(gg, lambda pairs: add_cols(acc2, pairs, lambda j: gb[uid(*pairs[j])]), zero2, finish3,
          lambda pre, i: None, False)

    total_rows = w2acc.shape[0]
    half_rows = total_rows // 2
    piece = half_rows // 8
    chips = DEVICES // 2
    chip = me // 2

    def w2rows(start, n):
        return pl.ds(pl.multiple_of(start, 8), n)

    mine = w2rows(core * half_rows, half_rows)

    def w2_sib():
        out = w2acc.at[w2rows((1 - core) * half_rows, half_rows)]
        return remote(out, w2rcv, w2s_sem.at[0], w2r_sem.at[0], sib)

    def w2_scatter(j):
        to = (chip + j) % chips
        out = w2acc.at[w2rows(core * half_rows + to * piece, piece)]
        return remote(out, w2part.at[j], w2s_sem.at[j], w2r_sem.at[j], to * 2 + core)

    def w2_gather(j, frm):
        to = (chip + j) % chips
        out = w2f.at[w2rows(core * half_rows + frm * piece, piece)]
        return remote(out, out, w2s_sem.at[chips + j], w2r_sem.at[chips + j], to * 2 + core)

    def w2_sib_gather(c):
        out = w2f.at[w2rows(c * half_rows, half_rows)]
        return remote(out, out, w2s_sem.at[chips], w2r_sem.at[chips], sib)

    def hook4(pre, i):
        if i is None:
            w2acc[...] = jnp.zeros_like(w2acc)
            w2acc[:cpad, :] = dot(e2own[...], hown[...])
            w2acc[total_rows - 1:, :LANES] = loss_acc[...]
            return

        @pl.when(i == 0)
        def _():
            w2_sib().start()

        @pl.when(i == 1)
        def _():
            w2_sib().wait_recv()
            w2acc[mine, :] = w2acc[mine, :] + w2rcv[...]

        @pl.when(i == 2)
        def _():
            w2_sib().wait_send()
            for j in range(1, chips):
                w2_scatter(j).start()

        @pl.when(i == 8)
        def _():
            own = w2rows(core * half_rows + chip * piece, piece)
            total = w2acc[own, :]
            for j in range(1, chips):
                w2_scatter(j).wait_recv()
            for j in range(1, chips):
                total = total + w2part[j]
            w2f[own, :] = total
            for j in range(1, chips):
                w2_scatter(j).wait_send()

        @pl.when(i == 9)
        def _():
            for j in range(1, chips):
                w2_gather(j, chip).start()

    def finish4(m, pairs):
        s = mrows(m)
        z = acc1[s, :]
        for dev, q in pairs:
            z = z + dot(a_v[s, rows_of(dev, q)], hb[rows_of(dev, q), :])
        part = dot_tn(x_ref[s, :], z.astype(BF16))
        w1p[...] = w1p[...] + part

    w1p[...] = jnp.zeros_like(w1p)
    phase(gh, lambda pairs: add_rows(acc1, pairs, lambda j: hb[rows_of(*pairs[j]), :]), zero1, finish4, hook4, False)

    sl = fin // DEVICES

    def w1rows(dev):
        return pl.ds(pl.multiple_of(dev * sl, sl), sl)

    def w1_scatter(i):
        dev = (me + i) % DEVICES
        return remote(w1p.at[w1rows(dev)], w1r.at[i], w1s_sem.at[i], w1r_sem.at[i], dev)

    def w1_gather(i):
        dev = (me + i) % DEVICES
        return remote(w1f.at[w1rows(me)], w1f.at[w1rows(me)], w1gs_sem.at[i], w1gr_sem.at[i], dev)

    def w1_gather_in(i):
        dev = (me + DEVICES - i) % DEVICES
        return remote(w1f.at[w1rows(dev)], w1f.at[w1rows(dev)], w1gs_sem.at[i], w1gr_sem.at[i], dev)

    for i in range(1, DEVICES):
        w1_scatter(i).start()
    total = w1p[w1rows(me), :]
    for j in range(1, chips):
        w2_gather(j, (chip + chips - j) % chips).wait_recv()
    w2_sib_gather(core).start()
    for j in range(1, chips):
        w2_gather(j, chip).wait_send()
    for i in range(1, DEVICES):
        w1_scatter(i).wait_recv()
    for i in range(1, DEVICES):
        total = total + w1r[i]
    w1f[w1rows(me), :] = total
    for i in range(1, DEVICES):
        w1_scatter(i).wait_send()
    for i in range(1, DEVICES):
        w1_gather(i).start()
    w2_sib_gather(1 - core).wait_recv()
    w2_sib_gather(core).wait_send()
    g2_out[...] = w2f[:classes, :]
    loss_out[0, 0] = jnp.sum(w2f[total_rows - 1:, :LANES] / cnt[0:1, :])
    for i in range(1, DEVICES):
        w1_gather_in(i).wait_recv()
    g1_out[...] = w1f[...]
    for i in range(1, DEVICES):
        w1_gather(i).wait_send()


def solution(mesh):
    axis = mesh.axis_names[0]

    def local_step(adj, x, w1, w2, labels, mask):
        rows, nodes = adj.shape
        fin, hid = w1.shape
        classes = w2.shape[1]
        unit = rows // UNITS
        cpad = -(-classes // 16) * 16
        total_rows = -(-(cpad + 1) // LANES) * LANES
        dma = pltpu.SemaphoreType.DMA
        vm = pl.BlockSpec(memory_space=pltpu.VMEM)
        loss, g1, g2 = pl.pallas_call(
            functools.partial(step_kernel, classes),
            out_shape=(jax.ShapeDtypeStruct((1, 1), F32),
                       jax.ShapeDtypeStruct((fin, hid), F32),
                       jax.ShapeDtypeStruct((classes, hid), F32)),
            in_specs=[pl.BlockSpec(memory_space=pl.ANY)] * 6,
            out_specs=(pl.BlockSpec(memory_space=pltpu.SMEM), vm, vm),
            scratch_shapes=[
                pltpu.VMEM((rows, fin), BF16),
                pltpu.VMEM((fin, hid), F32),
                pltpu.VMEM((classes, hid), F32),
                pltpu.VMEM((rows // LANES, LANES), jnp.int32),
                pltpu.VMEM((rows // LANES, LANES), jnp.int32),
                dma((UNITS + 5,)),
                pltpu.VMEM((rows, nodes), BF16),
                pltpu.VMEM((nodes // unit, cpad, unit), BF16),
                pltpu.VMEM((nodes, hid), BF16),
                pltpu.VMEM((rows, hid), F32),
                pltpu.VMEM((cpad, rows), F32),
                pltpu.VMEM((UNITS, unit, hid), BF16),
                pltpu.VMEM((UNITS, cpad, unit), BF16),
                pltpu.VMEM((rows, hid), BF16),
                pltpu.VMEM((cpad, rows), BF16),
                pltpu.VMEM((fin, hid), BF16),
                pltpu.VMEM((cpad, hid), BF16),
                pltpu.VMEM((total_rows, hid), F32),
                pltpu.VMEM((total_rows // 2, hid), F32),
                pltpu.VMEM((8, total_rows // 16, hid), F32),
                pltpu.VMEM((total_rows, hid), F32),
                pltpu.VMEM((fin, hid), F32),
                pltpu.VMEM((DEVICES, fin // DEVICES, hid), F32),
                pltpu.VMEM((fin, hid), F32),
                pltpu.VMEM((8, LANES), F32),
                pltpu.VMEM((DEVICES, 8, LANES), F32),
                pltpu.VMEM((8, LANES), F32),
                pltpu.VMEM((1, LANES), F32),
                dma((DEVICES,)),
                dma((2, 30)), dma((2, 30)), dma((2, 32)), dma((2, 32)),
                dma((DEVICES,)), dma((DEVICES,)), dma((DEVICES,)), dma((DEVICES,)),
                dma((DEVICES,)), dma((DEVICES,)), dma((DEVICES,)), dma((DEVICES,)),
            ],
            compiler_params=pltpu.CompilerParams(collective_id=0, has_side_effects=True,
                                                 vmem_limit_bytes=67043328),
            name="gcn_step",
        )(adj, x, w1, w2.T, labels.reshape(rows // LANES, LANES), mask.reshape(rows // LANES, LANES))
        return loss[0, 0], g1, g2.T

    return jax.shard_map(local_step, mesh=mesh,
                         in_specs=(P(axis, None), P(axis, None), P(None, None), P(None, None), P(axis), P(axis)),
                         out_specs=(P(), P(None, None), P(None, None)), check_vma=False)
```

```python
import functools

import jax
import jax.numpy as jnp
from jax import lax
from jax.experimental import pallas as pl
from jax.experimental.pallas import tpu as pltpu
from jax.sharding import PartitionSpec as P

F32 = jnp.float32
BF16 = jnp.bfloat16
MESH = pl.DeviceIdType.MESH
DEVICES = 16
UNITS = 4
LANES = 128
CHUNK = 1024


def dot(a, b):
    return jnp.dot(a, b, preferred_element_type=F32)


def dot_tn(a, b):
    return lax.dot_general(a, b, (((0,), (0,)), ((), ())), preferred_element_type=F32)


def dot_nt(a, b):
    return lax.dot_general(a, b, (((1,), (1,)), ((), ())), preferred_element_type=F32)


def loop(n, fn):
    lax.fori_loop(0, n, lambda i, c: (fn(i), c)[1], 0)


def step_kernel(classes, adj, x_hbm, w1_hbm, w2_hbm, lab_hbm, msk_hbm,
                loss_out, g1_out, g2_out,
                x_ref, w1_ref, w2_ref, lab_ref, msk_ref, in_sem,
                a_v, gb, hb, acc1, acc2, ys1, ys2, hown, e2own, w1b, w2b,
                w2acc, w2rcv, w2part, w2f, w1p, w1r, w1f, cnt_own, cnt_rcv, cnt, loss_acc,
                a_sem, rsem, ssem, sib_rsem, sib_ssem, cs_sem, cr_sem,
                w2s_sem, w2r_sem, w1s_sem, w1r_sem, w1gs_sem, w1gr_sem):
    rows = x_ref.shape[0]
    fin = x_ref.shape[1]
    unit = rows // UNITS
    hid = w1_ref.shape[1]
    cpad = w2b.shape[0]
    me = lax.axis_index("nodes")
    core = me % 2
    sib = me + 1 - 2 * core
    bit = [(me // v) % 2 for v in (2, 4, 8)]
    step = [v * (1 - 2 * b) for v, b in zip((2, 4, 8), bit)]
    own_d = [(1 - core) * step[r] + core * step[(r + 1) % 3] for r in range(3)]
    sib_d = [core * step[r] + (1 - core) * step[(r + 1) % 3] for r in range(3)]
    role_bit = [(1 - core) * bit[r] + core * bit[(r + 1) % 3] for r in range(3)]
    nbr = [me + d for d in own_d]

    def src_dev(base, deltas, hop, r):
        return base + deltas[r] + hop * deltas[(r + 2) % 3]

    anti = me + own_d[0] + own_d[1] + own_d[2]
    anti_sib = anti + 1 - 2 * core

    def remote(src, dst, ss, rs, dev):
        return pltpu.make_async_remote_copy(src_ref=src, dst_ref=dst, send_sem=ss, recv_sem=rs,
                                            device_id=(dev,), device_id_type=MESH)

    barrier = pltpu.get_barrier_semaphore()
    for dev in [sib] + nbr:
        pl.semaphore_signal(barrier, inc=1, device_id=(dev,), device_id_type=MESH)

    def uid(dev, q):
        return dev * UNITS + q

    order = [me, sib]
    for hop in (0, 1):
        order += [src_dev(me, own_d, hop, r) for r in range(3)]
        order += [src_dev(sib, sib_d, hop, r) for r in range(3)]
    order += [anti, anti_sib]

    def a_cols(dev):
        return pl.ds(pl.multiple_of(dev * rows, rows), rows)

    def a_copy(i):
        return pltpu.make_async_copy(adj.at[:, a_cols(order[i])], a_v.at[:, a_cols(order[i])], a_sem.at[i])

    x_units = [pltpu.make_async_copy(x_hbm.at[pl.ds(q * unit, unit)], gb.at[uid(me, q), pl.ds(0, unit), pl.ds(0, fin)],
                                     in_sem.at[q]) for q in range(UNITS)]
    inputs = [pltpu.make_async_copy(src, dst, in_sem.at[UNITS + i]) for i, (src, dst) in enumerate(
        [(w1_hbm, w1_ref), (w2_hbm, w2_ref), (msk_hbm, msk_ref), (lab_hbm, lab_ref), (x_hbm, x_ref)])]
    for c in x_units + inputs:
        c.start()
    for i in range(2):
        a_copy(i).start()

    def rows_of(dev, q):
        return pl.ds(pl.multiple_of(dev * rows + q * unit, unit), unit)

    pl.semaphore_wait(barrier, 4)

    def pick(f, vals):
        return jnp.where(f == 0, vals[0], jnp.where(f == 1, vals[1], vals[2]))

    class Gather:
        def __init__(self, view, height, par, sib_view=None):
            self.view, self.height, self.par = view, height, par
            self.shared, self.sib_view = sib_view is not None, sib_view or view

        def hop_copy(self, dev, q, to, sslot, rslot):
            v = self.view(dev, q)
            return remote(v, v, ssem.at[self.par, sslot], rsem.at[self.par, rslot], to)

        def sib_copy(self, dev, q, slot, src=None):
            v = self.sib_view(dev, q)
            return remote(v if src is None else src, v, sib_ssem.at[self.par, slot], sib_rsem.at[self.par, slot], sib)

        def own_copies(self, q):
            hops = [self.hop_copy(me, q, nbr[r], r * 4 + q, r * 4 + q) for r in range(3)]
            return hops if self.shared else hops + [self.sib_copy(me, q, 28 + q)]

        def start_own(self, q):
            for c in self.own_copies(q):
                c.start()

        def forward(self, q):
            return [self.hop_copy(src_dev(me, own_d, 0, r), q, nbr[(r + 1) % 3], 12 + r * 4 + q,
                                  12 + ((r + 1) % 3) * 4 + q) for r in range(3)]

        def last_forward(self, q):
            to = q % 3
            dev = pick((to + 2) % 3, [src_dev(me, own_d, 1, r) for r in range(3)])
            return self.hop_copy(dev, q, pick(to, nbr), 24 + q, 24 + q)

        def thirds(self, dev):
            tiles = self.height // 16
            at = [0, tiles // 3 * 16, 2 * (tiles // 3) * 16, self.height]
            return [self.view(dev, 3).at[pl.ds(at[t], at[t + 1] - at[t])] for t in range(3)]

        def third_copy(self, t):
            v = self.thirds(src_dev(me, own_d, 1, (t + 2) % 3))[t]
            return remote(v, v, ssem.at[self.par, 27 + t], rsem.at[self.par, 27 + t], nbr[t])

        def third_in(self, t):
            v = self.thirds(anti)[t]
            return remote(v, v, ssem.at[self.par, 27 + t], rsem.at[self.par, 27 + t], nbr[t])

        def arrive(self, hop, q):
            for r in range(3):
                d = src_dev(me, own_d, hop, r)
                self.hop_copy(d, q, nbr[r], r * 4 + q, hop * 12 + r * 4 + q).wait_recv()

            @pl.when(hop == 0)
            def _():
                for c in self.forward(q):
                    c.start()

            @pl.when((hop == 1) & (q < 3))
            def _():
                self.last_forward(q).start()

            @pl.when((hop == 1) & (q == 3))
            def _():
                for t in range(3):
                    self.third_copy(t).start()
            if not self.shared:
                for r in range(3):
                    self.sib_copy(src_dev(me, own_d, hop, r), q, hop * 12 + r * 4 + q).start()

        def arrive_last(self, q):
            if q < 3:
                self.hop_copy(anti, q, nbr[0], 24 + q, 24 + q).wait_recv()
            else:
                for t in range(3):
                    self.third_in(t).wait_recv()
            if not self.shared:
                self.sib_copy(anti, q, 24 + q).start()

        def sib_wait(self, hop, q):
            for r in range(3):
                self.sib_copy(src_dev(sib, sib_d, hop, r), q, hop * 12 + r * 4 + q).wait_recv()

        def sib_wait_own(self, q):
            self.sib_copy(sib, q, 28 + q).wait_recv()

        def sib_wait_last(self, q):
            self.sib_copy(anti_sib, q, 24 + q).wait_recv()

        def wait_sends(self):
            def body(q):
                for c in self.own_copies(q) + self.forward(q):
                    c.wait_send()
                if not self.shared:
                    for slot in (q, 4 + q, 8 + q, 12 + q, 16 + q, 20 + q, 24 + q):
                        self.sib_copy(me, q, slot).wait_send()
            loop(UNITS, body)
            if self.shared:
                for slot in (15, 19, 23, 24, 25, 26, 27, 28, 29, 30, 31):
                    self.sib_copy(me, 0, slot).wait_send()
            for q in range(3):
                self.last_forward(q).wait_send()
            for t in range(3):
                self.third_copy(t).wait_send()

    def phase(g, add, zero, finish, hook, first):
        def a_wait(lo, hi):
            if first:
                for i in range(lo, hi):
                    a_copy(i).wait()

        zero()

        def halves(fn):
            if g.shared:
                fn(0)
                fn(1)
            else:
                loop(2, fn)

        def near(t):
            if first and t == 0:
                a_wait(0, 1)

            def wait_sib():
                for q in range(UNITS):
                    g.sib_wait_own(q)
                a_wait(1, 2)
            if not g.shared:
                pl.when(t == 1)(wait_sib)
            elif t == 1:
                wait_sib()
            dev = me + t * (sib - me)
            add([(dev, q) for q in range(UNITS)], t, -1)
        halves(near)
        hook(-1, None)

        def group(i):
            @pl.when(i < 8)
            def _():
                g.arrive(i // 4, i % 4)

            @pl.when(i == 8)
            def _():
                for j in range(3):
                    g.arrive_last(j)

            @pl.when(i == 9)
            def _():
                g.arrive_last(3)
            hook(None, i)

            def half(t):
                k = i - t
                hop, q, far = (k // 4) % 2, k % 4, k // 8

                @pl.when((k >= 0) & (k <= 8))
                def _():
                    def on_sib(cond, fn):
                        if not g.shared:
                            pl.when((t == 1) & cond)(fn)
                        elif t == 1:
                            pl.when(cond)(fn)

                    on_sib(k < 8, lambda: g.sib_wait(hop, q))
                    on_sib(k == 8, lambda: [g.sib_wait_last(j) for j in range(3)] and None)
                    if first:
                        for key, (lo, hi) in {(0, 0): (2, 5), (0, 1): (5, 8), (4, 0): (8, 11), (4, 1): (11, 14),
                                              (8, 0): (14, 15), (8, 1): (15, 16)}.items():
                            if t == key[1]:
                                @pl.when(k == key[0])
                                def _(lo=lo, hi=hi):
                                    a_wait(lo, hi)
                    pairs = []
                    for r in range(3):
                        o, s = src_dev(me, own_d, hop, r), src_dev(sib, sib_d, hop, r)
                        near_dev = o + t * (s - o)
                        far_dev = anti + t * (anti_sib - anti)
                        pairs.append((near_dev + far * (far_dev - near_dev), q + far * (r - q)))
                    add(pairs, t, k)
            halves(half)
        loop(10, group)
        add([(anti, 3)], 0, 9)
        g.sib_wait_last(3)

        def last(m):
            @pl.when(m == UNITS - 1)
            def _():
                g.wait_sends()
            finish(m, [(anti_sib, 3)])
        loop(UNITS, last)

    gx = Gather(lambda dev, q: gb.at[uid(dev, q), pl.ds(0, unit), pl.ds(0, fin)], unit, 0,
                lambda dev, q: gb.at[uid(dev, q), pl.ds(0, unit), pl.ds(0, hid)])
    gh = Gather(lambda dev, q: hb.at[rows_of(dev, q)], unit, 1)
    gg = Gather(lambda dev, q: gb.at[uid(dev, q)], cpad, 0)

    def mrows(m):
        return pl.ds(pl.multiple_of(m * unit, unit), unit)

    def chunk(c):
        return pl.ds(pl.multiple_of(c * CHUNK, CHUNK), CHUNK)

    for q in range(UNITS):
        x_units[q].wait()
        gx.start_own(q)
    for i in range(2, 8):
        a_copy(i).start()
    for c in inputs:
        c.wait()
    w1b[...] = w1_ref[...].astype(BF16)
    w2acc[...] = jnp.zeros_like(w2acc)
    w2acc[:classes, :] = w2_ref[...]
    w2b[...] = w2acc[:cpad, :].astype(BF16)

    def cnt_copy(i):
        return remote(cnt_own, cnt_rcv.at[i], cs_sem.at[i], cr_sem.at[i], (me + i) % DEVICES)

    local = jnp.sum(msk_ref[...].astype(F32), axis=1, keepdims=True)
    local = jnp.sum(local, axis=0, keepdims=True)
    cnt_own[...] = jnp.broadcast_to(local, (8, LANES))

    def hook1(pre, i):
        if i is None:
            for j in range(8, DEVICES):
                a_copy(j).start()

    def zero1():
        acc1[...] = jnp.zeros_like(acc1)

    def add_rows(acc, pairs, operand):
        def body(c):
            s = chunk(c)
            v = acc[s, :]
            for j, (dev, q) in enumerate(pairs):
                v = v + dot(a_v[s, rows_of(dev, q)], operand(j))
            acc[s, :] = v
        loop(rows // CHUNK, body)

    def add1(pairs, t, k):
        if t == 1:
            add_rows(acc1, pairs, lambda j: gb[uid(*pairs[j]), :unit, :hid])
            return
        n = len(pairs)
        if isinstance(k, int):
            at = 0 if k < 0 else 10
            slots = [28 + j for j in range(n)] if k < 0 else [27]
        else:
            hop, q, far = (k // 4) % 2, k % 4, k // 8
            at = UNITS + 3 * (k % 2)
            slots = [hop * 12 + r * 4 + q + far * (24 + r - hop * 12 - r * 4 - q) for r in range(3)]

            @pl.when(k >= 2)
            def _():
                back = k - 2
                for r in range(3):
                    gx.sib_copy(me, 0, (back // 4) * 12 + r * 4 + back % 4).wait_send()
        for j, (dev, q) in enumerate(pairs):
            ys1[at + j] = dot(gb[uid(dev, q), :unit, :fin], w1b[...]).astype(BF16)

        def send():
            for j, (dev, q) in enumerate(pairs):
                gx.sib_copy(dev, q, slots[j], ys1.at[at + j]).start()
        if isinstance(k, int):
            send()
        add_rows(acc1, pairs, lambda j: ys1[at + j])
        if not isinstance(k, int):
            send()

    def finish1(m, pairs):
        s = mrows(m)
        z = acc1[s, :]
        for dev, q in pairs:
            z = z + dot(a_v[s, rows_of(dev, q)], gb[uid(dev, q), :unit, :hid])
        acc1[s, :] = z
        h = jnp.maximum(z, 0.0).astype(BF16)
        hb[rows_of(me, m), :] = h
        hown[s, :] = h
        gh.start_own(m)

    phase(gx, add1, zero1, finish1, hook1, True)

    def zero2():
        acc2[...] = jnp.zeros_like(acc2)

    def y2(dev, q):
        return dot_nt(w2b[...], hb[rows_of(dev, q), :]).astype(BF16)

    def add_cols(acc, pairs, operand):
        def body(c):
            s = chunk(c)
            v = acc[:, s]
            for j, (dev, q) in enumerate(pairs):
                v = v + dot_nt(operand(j), a_v[s, rows_of(dev, q)])
            acc[:, s] = v
        loop(rows // CHUNK, body)

    def add2(pairs, t, k):
        for j, (dev, q) in enumerate(pairs):
            ys2[j] = y2(dev, q)
        add_cols(acc2, pairs, lambda j: ys2[j])

    loss_acc[...] = jnp.zeros_like(loss_acc)

    def hook2(pre, i):
        if i is None:
            for j in range(1, DEVICES):
                cnt_copy(j).start()
            return

        @pl.when(i == 9)
        def _():
            for j in range(1, DEVICES):
                cnt_copy(j).wait_recv()
            total = cnt_own[...]
            for j in range(1, DEVICES):
                total = total + cnt_rcv[j]
            cnt[...] = total
            for j in range(1, DEVICES):
                cnt_copy(j).wait_send()

    def finish2(m, pairs):
        s = mrows(m)

        @pl.when(m == 0)
        def _():
            for j, (dev, q) in enumerate(pairs):
                ys2[j] = y2(dev, q)
        z = acc2[:, s]
        for j, (dev, q) in enumerate(pairs):
            z = z + dot_nt(ys2[j], a_v[s, rows_of(dev, q)])
        acc2[:, s] = z
        for h in range(unit // LANES):
            at = pl.ds(pl.multiple_of(m * unit + h * LANES, LANES), LANES)
            zc = acc2[:, at]
            row = lax.broadcasted_iota(jnp.int32, (cpad, LANES), 0)
            zm = jnp.where(row < classes, zc, -jnp.inf)
            top = jnp.max(zm, axis=0, keepdims=True)
            log_norm = top + jnp.log(jnp.sum(jnp.exp(zm - top), axis=0, keepdims=True))
            which = m * (unit // LANES) + h
            hot = row == lab_ref[pl.ds(which, 1), :]
            mask = msk_ref[pl.ds(which, 1), :].astype(F32)
            picked = jnp.sum(jnp.where(hot, zc, 0.0), axis=0, keepdims=True)
            loss_acc[...] = loss_acc[...] + mask * (log_norm - picked)
            gr = (jnp.exp(zm - log_norm) - jnp.where(hot, 1.0, 0.0)) * (mask / cnt[0:1, :])
            gb[uid(me, m), :, h * LANES:(h + 1) * LANES] = gr.astype(BF16)
        gg.start_own(m)

    phase(gh, add2, zero2, finish2, hook2, False)

    def finish3(m, pairs):
        s = mrows(m)
        z = acc2[:, s]
        for dev, q in pairs:
            z = z + dot_nt(gb[uid(dev, q)], a_v[s, rows_of(dev, q)])
        e = z.astype(BF16)
        e2own[:, s] = e
        gz = dot_tn(e, w2b[...])
        hb[rows_of(me, m), :] = jnp.where(acc1[s, :] > 0.0, gz, 0.0).astype(BF16)
        gh.start_own(m)

    phase(gg, lambda pairs, t, k: add_cols(acc2, pairs, lambda j: gb[uid(*pairs[j])]), zero2, finish3,
          lambda pre, i: None, False)

    total_rows = w2acc.shape[0]
    half_rows = total_rows // 2
    piece = half_rows // 8
    chips = DEVICES // 2
    chip = me // 2

    def w2rows(start, n):
        return pl.ds(pl.multiple_of(start, 8), n)

    mine = w2rows(core * half_rows, half_rows)

    def w2_sib():
        out = w2acc.at[w2rows((1 - core) * half_rows, half_rows)]
        return remote(out, w2rcv, w2s_sem.at[0], w2r_sem.at[0], sib)

    def w2_scatter(j):
        to = (chip + j) % chips
        out = w2acc.at[w2rows(core * half_rows + to * piece, piece)]
        return remote(out, w2part.at[j], w2s_sem.at[j], w2r_sem.at[j], to * 2 + core)

    def w2_gather(j, frm):
        to = (chip + j) % chips
        out = w2f.at[w2rows(core * half_rows + frm * piece, piece)]
        return remote(out, out, w2s_sem.at[chips + j], w2r_sem.at[chips + j], to * 2 + core)

    def w2_sib_gather(c):
        out = w2f.at[w2rows(c * half_rows, half_rows)]
        return remote(out, out, w2s_sem.at[chips], w2r_sem.at[chips], sib)

    def hook4(pre, i):
        if i is None:
            w2acc[...] = jnp.zeros_like(w2acc)
            w2acc[:cpad, :] = dot(e2own[...], hown[...])
            w2acc[total_rows - 1:, :LANES] = loss_acc[...]
            return

        @pl.when(i == 0)
        def _():
            w2_sib().start()

        @pl.when(i == 1)
        def _():
            w2_sib().wait_recv()
            w2acc[mine, :] = w2acc[mine, :] + w2rcv[...]

        @pl.when(i == 9)
        def _():
            w2_sib().wait_send()
            for j in range(1, chips):
                w2_scatter(j).start()

    def finish4(m, pairs):
        s = mrows(m)
        z = acc1[s, :]
        for dev, q in pairs:
            z = z + dot(a_v[s, rows_of(dev, q)], hb[rows_of(dev, q), :])
        part = dot_tn(x_ref[s, :], z.astype(BF16))
        w1p[...] = w1p[...] + part

    w1p[...] = jnp.zeros_like(w1p)
    phase(gh, lambda pairs, t, k: add_rows(acc1, pairs, lambda j: hb[rows_of(*pairs[j]), :]), zero1, finish4, hook4, False)

    sl = fin // DEVICES

    def w1rows(dev):
        return pl.ds(pl.multiple_of(dev * sl, sl), sl)

    def w1_scatter(i):
        dev = (me + i) % DEVICES
        return remote(w1p.at[w1rows(dev)], w1r.at[i], w1s_sem.at[i], w1r_sem.at[i], dev)

    def w1_gather(i):
        dev = (me + i) % DEVICES
        return remote(w1f.at[w1rows(me)], w1f.at[w1rows(me)], w1gs_sem.at[i], w1gr_sem.at[i], dev)

    def w1_gather_in(i):
        dev = (me + DEVICES - i) % DEVICES
        return remote(w1f.at[w1rows(dev)], w1f.at[w1rows(dev)], w1gs_sem.at[i], w1gr_sem.at[i], dev)

    for i in range(1, DEVICES):
        w1_scatter(i).start()
    own = w2rows(core * half_rows + chip * piece, piece)
    total2 = w2acc[own, :]
    for j in range(1, chips):
        w2_scatter(j).wait_recv()
    for j in range(1, chips):
        total2 = total2 + w2part[j]
    w2f[own, :] = total2
    for j in range(1, chips):
        w2_scatter(j).wait_send()
    for j in range(1, chips):
        w2_gather(j, chip).start()
    total = w1p[w1rows(me), :]
    for i in range(1, DEVICES):
        w1_scatter(i).wait_recv()
    for i in range(1, DEVICES):
        total = total + w1r[i]
    w1f[w1rows(me), :] = total
    for i in range(1, DEVICES):
        w1_scatter(i).wait_send()
    for i in range(1, DEVICES):
        w1_gather(i).start()
    for j in range(1, chips):
        w2_gather(j, (chip + chips - j) % chips).wait_recv()
    w2_sib_gather(core).start()
    for j in range(1, chips):
        w2_gather(j, chip).wait_send()
    w2_sib_gather(1 - core).wait_recv()
    g2_out[...] = w2f[:classes, :]
    loss_out[0, 0] = jnp.sum(w2f[total_rows - 1:, :LANES] / cnt[0:1, :])
    for i in range(1, DEVICES):
        w1_gather_in(i).wait_recv()
    g1_out[...] = w1f[...]
    w2_sib_gather(core).wait_send()
    for i in range(1, DEVICES):
        w1_gather(i).wait_send()


def solution(mesh):
    axis = mesh.axis_names[0]

    def local_step(adj, x, w1, w2, labels, mask):
        rows, nodes = adj.shape
        fin, hid = w1.shape
        classes = w2.shape[1]
        unit = rows // UNITS
        cpad = -(-classes // 16) * 16
        total_rows = -(-(cpad + 1) // LANES) * LANES
        dma = pltpu.SemaphoreType.DMA
        vm = pl.BlockSpec(memory_space=pltpu.VMEM)
        loss, g1, g2 = pl.pallas_call(
            functools.partial(step_kernel, classes),
            out_shape=(jax.ShapeDtypeStruct((1, 1), F32),
                       jax.ShapeDtypeStruct((fin, hid), F32),
                       jax.ShapeDtypeStruct((classes, hid), F32)),
            in_specs=[pl.BlockSpec(memory_space=pl.ANY)] * 6,
            out_specs=(pl.BlockSpec(memory_space=pltpu.SMEM), vm, vm),
            scratch_shapes=[
                pltpu.VMEM((rows, fin), BF16),
                pltpu.VMEM((fin, hid), F32),
                pltpu.VMEM((classes, hid), F32),
                pltpu.VMEM((rows // LANES, LANES), jnp.int32),
                pltpu.VMEM((rows // LANES, LANES), jnp.int32),
                dma((UNITS + 5,)),
                pltpu.VMEM((rows, nodes), BF16),
                pltpu.VMEM((nodes // unit, cpad, unit), BF16),
                pltpu.VMEM((nodes, hid), BF16),
                pltpu.VMEM((rows, hid), F32),
                pltpu.VMEM((cpad, rows), F32),
                pltpu.VMEM((UNITS + 7, unit, hid), BF16),
                pltpu.VMEM((UNITS, cpad, unit), BF16),
                pltpu.VMEM((rows, hid), BF16),
                pltpu.VMEM((cpad, rows), BF16),
                pltpu.VMEM((fin, hid), BF16),
                pltpu.VMEM((cpad, hid), BF16),
                pltpu.VMEM((total_rows, hid), F32),
                pltpu.VMEM((total_rows // 2, hid), F32),
                pltpu.VMEM((8, total_rows // 16, hid), F32),
                pltpu.VMEM((total_rows, hid), F32),
                pltpu.VMEM((fin, hid), F32),
                pltpu.VMEM((DEVICES, fin // DEVICES, hid), F32),
                pltpu.VMEM((fin, hid), F32),
                pltpu.VMEM((8, LANES), F32),
                pltpu.VMEM((DEVICES, 8, LANES), F32),
                pltpu.VMEM((8, LANES), F32),
                pltpu.VMEM((1, LANES), F32),
                dma((DEVICES,)),
                dma((2, 30)), dma((2, 30)), dma((2, 32)), dma((2, 32)),
                dma((DEVICES,)), dma((DEVICES,)), dma((DEVICES,)), dma((DEVICES,)),
                dma((DEVICES,)), dma((DEVICES,)), dma((DEVICES,)), dma((DEVICES,)),
            ],
            compiler_params=pltpu.CompilerParams(collective_id=0, has_side_effects=True,
                                                 vmem_limit_bytes=67043328),
            name="gcn_step",
        )(adj, x, w1, w2.T, labels.reshape(rows // LANES, LANES), mask.reshape(rows // LANES, LANES))
        return loss[0, 0], g1, g2.T

    return jax.shard_map(local_step, mesh=mesh,
                         in_specs=(P(axis, None), P(axis, None), P(None, None), P(None, None), P(axis), P(axis)),
                         out_specs=(P(), P(None, None), P(None, None)), check_vma=False)
```

```python
import functools

import jax
import jax.numpy as jnp
from jax import lax
from jax.experimental import pallas as pl
from jax.experimental.pallas import tpu as pltpu
from jax.sharding import PartitionSpec as P

F32 = jnp.float32
BF16 = jnp.bfloat16
MESH = pl.DeviceIdType.MESH
DEVICES = 16
UNITS = 4
LANES = 128
CHUNK = 1024


def dot(a, b):
    return jnp.dot(a, b, preferred_element_type=F32)


def dot_tn(a, b):
    return lax.dot_general(a, b, (((0,), (0,)), ((), ())), preferred_element_type=F32)


def dot_nt(a, b):
    return lax.dot_general(a, b, (((1,), (1,)), ((), ())), preferred_element_type=F32)


def loop(n, fn):
    lax.fori_loop(0, n, lambda i, c: (fn(i), c)[1], 0)


def step_kernel(classes, adj, x_hbm, w1_hbm, w2_hbm, lab_hbm, msk_hbm,
                loss_out, g1_out, g2_out,
                x_ref, w1_ref, w2_ref, lab_ref, msk_ref, in_sem,
                a_v, gb, hb, acc1, acc2, ys1, ys2, hown, e2own, w1b, w2b,
                w2acc, w2rcv, w2part, w2f, w1p, w1r, w1f, cnt_src, cnt_rcv, loss_acc, xt,
                a_sem, rsem, ssem, sib_rsem, sib_ssem, cs_sem, cr_sem,
                w2s_sem, w2r_sem, w1s_sem, w1r_sem, w1gs_sem, w1gr_sem):
    rows = x_ref.shape[0]
    fin = x_ref.shape[1]
    unit = rows // UNITS
    hid = w1_ref.shape[1]
    cpad = w2b.shape[0]
    me = lax.axis_index("nodes")
    core = me % 2
    sib = me + 1 - 2 * core
    bit = [(me // v) % 2 for v in (2, 4, 8)]
    step = [v * (1 - 2 * b) for v, b in zip((2, 4, 8), bit)]
    own_d = [(1 - core) * step[r] + core * step[(r + 1) % 3] for r in range(3)]
    sib_d = [core * step[r] + (1 - core) * step[(r + 1) % 3] for r in range(3)]
    role_bit = [(1 - core) * bit[r] + core * bit[(r + 1) % 3] for r in range(3)]
    nbr = [me + d for d in own_d]

    def src_dev(base, deltas, hop, r):
        return base + deltas[r] + hop * deltas[(r + 2) % 3]

    anti = me + own_d[0] + own_d[1] + own_d[2]
    anti_sib = anti + 1 - 2 * core

    def remote(src, dst, ss, rs, dev):
        return pltpu.make_async_remote_copy(src_ref=src, dst_ref=dst, send_sem=ss, recv_sem=rs,
                                            device_id=(dev,), device_id_type=MESH)

    barrier = pltpu.get_barrier_semaphore()
    for dev in [sib] + nbr:
        pl.semaphore_signal(barrier, inc=1, device_id=(dev,), device_id_type=MESH)

    def uid(dev, q):
        return dev * UNITS + q

    order = [me, sib]
    for hop in (0, 1):
        order += [src_dev(me, own_d, hop, r) for r in range(3)]
        order += [src_dev(sib, sib_d, hop, r) for r in range(3)]
    order += [anti, anti_sib]

    def a_cols(dev):
        return pl.ds(pl.multiple_of(dev * rows, rows), rows)

    def a_copy(i):
        return pltpu.make_async_copy(adj.at[:, a_cols(order[i])], a_v.at[:, a_cols(order[i])], a_sem.at[i])

    x_units = [pltpu.make_async_copy(x_hbm.at[pl.ds(q * unit, unit)], gb.at[uid(me, q), pl.ds(0, unit), pl.ds(0, fin)],
                                     in_sem.at[q]) for q in range(UNITS)]
    inputs = [pltpu.make_async_copy(src, dst, in_sem.at[UNITS + i]) for i, (src, dst) in enumerate(
        [(w1_hbm, w1_ref), (w2_hbm, w2_ref), (msk_hbm, msk_ref), (lab_hbm, lab_ref), (x_hbm, x_ref)])]
    for c in x_units + inputs:
        c.start()
    for i in range(2):
        a_copy(i).start()

    def rows_of(dev, q):
        return pl.ds(pl.multiple_of(dev * rows + q * unit, unit), unit)

    pl.semaphore_wait(barrier, 4)

    def pick(f, vals):
        return jnp.where(f == 0, vals[0], jnp.where(f == 1, vals[1], vals[2]))

    class Gather:
        def __init__(self, view, height, par, sib_view=None):
            self.view, self.height, self.par = view, height, par
            self.shared, self.sib_view = sib_view is not None, sib_view or view

        def hop_copy(self, dev, q, to, sslot, rslot):
            v = self.view(dev, q)
            return remote(v, v, ssem.at[self.par, sslot], rsem.at[self.par, rslot], to)

        def sib_copy(self, dev, q, slot, src=None):
            v = self.sib_view(dev, q)
            return remote(v if src is None else src, v, sib_ssem.at[self.par, slot], sib_rsem.at[self.par, slot], sib)

        def own_copies(self, q):
            hops = [self.hop_copy(me, q, nbr[r], r * 4 + q, r * 4 + q) for r in range(3)]
            return hops if self.shared else hops + [self.sib_copy(me, q, 28 + q)]

        def start_own(self, q):
            for c in self.own_copies(q):
                c.start()

        def forward(self, q):
            return [self.hop_copy(src_dev(me, own_d, 0, r), q, nbr[(r + 1) % 3], 12 + r * 4 + q,
                                  12 + ((r + 1) % 3) * 4 + q) for r in range(3)]

        def last_forward(self, q):
            to = q % 3
            dev = pick((to + 2) % 3, [src_dev(me, own_d, 1, r) for r in range(3)])
            return self.hop_copy(dev, q, pick(to, nbr), 24 + q, 24 + q)

        def thirds(self, dev):
            tiles = self.height // 16
            at = [0, tiles // 3 * 16, 2 * (tiles // 3) * 16, self.height]
            return [self.view(dev, 3).at[pl.ds(at[t], at[t + 1] - at[t])] for t in range(3)]

        def third_copy(self, t):
            v = self.thirds(src_dev(me, own_d, 1, (t + 2) % 3))[t]
            return remote(v, v, ssem.at[self.par, 27 + t], rsem.at[self.par, 27 + t], nbr[t])

        def third_in(self, t):
            v = self.thirds(anti)[t]
            return remote(v, v, ssem.at[self.par, 27 + t], rsem.at[self.par, 27 + t], nbr[t])

        def arrive(self, hop, q):
            for r in range(3):
                d = src_dev(me, own_d, hop, r)
                self.hop_copy(d, q, nbr[r], r * 4 + q, hop * 12 + r * 4 + q).wait_recv()

            @pl.when(hop == 0)
            def _():
                for c in self.forward(q):
                    c.start()

            @pl.when((hop == 1) & (q < 3))
            def _():
                self.last_forward(q).start()

            @pl.when((hop == 1) & (q == 3))
            def _():
                for t in range(3):
                    self.third_copy(t).start()
            if not self.shared:
                for r in range(3):
                    self.sib_copy(src_dev(me, own_d, hop, r), q, hop * 12 + r * 4 + q).start()

        def arrive_last(self, q):
            if q < 3:
                self.hop_copy(anti, q, nbr[0], 24 + q, 24 + q).wait_recv()
            else:
                for t in range(3):
                    self.third_in(t).wait_recv()
            if not self.shared:
                self.sib_copy(anti, q, 24 + q).start()

        def sib_wait(self, hop, q):
            for r in range(3):
                self.sib_copy(src_dev(sib, sib_d, hop, r), q, hop * 12 + r * 4 + q).wait_recv()

        def sib_wait_own(self, q):
            self.sib_copy(sib, q, 28 + q).wait_recv()

        def sib_wait_last(self, q):
            self.sib_copy(anti_sib, q, 24 + q).wait_recv()

        def wait_sends(self):
            def body(q):
                for c in self.own_copies(q) + self.forward(q):
                    c.wait_send()
                if not self.shared:
                    for slot in (q, 4 + q, 8 + q, 12 + q, 16 + q, 20 + q, 24 + q):
                        self.sib_copy(me, q, slot).wait_send()
            loop(UNITS, body)
            if self.shared:
                for slot in (15, 19, 23, 24, 25, 26, 27, 28, 29, 30, 31):
                    self.sib_copy(me, 0, slot).wait_send()
            for q in range(3):
                self.last_forward(q).wait_send()
            for t in range(3):
                self.third_copy(t).wait_send()

    def phase(g, add, zero, finish, hook, first, whole=False):
        def a_wait(lo, hi):
            if first:
                for i in range(lo, hi):
                    a_copy(i).wait()

        zero()

        def halves(fn):
            if g.shared:
                fn(0)
                fn(1)
            else:
                loop(2, fn)

        def near(t):
            if first and t == 0:
                a_wait(0, 1)

            def wait_sib():
                for q in range(UNITS):
                    g.sib_wait_own(q)
                a_wait(1, 2)
            if not g.shared:
                pl.when(t == 1)(wait_sib)
            elif t == 1:
                wait_sib()
            dev = me + t * (sib - me)
            add([(dev, q) for q in range(UNITS)], t, -1)
        halves(near)
        hook(-1, None)

        def group(i):
            @pl.when(i < 8)
            def _():
                g.arrive(i // 4, i % 4)

            @pl.when(i == 8)
            def _():
                for j in range(3):
                    g.arrive_last(j)

            @pl.when(i == 9)
            def _():
                g.arrive_last(3)
            hook(None, i)

            def half(t):
                k = i - t
                hop, q, far = (k // 4) % 2, k % 4, k // 8

                @pl.when((k >= 0) & (k <= 8))
                def _():
                    def on_sib(cond, fn):
                        if not g.shared:
                            pl.when((t == 1) & cond)(fn)
                        elif t == 1:
                            pl.when(cond)(fn)

                    on_sib(k < 8, lambda: g.sib_wait(hop, q))
                    on_sib(k == 8, lambda: [g.sib_wait_last(j) for j in range(3)] and None)
                    if first:
                        for key, (lo, hi) in {(0, 0): (2, 5), (0, 1): (5, 8), (4, 0): (8, 11), (4, 1): (11, 14),
                                              (8, 0): (14, 15), (8, 1): (15, 16)}.items():
                            if t == key[1]:
                                @pl.when(k == key[0])
                                def _(lo=lo, hi=hi):
                                    a_wait(lo, hi)
                    pairs = []
                    for r in range(3):
                        o, s = src_dev(me, own_d, hop, r), src_dev(sib, sib_d, hop, r)
                        near_dev = o + t * (s - o)
                        far_dev = anti + t * (anti_sib - anti)
                        pairs.append((near_dev + far * (far_dev - near_dev), q + far * (r - q)))
                    add(pairs, t, k)
            halves(half)
        loop(10, group)
        add([(anti, 3)], 0, 9)
        g.sib_wait_last(3)

        if whole:
            finish(None, [(anti_sib, 3)])
            return

        def last(m):
            @pl.when(m == UNITS - 1)
            def _():
                g.wait_sends()
            finish(m, [(anti_sib, 3)])
        loop(UNITS, last)

    gx = Gather(lambda dev, q: gb.at[uid(dev, q), pl.ds(0, unit), pl.ds(0, fin)], unit, 0,
                lambda dev, q: gb.at[uid(dev, q), pl.ds(0, unit), pl.ds(0, hid)])
    gh = Gather(lambda dev, q: hb.at[rows_of(dev, q)], unit, 1)
    gg = Gather(lambda dev, q: gb.at[uid(dev, q)], cpad, 0)

    def mrows(m):
        return pl.ds(pl.multiple_of(m * unit, unit), unit)

    def chunk(c):
        return pl.ds(pl.multiple_of(c * CHUNK, CHUNK), CHUNK)

    for q in range(UNITS):
        x_units[q].wait()
        gx.start_own(q)
    for i in range(2, 8):
        a_copy(i).start()
    for c in inputs:
        c.wait()
    w1b[...] = w1_ref[...].astype(BF16)
    w2acc[...] = jnp.zeros_like(w2acc)
    w2acc[:classes, :] = w2_ref[...]
    w2b[...] = w2acc[:cpad, :].astype(BF16)

    partners = [sib] + nbr

    def cnt_copy(k):
        return remote(cnt_src.at[k], cnt_rcv.at[k], cs_sem.at[k], cr_sem.at[k], partners[k])

    def cnt_next(k):
        cnt_copy(k).wait_recv()
        cnt_src[k + 1] = cnt_src[k] + cnt_rcv[k]
        if k < 3:
            cnt_copy(k + 1).start()

    local = jnp.sum(msk_ref[...].astype(F32), axis=1, keepdims=True)
    local = jnp.sum(local, axis=0, keepdims=True)
    cnt_src[0] = jnp.broadcast_to(local, (8, LANES))

    def hook1(pre, i):
        if i is None:
            for j in range(8, DEVICES):
                a_copy(j).start()
            cnt_copy(0).start()
            return

        @pl.when(i == 1)
        def _():
            cnt_next(0)

        @pl.when(i == 9)
        def _():
            cnt_next(1)

    def zero1():
        acc1[...] = jnp.zeros_like(acc1)

    def add_rows(acc, pairs, operand):
        def body(c):
            s = chunk(c)
            v = acc[s, :]
            for j, (dev, q) in enumerate(pairs):
                v = v + dot(a_v[s, rows_of(dev, q)], operand(j))
            acc[s, :] = v
        loop(rows // CHUNK, body)

    def add1(pairs, t, k):
        if t == 1:
            add_rows(acc1, pairs, lambda j: gb[uid(*pairs[j]), :unit, :hid])
            return
        n = len(pairs)
        if isinstance(k, int):
            at = 0 if k < 0 else 10
            slots = [28 + j for j in range(n)] if k < 0 else [27]
        else:
            hop, q, far = (k // 4) % 2, k % 4, k // 8
            at = UNITS + 3 * (k % 2)
            slots = [hop * 12 + r * 4 + q + far * (24 + r - hop * 12 - r * 4 - q) for r in range(3)]

            @pl.when(k >= 2)
            def _():
                back = k - 2
                for r in range(3):
                    gx.sib_copy(me, 0, (back // 4) * 12 + r * 4 + back % 4).wait_send()
        for j, (dev, q) in enumerate(pairs):
            ys1[at + j] = dot(gb[uid(dev, q), :unit, :fin], w1b[...]).astype(BF16)

        def send():
            for j, (dev, q) in enumerate(pairs):
                gx.sib_copy(dev, q, slots[j], ys1.at[at + j]).start()
        if isinstance(k, int):
            send()
        add_rows(acc1, pairs, lambda j: ys1[at + j])
        if not isinstance(k, int):
            send()

    def finish1(m, pairs):
        s = mrows(m)
        z = acc1[s, :]
        for dev, q in pairs:
            z = z + dot(a_v[s, rows_of(dev, q)], gb[uid(dev, q), :unit, :hid])
        acc1[s, :] = z
        h = jnp.maximum(z, 0.0).astype(BF16)
        hb[rows_of(me, m), :] = h
        hown[s, :] = h
        gh.start_own(m)

    phase(gx, add1, zero1, finish1, hook1, True)

    def zero2():
        acc2[...] = jnp.zeros_like(acc2)

    def y2(dev, q):
        return dot_nt(w2b[...], hb[rows_of(dev, q), :]).astype(BF16)

    def add_cols(acc, pairs, operand):
        def body(c):
            s = chunk(c)
            v = acc[:, s]
            for j, (dev, q) in enumerate(pairs):
                v = v + dot_nt(operand(j), a_v[s, rows_of(dev, q)])
            acc[:, s] = v
        loop(rows // CHUNK, body)

    def add2(pairs, t, k):
        for j, (dev, q) in enumerate(pairs):
            ys2[j] = y2(dev, q)
        add_cols(acc2, pairs, lambda j: ys2[j])

    loss_acc[...] = jnp.zeros_like(loss_acc)

    def hook2(pre, i):
        if i is None:
            return

        @pl.when(i == 0)
        def _():
            cnt_next(2)

        @pl.when(i == 9)
        def _():
            cnt_next(3)
            for k in range(4):
                cnt_copy(k).wait_send()

    def finish2(m, pairs):
        s = mrows(m)

        @pl.when(m == 0)
        def _():
            for j, (dev, q) in enumerate(pairs):
                ys2[j] = y2(dev, q)
        z = acc2[:, s]
        for j, (dev, q) in enumerate(pairs):
            z = z + dot_nt(ys2[j], a_v[s, rows_of(dev, q)])
        acc2[:, s] = z
        for h in range(unit // LANES):
            at = pl.ds(pl.multiple_of(m * unit + h * LANES, LANES), LANES)
            zc = acc2[:, at]
            row = lax.broadcasted_iota(jnp.int32, (cpad, LANES), 0)
            zm = jnp.where(row < classes, zc, -jnp.inf)
            top = jnp.max(zm, axis=0, keepdims=True)
            log_norm = top + jnp.log(jnp.sum(jnp.exp(zm - top), axis=0, keepdims=True))
            which = m * (unit // LANES) + h
            hot = row == lab_ref[pl.ds(which, 1), :]
            mask = msk_ref[pl.ds(which, 1), :].astype(F32)
            picked = jnp.sum(jnp.where(hot, zc, 0.0), axis=0, keepdims=True)
            loss_acc[...] = loss_acc[...] + mask * (log_norm - picked)
            gr = (jnp.exp(zm - log_norm) - jnp.where(hot, 1.0, 0.0)) * (mask / cnt_src[4][0:1, :])
            gb[uid(me, m), :, h * LANES:(h + 1) * LANES] = gr.astype(BF16)
        gg.start_own(m)

    phase(gh, add2, zero2, finish2, hook2, False)

    def hook3(pre, i):
        if i is None:
            xt[...] = x_ref[...].T

    def finish3(m, pairs):
        s = mrows(m)
        z = acc2[:, s]
        for dev, q in pairs:
            z = z + dot_nt(gb[uid(dev, q)], a_v[s, rows_of(dev, q)])
        e = z.astype(BF16)
        e2own[:, s] = e
        gz = dot_tn(e, w2b[...])
        hb[rows_of(me, m), :] = jnp.where(acc1[s, :] > 0.0, gz, 0.0).astype(BF16)
        gh.start_own(m)

    phase(gg, lambda pairs, t, k: add_cols(acc2, pairs, lambda j: gb[uid(*pairs[j])]), zero2, finish3,
          hook3, False)

    total_rows = w2acc.shape[0]
    half_rows = total_rows // 2
    piece = half_rows // 8
    chips = DEVICES // 2
    chip = me // 2

    def w2rows(start, n):
        return pl.ds(pl.multiple_of(start, 8), n)

    mine = w2rows(core * half_rows, half_rows)

    def w2_sib():
        out = w2acc.at[w2rows((1 - core) * half_rows, half_rows)]
        return remote(out, w2rcv, w2s_sem.at[0], w2r_sem.at[0], sib)

    def w2_scatter(j):
        to = (chip + j) % chips
        out = w2acc.at[w2rows(core * half_rows + to * piece, piece)]
        return remote(out, w2part.at[j], w2s_sem.at[j], w2r_sem.at[j], to * 2 + core)

    def w2_gather(j, frm):
        to = (chip + j) % chips
        out = w2f.at[w2rows(core * half_rows + frm * piece, piece)]
        return remote(out, out, w2s_sem.at[chips + j], w2r_sem.at[chips + j], to * 2 + core)

    def w2_sib_gather(c):
        out = w2f.at[w2rows(c * half_rows, half_rows)]
        return remote(out, out, w2s_sem.at[chips], w2r_sem.at[chips], sib)

    def hook4(pre, i):
        if i is None:
            w2acc[...] = jnp.zeros_like(w2acc)
            w2acc[:cpad, :] = dot(e2own[...], hown[...])
            w2acc[total_rows - 1:, :LANES] = loss_acc[...]
            return

        @pl.when(i == 0)
        def _():
            w2_sib().start()

        @pl.when(i == 1)
        def _():
            w2_sib().wait_recv()
            w2acc[mine, :] = w2acc[mine, :] + w2rcv[...]

        @pl.when(i == 9)
        def _():
            w2_sib().wait_send()
            for j in range(1, chips):
                w2_scatter(j).start()

    def finish4(m, pairs):
        z = acc1[...]
        for dev, q in pairs:
            z = z + dot(a_v[:, rows_of(dev, q)], hb[rows_of(dev, q), :])
        w1p[...] = dot(xt[...], z.astype(BF16))

    phase(gh, lambda pairs, t, k: add_rows(acc1, pairs, lambda j: hb[rows_of(*pairs[j]), :]), zero1, finish4, hook4, False, True)

    sl = fin // DEVICES

    def w1rows(dev):
        return pl.ds(pl.multiple_of(dev * sl, sl), sl)

    def w1_scatter(i):
        dev = (me + i) % DEVICES
        return remote(w1p.at[w1rows(dev)], w1r.at[i], w1s_sem.at[i], w1r_sem.at[i], dev)

    def w1_gather(i):
        dev = (me + i) % DEVICES
        return remote(w1f.at[w1rows(me)], w1f.at[w1rows(me)], w1gs_sem.at[i], w1gr_sem.at[i], dev)

    def w1_gather_in(i):
        dev = (me + DEVICES - i) % DEVICES
        return remote(w1f.at[w1rows(dev)], w1f.at[w1rows(dev)], w1gs_sem.at[i], w1gr_sem.at[i], dev)

    for i in range(1, DEVICES):
        w1_scatter(i).start()
    gh.wait_sends()
    own = w2rows(core * half_rows + chip * piece, piece)
    total2 = w2acc[own, :]
    for j in range(1, chips):
        w2_scatter(j).wait_recv()
    for j in range(1, chips):
        total2 = total2 + w2part[j]
    w2f[own, :] = total2
    for j in range(1, chips):
        w2_scatter(j).wait_send()
    for j in range(1, chips):
        w2_gather(j, chip).start()
    total = w1p[w1rows(me), :]
    for i in range(1, DEVICES):
        w1_scatter(i).wait_recv()
    for i in range(1, DEVICES):
        total = total + w1r[i]
    w1f[w1rows(me), :] = total
    for i in range(1, DEVICES):
        w1_scatter(i).wait_send()
    for i in range(1, DEVICES):
        w1_gather(i).start()
    for j in range(1, chips):
        w2_gather(j, (chip + chips - j) % chips).wait_recv()
    w2_sib_gather(core).start()
    for j in range(1, chips):
        w2_gather(j, chip).wait_send()
    w2_sib_gather(1 - core).wait_recv()
    g2_out[...] = w2f[:classes, :]
    loss_out[0, 0] = jnp.sum(w2f[total_rows - 1:, :LANES] / cnt_src[4][0:1, :])
    for i in range(1, DEVICES):
        w1_gather_in(i).wait_recv()
    g1_out[...] = w1f[...]
    w2_sib_gather(core).wait_send()
    for i in range(1, DEVICES):
        w1_gather(i).wait_send()


def solution(mesh):
    axis = mesh.axis_names[0]

    def local_step(adj, x, w1, w2, labels, mask):
        rows, nodes = adj.shape
        fin, hid = w1.shape
        classes = w2.shape[1]
        unit = rows // UNITS
        cpad = -(-classes // 16) * 16
        total_rows = -(-(cpad + 1) // LANES) * LANES
        dma = pltpu.SemaphoreType.DMA
        vm = pl.BlockSpec(memory_space=pltpu.VMEM)
        loss, g1, g2 = pl.pallas_call(
            functools.partial(step_kernel, classes),
            out_shape=(jax.ShapeDtypeStruct((1, 1), F32),
                       jax.ShapeDtypeStruct((fin, hid), F32),
                       jax.ShapeDtypeStruct((classes, hid), F32)),
            in_specs=[pl.BlockSpec(memory_space=pl.ANY)] * 6,
            out_specs=(pl.BlockSpec(memory_space=pltpu.SMEM), vm, vm),
            scratch_shapes=[
                pltpu.VMEM((rows, fin), BF16),
                pltpu.VMEM((fin, hid), F32),
                pltpu.VMEM((classes, hid), F32),
                pltpu.VMEM((rows // LANES, LANES), jnp.int32),
                pltpu.VMEM((rows // LANES, LANES), jnp.int32),
                dma((UNITS + 5,)),
                pltpu.VMEM((rows, nodes), BF16),
                pltpu.VMEM((nodes // unit, cpad, unit), BF16),
                pltpu.VMEM((nodes, hid), BF16),
                pltpu.VMEM((rows, hid), F32),
                pltpu.VMEM((cpad, rows), F32),
                pltpu.VMEM((UNITS + 7, unit, hid), BF16),
                pltpu.VMEM((UNITS, cpad, unit), BF16),
                pltpu.VMEM((rows, hid), BF16),
                pltpu.VMEM((cpad, rows), BF16),
                pltpu.VMEM((fin, hid), BF16),
                pltpu.VMEM((cpad, hid), BF16),
                pltpu.VMEM((total_rows, hid), F32),
                pltpu.VMEM((total_rows // 2, hid), F32),
                pltpu.VMEM((8, total_rows // 16, hid), F32),
                pltpu.VMEM((total_rows, hid), F32),
                pltpu.VMEM((fin, hid), F32),
                pltpu.VMEM((DEVICES, fin // DEVICES, hid), F32),
                pltpu.VMEM((fin, hid), F32),
                pltpu.VMEM((5, 8, LANES), F32),
                pltpu.VMEM((4, 8, LANES), F32),
                pltpu.VMEM((1, LANES), F32),
                pltpu.VMEM((fin, rows), BF16),
                dma((DEVICES,)),
                dma((2, 30)), dma((2, 30)), dma((2, 32)), dma((2, 32)),
                dma((DEVICES,)), dma((DEVICES,)), dma((DEVICES,)), dma((DEVICES,)),
                dma((DEVICES,)), dma((DEVICES,)), dma((DEVICES,)), dma((DEVICES,)),
            ],
            compiler_params=pltpu.CompilerParams(collective_id=0, has_side_effects=True,
                                                 vmem_limit_bytes=67043328),
            name="gcn_step",
        )(adj, x, w1, w2.T, labels.reshape(rows // LANES, LANES), mask.reshape(rows // LANES, LANES))
        return loss[0, 0], g1, g2.T

    return jax.shard_map(local_step, mesh=mesh,
                         in_specs=(P(axis, None), P(axis, None), P(None, None), P(None, None), P(axis), P(axis)),
                         out_specs=(P(), P(None, None), P(None, None)), check_vma=False)
```

```python
import functools

import jax
import jax.numpy as jnp
from jax import lax
from jax.experimental import pallas as pl
from jax.experimental.pallas import tpu as pltpu
from jax.sharding import PartitionSpec as P

F32 = jnp.float32
BF16 = jnp.bfloat16
MESH = pl.DeviceIdType.MESH
DEVICES = 16
UNITS = 4
LANES = 128
CHUNK = 1024


def dot(a, b):
    return jnp.dot(a, b, preferred_element_type=F32)


def dot_tn(a, b):
    return lax.dot_general(a, b, (((0,), (0,)), ((), ())), preferred_element_type=F32)


def dot_nt(a, b):
    return lax.dot_general(a, b, (((1,), (1,)), ((), ())), preferred_element_type=F32)


def loop(n, fn):
    lax.fori_loop(0, n, lambda i, c: (fn(i), c)[1], 0)


def step_kernel(classes, adj, x_hbm, w1_hbm, w2_hbm, lab_hbm, msk_hbm,
                loss_out, g1_out, g2_out,
                w1_ref, w2_ref, lab_ref, msk_ref, in_sem,
                a_v, gb, hb, acc1, acc2, ys, hown, w1b, w2b,
                w2acc, w2rcv, w2part, w2f, w1p, w1r, w1f, cnt_src, cnt_rcv, loss_acc, xt,
                a_sem, rsem, ssem, sib_rsem, sib_ssem, cs_sem, cr_sem,
                w2s_sem, w2r_sem, w1s_sem, w1r_sem, w1gs_sem, w1gr_sem):
    rows = x_hbm.shape[0]
    fin = x_hbm.shape[1]
    unit = rows // UNITS
    hid = w1_ref.shape[1]
    cpad = w2b.shape[0]
    me = lax.axis_index("nodes")
    core = me % 2
    sib = me + 1 - 2 * core
    bit = [(me // v) % 2 for v in (2, 4, 8)]
    step = [v * (1 - 2 * b) for v, b in zip((2, 4, 8), bit)]
    own_d = [(1 - core) * step[r] + core * step[(r + 1) % 3] for r in range(3)]
    sib_d = [core * step[r] + (1 - core) * step[(r + 1) % 3] for r in range(3)]
    role_bit = [(1 - core) * bit[r] + core * bit[(r + 1) % 3] for r in range(3)]
    nbr = [me + d for d in own_d]

    def src_dev(base, deltas, hop, r):
        return base + deltas[r] + hop * deltas[(r + 2) % 3]

    anti = me + own_d[0] + own_d[1] + own_d[2]
    anti_sib = anti + 1 - 2 * core

    def remote(src, dst, ss, rs, dev):
        return pltpu.make_async_remote_copy(src_ref=src, dst_ref=dst, send_sem=ss, recv_sem=rs,
                                            device_id=(dev,), device_id_type=MESH)

    barrier = pltpu.get_barrier_semaphore()
    for dev in [sib] + nbr:
        pl.semaphore_signal(barrier, inc=1, device_id=(dev,), device_id_type=MESH)

    def uid(dev, q):
        return dev * UNITS + q

    order = [me, sib]
    for hop in (0, 1):
        order += [src_dev(me, own_d, hop, r) for r in range(3)]
        order += [src_dev(sib, sib_d, hop, r) for r in range(3)]
    order += [anti, anti_sib]

    def a_cols(dev):
        return pl.ds(pl.multiple_of(dev * rows, rows), rows)

    def a_copy(i):
        return pltpu.make_async_copy(adj.at[:, a_cols(order[i])], a_v.at[:, a_cols(order[i])], a_sem.at[i])

    x_units = [pltpu.make_async_copy(x_hbm.at[pl.ds(q * unit, unit)], gb.at[uid(me, q), pl.ds(0, unit), pl.ds(0, fin)],
                                     in_sem.at[q]) for q in range(UNITS)]
    inputs = [pltpu.make_async_copy(src, dst, in_sem.at[UNITS + i]) for i, (src, dst) in enumerate(
        [(w1_hbm, w1_ref), (w2_hbm, w2_ref), (msk_hbm, msk_ref), (lab_hbm, lab_ref)])]
    for c in x_units + inputs:
        c.start()
    for i in range(2):
        a_copy(i).start()

    def rows_of(dev, q):
        return pl.ds(pl.multiple_of(dev * rows + q * unit, unit), unit)

    pl.semaphore_wait(barrier, 4)

    def pick(f, vals):
        return jnp.where(f == 0, vals[0], jnp.where(f == 1, vals[1], vals[2]))

    class Gather:
        def __init__(self, view, height, par, sib_view=None):
            self.view, self.height, self.par = view, height, par
            self.shared, self.sib_view = sib_view is not None, sib_view or view

        def hop_copy(self, dev, q, to, sslot, rslot):
            v = self.view(dev, q)
            return remote(v, v, ssem.at[self.par, sslot], rsem.at[self.par, rslot], to)

        def sib_copy(self, dev, q, slot, src=None):
            v = self.sib_view(dev, q)
            return remote(v if src is None else src, v, sib_ssem.at[self.par, slot], sib_rsem.at[self.par, slot], sib)

        def own_copies(self, q):
            hops = [self.hop_copy(me, q, nbr[r], r * 4 + q, r * 4 + q) for r in range(3)]
            return hops if self.shared else hops + [self.sib_copy(me, q, 28 + q)]

        def start_own(self, q):
            for c in self.own_copies(q):
                c.start()

        def forward(self, q):
            return [self.hop_copy(src_dev(me, own_d, 0, r), q, nbr[(r + 1) % 3], 12 + r * 4 + q,
                                  12 + ((r + 1) % 3) * 4 + q) for r in range(3)]

        def last_forward(self, q):
            to = q % 3
            dev = pick((to + 2) % 3, [src_dev(me, own_d, 1, r) for r in range(3)])
            return self.hop_copy(dev, q, pick(to, nbr), 24 + q, 24 + q)

        def thirds(self, dev):
            tiles = self.height // 16
            at = [0, tiles // 3 * 16, 2 * (tiles // 3) * 16, self.height]
            return [self.view(dev, 3).at[pl.ds(at[t], at[t + 1] - at[t])] for t in range(3)]

        def third_copy(self, t):
            v = self.thirds(src_dev(me, own_d, 1, (t + 2) % 3))[t]
            return remote(v, v, ssem.at[self.par, 27 + t], rsem.at[self.par, 27 + t], nbr[t])

        def third_in(self, t):
            v = self.thirds(anti)[t]
            return remote(v, v, ssem.at[self.par, 27 + t], rsem.at[self.par, 27 + t], nbr[t])

        def arrive(self, hop, q):
            for r in range(3):
                d = src_dev(me, own_d, hop, r)
                self.hop_copy(d, q, nbr[r], r * 4 + q, hop * 12 + r * 4 + q).wait_recv()

            @pl.when(hop == 0)
            def _():
                for c in self.forward(q):
                    c.start()

            @pl.when((hop == 1) & (q < 3))
            def _():
                self.last_forward(q).start()

            @pl.when((hop == 1) & (q == 3))
            def _():
                for t in range(3):
                    self.third_copy(t).start()
            if not self.shared:
                for r in range(3):
                    self.sib_copy(src_dev(me, own_d, hop, r), q, hop * 12 + r * 4 + q).start()

        def arrive_last(self, q):
            if q < 3:
                self.hop_copy(anti, q, nbr[0], 24 + q, 24 + q).wait_recv()
            else:
                for t in range(3):
                    self.third_in(t).wait_recv()
            if not self.shared:
                self.sib_copy(anti, q, 24 + q).start()

        def sib_wait(self, hop, q):
            for r in range(3):
                self.sib_copy(src_dev(sib, sib_d, hop, r), q, hop * 12 + r * 4 + q).wait_recv()

        def sib_wait_own(self, q):
            self.sib_copy(sib, q, 28 + q).wait_recv()

        def sib_wait_last(self, q):
            self.sib_copy(anti_sib, q, 24 + q).wait_recv()

        def wait_sends(self):
            def body(q):
                for c in self.own_copies(q) + self.forward(q):
                    c.wait_send()
                if not self.shared:
                    for slot in (q, 4 + q, 8 + q, 12 + q, 16 + q, 20 + q, 24 + q):
                        self.sib_copy(me, q, slot).wait_send()
            loop(UNITS, body)
            if self.shared:
                for slot in (15, 19, 23, 24, 25, 26, 27, 28, 29, 30, 31):
                    self.sib_copy(me, 0, slot).wait_send()
            for q in range(3):
                self.last_forward(q).wait_send()
            for t in range(3):
                self.third_copy(t).wait_send()

    def phase(g, add, zero, finish, hook, first, whole=False):
        def a_wait(lo, hi):
            if first:
                for i in range(lo, hi):
                    a_copy(i).wait()

        zero()

        def halves(fn):
            if g.shared:
                fn(0)
                fn(1)
            else:
                loop(2, fn)

        def near(t):
            if first and t == 0:
                a_wait(0, 1)

            def wait_sib():
                for q in range(UNITS):
                    g.sib_wait_own(q)
                a_wait(1, 2)
            if not g.shared:
                pl.when(t == 1)(wait_sib)
            elif t == 1:
                wait_sib()
            dev = me + t * (sib - me)
            add([(dev, q) for q in range(UNITS)], t, -1)
        halves(near)
        hook(-1, None)

        def group(i):
            @pl.when(i < 8)
            def _():
                g.arrive(i // 4, i % 4)

            @pl.when(i == 8)
            def _():
                for j in range(3):
                    g.arrive_last(j)

            if g.shared:
                @pl.when(i == 9)
                def _():
                    g.arrive_last(3)
            hook(None, i)

            def half(t):
                k = i - t if g.shared else i
                hop, q, far = (k // 4) % 2, k % 4, k // 8

                if not g.shared:
                    @pl.when((t == 1) & (i == 8))
                    def _():
                        g.arrive_last(3)
                        add([(anti, 3)], 0, 9)

                @pl.when((k >= 0) & (k <= 8))
                def _():
                    def on_sib(cond, fn):
                        if not g.shared:
                            pl.when((t == 1) & cond)(fn)
                        elif t == 1:
                            pl.when(cond)(fn)

                    on_sib(k < 8, lambda: g.sib_wait(hop, q))
                    on_sib(k == 8, lambda: [g.sib_wait_last(j) for j in range(3)] and None)
                    if first:
                        for key, (lo, hi) in {(0, 0): (2, 5), (0, 1): (5, 8), (4, 0): (8, 11), (4, 1): (11, 14),
                                              (8, 0): (14, 15), (8, 1): (15, 16)}.items():
                            if t == key[1]:
                                @pl.when(k == key[0])
                                def _(lo=lo, hi=hi):
                                    a_wait(lo, hi)
                    pairs = []
                    for r in range(3):
                        o, s = src_dev(me, own_d, hop, r), src_dev(sib, sib_d, hop, r)
                        near_dev = o + t * (s - o)
                        far_dev = anti + t * (anti_sib - anti)
                        pairs.append((near_dev + far * (far_dev - near_dev), q + far * (r - q)))
                    add(pairs, t, k)
            halves(half)
        if g.shared:
            loop(10, group)
            add([(anti, 3)], 0, 9)
        else:
            loop(9, group)
            hook(None, 9)
        g.sib_wait_last(3)

        if whole:
            finish(None, [(anti_sib, 3)])
            return

        def last(m):
            @pl.when(m == UNITS - 1)
            def _():
                g.wait_sends()
            finish(m, [(anti_sib, 3)])
        loop(UNITS, last)

    gx = Gather(lambda dev, q: gb.at[uid(dev, q), pl.ds(0, unit), pl.ds(0, fin)], unit, 0,
                lambda dev, q: gb.at[uid(dev, q), pl.ds(0, unit), pl.ds(0, hid)])
    gh = Gather(lambda dev, q: hb.at[rows_of(dev, q)], unit, 1)
    gg = Gather(lambda dev, q: gb.at[uid(dev, q)], cpad, 0)

    def mrows(m):
        return pl.ds(pl.multiple_of(m * unit, unit), unit)

    def chunk(c):
        return pl.ds(pl.multiple_of(c * CHUNK, CHUNK), CHUNK)

    for q in range(UNITS):
        x_units[q].wait()
        gx.start_own(q)
    for i in range(2, 8):
        a_copy(i).start()
    for c in inputs:
        c.wait()
    w1b[...] = w1_ref[...].astype(BF16)
    w2acc[...] = jnp.zeros_like(w2acc)
    w2acc[:classes, :] = w2_ref[...]
    w2b[...] = w2acc[:cpad, :].astype(BF16)

    partners = [sib] + nbr

    def cnt_copy(k):
        return remote(cnt_src.at[k], cnt_rcv.at[k], cs_sem.at[k], cr_sem.at[k], partners[k])

    def cnt_next(k):
        cnt_copy(k).wait_recv()
        cnt_src[k + 1] = cnt_src[k] + cnt_rcv[k]
        if k < 3:
            cnt_copy(k + 1).start()

    local = jnp.sum(msk_ref[...].astype(F32), axis=1, keepdims=True)
    local = jnp.sum(local, axis=0, keepdims=True)
    cnt_src[0] = jnp.broadcast_to(local, (8, LANES))

    def hook1(pre, i):
        if i is None:
            for j in range(8, DEVICES):
                a_copy(j).start()
            cnt_copy(0).start()
            return

        @pl.when(i == 1)
        def _():
            cnt_next(0)

        @pl.when(i == 9)
        def _():
            cnt_next(1)

    def zero1():
        acc1[...] = jnp.zeros_like(acc1)

    def add_rows(acc, pairs, operand):
        def body(c):
            s = chunk(c)
            v = acc[s, :]
            for j, (dev, q) in enumerate(pairs):
                v = v + dot(a_v[s, rows_of(dev, q)], operand(j))
            acc[s, :] = v
        loop(rows // CHUNK, body)

    def add1(pairs, t, k):
        if t == 1:
            add_rows(acc1, pairs, lambda j: gb[uid(*pairs[j]), :unit, :hid])
            return
        n = len(pairs)
        if isinstance(k, int):
            at = 0 if k < 0 else 10
            slots = [28 + j for j in range(n)] if k < 0 else [27]
        else:
            hop, q, far = (k // 4) % 2, k % 4, k // 8
            at = UNITS + 3 * (k % 2)
            slots = [hop * 12 + r * 4 + q + far * (24 + r - hop * 12 - r * 4 - q) for r in range(3)]

            @pl.when(k >= 2)
            def _():
                back = k - 2
                for r in range(3):
                    gx.sib_copy(me, 0, (back // 4) * 12 + r * 4 + back % 4).wait_send()
        for j, (dev, q) in enumerate(pairs):
            ys[at + j, :unit, :hid] = dot(gb[uid(dev, q), :unit, :fin], w1b[...]).astype(BF16)

        def send():
            for j, (dev, q) in enumerate(pairs):
                gx.sib_copy(dev, q, slots[j], ys.at[at + j, pl.ds(0, unit), pl.ds(0, hid)]).start()
        if isinstance(k, int):
            send()
        add_rows(acc1, pairs, lambda j: ys[at + j, :unit, :hid])
        if not isinstance(k, int):
            send()

    def finish1(m, pairs):
        s = mrows(m)
        z = acc1[s, :]
        for dev, q in pairs:
            z = z + dot(a_v[s, rows_of(dev, q)], gb[uid(dev, q), :unit, :hid])
        acc1[s, :] = z
        h = jnp.maximum(z, 0.0).astype(BF16)
        hb[rows_of(me, m), :] = h
        hown[s, :] = h
        gh.start_own(m)

    phase(gx, add1, zero1, finish1, hook1, True)

    def zero2():
        acc2[...] = jnp.zeros_like(acc2)

    def y2(dev, q):
        return dot_nt(w2b[...], hb[rows_of(dev, q), :]).astype(BF16)

    def add_cols(acc, pairs, operand):
        def body(c):
            s = chunk(c)
            v = acc[:, s]
            for j, (dev, q) in enumerate(pairs):
                v = v + dot_nt(operand(j), a_v[s, rows_of(dev, q)])
            acc[:, s] = v
        loop(rows // CHUNK, body)

    def add2(pairs, t, k):
        for j, (dev, q) in enumerate(pairs):
            ys[j] = y2(dev, q)
        add_cols(acc2, pairs, lambda j: ys[j])

    loss_acc[...] = jnp.zeros_like(loss_acc)

    def hook2(pre, i):
        if i is None:
            for q in range(UNITS):
                xt[:, q * unit:(q + 1) * unit] = gb[uid(me, q), :unit, :fin].T
            return

        @pl.when(i == 0)
        def _():
            cnt_next(2)

        @pl.when(i == 9)
        def _():
            cnt_next(3)
            for k in range(4):
                cnt_copy(k).wait_send()

    def finish2(m, pairs):
        s = mrows(m)

        @pl.when(m == 0)
        def _():
            for j, (dev, q) in enumerate(pairs):
                ys[j] = y2(dev, q)
        z = acc2[:, s]
        for j, (dev, q) in enumerate(pairs):
            z = z + dot_nt(ys[j], a_v[s, rows_of(dev, q)])
        acc2[:, s] = z
        for h in range(unit // LANES):
            at = pl.ds(pl.multiple_of(m * unit + h * LANES, LANES), LANES)
            zc = acc2[:, at]
            row = lax.broadcasted_iota(jnp.int32, (cpad, LANES), 0)
            zm = jnp.where(row < classes, zc, -jnp.inf)
            top = jnp.max(zm, axis=0, keepdims=True)
            log_norm = top + jnp.log(jnp.sum(jnp.exp(zm - top), axis=0, keepdims=True))
            which = m * (unit // LANES) + h
            hot = row == lab_ref[pl.ds(which, 1), :]
            mask = msk_ref[pl.ds(which, 1), :].astype(F32)
            picked = jnp.sum(jnp.where(hot, zc, 0.0), axis=0, keepdims=True)
            loss_acc[...] = loss_acc[...] + mask * (log_norm - picked)
            gr = (jnp.exp(zm - log_norm) - jnp.where(hot, 1.0, 0.0)) * (mask / cnt_src[4][0:1, :])
            gb[uid(me, m), :, h * LANES:(h + 1) * LANES] = gr.astype(BF16)
        gg.start_own(m)

    phase(gh, add2, zero2, finish2, hook2, False)

    def finish3(m, pairs):
        s = mrows(m)
        z = acc2[:, s]
        for dev, q in pairs:
            z = z + dot_nt(gb[uid(dev, q)], a_v[s, rows_of(dev, q)])
        e = z.astype(BF16)
        ys[m] = e
        gz = dot_tn(e, w2b[...])
        hb[rows_of(me, m), :] = jnp.where(acc1[s, :] > 0.0, gz, 0.0).astype(BF16)
        gh.start_own(m)

    phase(gg, lambda pairs, t, k: add_cols(acc2, pairs, lambda j: gb[uid(*pairs[j])]), zero2, finish3,
          lambda pre, i: None, False)

    total_rows = w2acc.shape[0]
    half_rows = total_rows // 2
    piece = half_rows // 8
    chips = DEVICES // 2
    chip = me // 2

    def w2rows(start, n):
        return pl.ds(pl.multiple_of(start, 8), n)

    mine = w2rows(core * half_rows, half_rows)

    def w2_sib():
        out = w2acc.at[w2rows((1 - core) * half_rows, half_rows)]
        return remote(out, w2rcv, w2s_sem.at[0], w2r_sem.at[0], sib)

    def w2_scatter(j):
        to = (chip + j) % chips
        out = w2acc.at[w2rows(core * half_rows + to * piece, piece)]
        return remote(out, w2part.at[j], w2s_sem.at[j], w2r_sem.at[j], to * 2 + core)

    def w2_gather(j, frm):
        to = (chip + j) % chips
        out = w2f.at[w2rows(core * half_rows + frm * piece, piece)]
        return remote(out, out, w2s_sem.at[chips + j], w2r_sem.at[chips + j], to * 2 + core)

    def w2_sib_gather(c):
        out = w2f.at[w2rows(c * half_rows, half_rows)]
        return remote(out, out, w2s_sem.at[chips], w2r_sem.at[chips], sib)

    def hook4(pre, i):
        if i is None:
            w2acc[...] = jnp.zeros_like(w2acc)
            w2acc[:cpad, :] = sum(dot(ys[q], hown[q * unit:(q + 1) * unit, :]) for q in range(UNITS))
            w2acc[total_rows - 1:, :LANES] = loss_acc[...]
            return

        @pl.when(i == 0)
        def _():
            w2_sib().start()

        @pl.when(i == 1)
        def _():
            w2_sib().wait_recv()
            w2acc[mine, :] = w2acc[mine, :] + w2rcv[...]

        @pl.when(i == 9)
        def _():
            w2_sib().wait_send()
            for j in range(1, chips):
                w2_scatter(j).start()

    def finish4(m, pairs):
        z = acc1[...]
        for dev, q in pairs:
            z = z + dot(a_v[:, rows_of(dev, q)], hb[rows_of(dev, q), :])
        w1p[...] = dot(xt[...], z.astype(BF16))

    phase(gh, lambda pairs, t, k: add_rows(acc1, pairs, lambda j: hb[rows_of(*pairs[j]), :]), zero1, finish4, hook4, False, True)

    sl = fin // DEVICES

    def w1rows(dev):
        return pl.ds(pl.multiple_of(dev * sl, sl), sl)

    def w1_scatter(i):
        dev = (me + i) % DEVICES
        return remote(w1p.at[w1rows(dev)], w1r.at[i], w1s_sem.at[i], w1r_sem.at[i], dev)

    def w1_gather(i):
        dev = (me + i) % DEVICES
        return remote(w1f.at[w1rows(me)], w1f.at[w1rows(me)], w1gs_sem.at[i], w1gr_sem.at[i], dev)

    def w1_gather_in(i):
        dev = (me + DEVICES - i) % DEVICES
        return remote(w1f.at[w1rows(dev)], w1f.at[w1rows(dev)], w1gs_sem.at[i], w1gr_sem.at[i], dev)

    for i in range(1, DEVICES):
        w1_scatter(i).start()
    gh.wait_sends()
    own = w2rows(core * half_rows + chip * piece, piece)
    total2 = w2acc[own, :]
    for j in range(1, chips):
        w2_scatter(j).wait_recv()
    for j in range(1, chips):
        total2 = total2 + w2part[j]
    w2f[own, :] = total2
    for j in range(1, chips):
        w2_scatter(j).wait_send()
    for j in range(1, chips):
        w2_gather(j, chip).start()
    total = w1p[w1rows(me), :]
    for i in range(1, DEVICES):
        w1_scatter(i).wait_recv()
    for i in range(1, DEVICES):
        total = total + w1r[i]
    w1f[w1rows(me), :] = total
    for i in range(1, DEVICES):
        w1_scatter(i).wait_send()
    for i in range(1, DEVICES):
        w1_gather(i).start()
    for j in range(1, chips):
        w2_gather(j, (chip + chips - j) % chips).wait_recv()
    w2_sib_gather(core).start()
    for j in range(1, chips):
        w2_gather(j, chip).wait_send()
    w2_sib_gather(1 - core).wait_recv()
    g2_out[...] = w2f[:classes, :]
    loss_out[0, 0] = jnp.sum(w2f[total_rows - 1:, :LANES] / cnt_src[4][0:1, :])
    for i in range(1, DEVICES):
        w1_gather_in(i).wait_recv()
    g1_out[...] = w1f[...]
    w2_sib_gather(core).wait_send()
    for i in range(1, DEVICES):
        w1_gather(i).wait_send()


def solution(mesh):
    axis = mesh.axis_names[0]

    def local_step(adj, x, w1, w2, labels, mask):
        rows, nodes = adj.shape
        fin, hid = w1.shape
        classes = w2.shape[1]
        unit = rows // UNITS
        cpad = -(-classes // 16) * 16
        total_rows = -(-(cpad + 1) // LANES) * LANES
        dma = pltpu.SemaphoreType.DMA
        vm = pl.BlockSpec(memory_space=pltpu.VMEM)
        loss, g1, g2 = pl.pallas_call(
            functools.partial(step_kernel, classes),
            out_shape=(jax.ShapeDtypeStruct((1, 1), F32),
                       jax.ShapeDtypeStruct((fin, hid), F32),
                       jax.ShapeDtypeStruct((classes, hid), F32)),
            in_specs=[pl.BlockSpec(memory_space=pl.ANY)] * 6,
            out_specs=(pl.BlockSpec(memory_space=pltpu.SMEM), vm, vm),
            scratch_shapes=[
                pltpu.VMEM((fin, hid), F32),
                pltpu.VMEM((classes, hid), F32),
                pltpu.VMEM((rows // LANES, LANES), jnp.int32),
                pltpu.VMEM((rows // LANES, LANES), jnp.int32),
                dma((UNITS + 4,)),
                pltpu.VMEM((rows, nodes), BF16),
                pltpu.VMEM((nodes // unit, cpad, unit), BF16),
                pltpu.VMEM((nodes, hid), BF16),
                pltpu.VMEM((rows, hid), F32),
                pltpu.VMEM((cpad, rows), F32),
                pltpu.VMEM((UNITS + 7, cpad, unit), BF16),
                pltpu.VMEM((rows, hid), BF16),
                pltpu.VMEM((fin, hid), BF16),
                pltpu.VMEM((cpad, hid), BF16),
                pltpu.VMEM((total_rows, hid), F32),
                pltpu.VMEM((total_rows // 2, hid), F32),
                pltpu.VMEM((8, total_rows // 16, hid), F32),
                pltpu.VMEM((total_rows, hid), F32),
                pltpu.VMEM((fin, hid), F32),
                pltpu.VMEM((DEVICES, fin // DEVICES, hid), F32),
                pltpu.VMEM((fin, hid), F32),
                pltpu.VMEM((5, 8, LANES), F32),
                pltpu.VMEM((4, 8, LANES), F32),
                pltpu.VMEM((1, LANES), F32),
                pltpu.VMEM((fin, rows), BF16),
                dma((DEVICES,)),
                dma((2, 30)), dma((2, 30)), dma((2, 32)), dma((2, 32)),
                dma((DEVICES,)), dma((DEVICES,)), dma((DEVICES,)), dma((DEVICES,)),
                dma((DEVICES,)), dma((DEVICES,)), dma((DEVICES,)), dma((DEVICES,)),
            ],
            compiler_params=pltpu.CompilerParams(collective_id=0, has_side_effects=True,
                                                 vmem_limit_bytes=67043328),
            name="gcn_step",
        )(adj, x, w1, w2.T, labels.reshape(rows // LANES, LANES), mask.reshape(rows // LANES, LANES))
        return loss[0, 0], g1, g2.T

    return jax.shard_map(local_step, mesh=mesh,
                         in_specs=(P(axis, None), P(axis, None), P(None, None), P(None, None), P(axis), P(axis)),
                         out_specs=(P(), P(None, None), P(None, None)), check_vma=False)
```

```python
import functools

import jax
import jax.numpy as jnp
from jax import lax
from jax.experimental import pallas as pl
from jax.experimental.pallas import tpu as pltpu
from jax.sharding import PartitionSpec as P

F32 = jnp.float32
BF16 = jnp.bfloat16
MESH = pl.DeviceIdType.MESH
DEVICES = 16
UNITS = 4
LANES = 128
CHUNK = 1024


def dot(a, b):
    return jnp.dot(a, b, preferred_element_type=F32)


def dot_tn(a, b):
    return lax.dot_general(a, b, (((0,), (0,)), ((), ())), preferred_element_type=F32)


def dot_nt(a, b):
    return lax.dot_general(a, b, (((1,), (1,)), ((), ())), preferred_element_type=F32)


def loop(n, fn):
    lax.fori_loop(0, n, lambda i, c: (fn(i), c)[1], 0)


def step_kernel(classes, adj, x_hbm, w1_hbm, w2_hbm, lab_hbm, msk_hbm,
                loss_out, g1_out, g2_out,
                w1_ref, w2_ref, lab_ref, msk_ref, in_sem,
                a_v, gb, hb, acc1, acc2, ys, hown, w1b, w2b,
                w2acc, w2rcv, w2part, w2f, w1p, w1r, w1f, cnt_src, cnt_rcv, loss_acc, xt,
                a_sem, rsem, ssem, sib_rsem, sib_ssem, cs_sem, cr_sem,
                w2s_sem, w2r_sem, w1s_sem, w1r_sem, w1gs_sem, w1gr_sem):
    rows = x_hbm.shape[0]
    fin = x_hbm.shape[1]
    unit = rows // UNITS
    hid = w1_ref.shape[1]
    cpad = w2b.shape[0]
    me = lax.axis_index("nodes")
    core = me % 2
    sib = me + 1 - 2 * core
    bit = [(me // v) % 2 for v in (2, 4, 8)]
    step = [v * (1 - 2 * b) for v, b in zip((2, 4, 8), bit)]
    own_d = [(1 - core) * step[r] + core * step[(r + 1) % 3] for r in range(3)]
    sib_d = [core * step[r] + (1 - core) * step[(r + 1) % 3] for r in range(3)]
    role_bit = [(1 - core) * bit[r] + core * bit[(r + 1) % 3] for r in range(3)]
    nbr = [me + d for d in own_d]

    def src_dev(base, deltas, hop, r):
        return base + deltas[r] + hop * deltas[(r + 2) % 3]

    anti = me + own_d[0] + own_d[1] + own_d[2]
    anti_sib = anti + 1 - 2 * core

    def remote(src, dst, ss, rs, dev):
        return pltpu.make_async_remote_copy(src_ref=src, dst_ref=dst, send_sem=ss, recv_sem=rs,
                                            device_id=(dev,), device_id_type=MESH)

    barrier = pltpu.get_barrier_semaphore()
    for dev in [sib] + nbr:
        pl.semaphore_signal(barrier, inc=1, device_id=(dev,), device_id_type=MESH)

    def uid(dev, q):
        return dev * UNITS + q

    order = [me, sib]
    for hop in (0, 1):
        order += [src_dev(me, own_d, hop, r) for r in range(3)]
        order += [src_dev(sib, sib_d, hop, r) for r in range(3)]
    order += [anti, anti_sib]

    def a_cols(dev):
        return pl.ds(pl.multiple_of(dev * rows, rows), rows)

    def a_copy(i):
        return pltpu.make_async_copy(adj.at[:, a_cols(order[i])], a_v.at[:, a_cols(order[i])], a_sem.at[i])

    x_units = [pltpu.make_async_copy(x_hbm.at[pl.ds(q * unit, unit)], gb.at[uid(me, q), pl.ds(0, unit), pl.ds(0, fin)],
                                     in_sem.at[q]) for q in range(UNITS)]
    inputs = [pltpu.make_async_copy(src, dst, in_sem.at[UNITS + i]) for i, (src, dst) in enumerate(
        [(w1_hbm, w1_ref), (w2_hbm, w2_ref), (msk_hbm, msk_ref), (lab_hbm, lab_ref)])]
    for c in x_units + inputs:
        c.start()
    for i in range(2):
        a_copy(i).start()

    def rows_of(dev, q):
        return pl.ds(pl.multiple_of(dev * rows + q * unit, unit), unit)

    pl.semaphore_wait(barrier, 4)

    def pick(f, vals):
        return jnp.where(f == 0, vals[0], jnp.where(f == 1, vals[1], vals[2]))

    class Gather:
        def __init__(self, view, height, par, sib_view=None):
            self.view, self.height, self.par = view, height, par
            self.shared, self.sib_view = sib_view is not None, sib_view or view

        def hop_copy(self, dev, q, to, sslot, rslot):
            v = self.view(dev, q)
            return remote(v, v, ssem.at[self.par, sslot], rsem.at[self.par, rslot], to)

        def sib_copy(self, dev, q, slot, src=None):
            v = self.sib_view(dev, q)
            return remote(v if src is None else src, v, sib_ssem.at[self.par, slot], sib_rsem.at[self.par, slot], sib)

        def own_copies(self, q):
            hops = [self.hop_copy(me, q, nbr[r], r * 4 + q, r * 4 + q) for r in range(3)]
            return hops if self.shared else hops + [self.sib_copy(me, q, 28 + q)]

        def start_own(self, q):
            for c in self.own_copies(q):
                c.start()

        def forward(self, q):
            return [self.hop_copy(src_dev(me, own_d, 0, r), q, nbr[(r + 1) % 3], 12 + r * 4 + q,
                                  12 + ((r + 1) % 3) * 4 + q) for r in range(3)]

        def last_forward(self, q):
            to = q % 3
            dev = pick((to + 2) % 3, [src_dev(me, own_d, 1, r) for r in range(3)])
            return self.hop_copy(dev, q, pick(to, nbr), 24 + q, 24 + q)

        def thirds(self, dev):
            tiles = self.height // 16
            at = [0, tiles // 3 * 16, 2 * (tiles // 3) * 16, self.height]
            return [self.view(dev, 3).at[pl.ds(at[t], at[t + 1] - at[t])] for t in range(3)]

        def third_copy(self, t):
            v = self.thirds(src_dev(me, own_d, 1, (t + 2) % 3))[t]
            return remote(v, v, ssem.at[self.par, 27 + t], rsem.at[self.par, 27 + t], nbr[t])

        def third_in(self, t):
            v = self.thirds(anti)[t]
            return remote(v, v, ssem.at[self.par, 27 + t], rsem.at[self.par, 27 + t], nbr[t])

        def arrive(self, hop, q):
            for r in range(3):
                d = src_dev(me, own_d, hop, r)
                self.hop_copy(d, q, nbr[r], r * 4 + q, hop * 12 + r * 4 + q).wait_recv()

            @pl.when(hop == 0)
            def _():
                for c in self.forward(q):
                    c.start()

            @pl.when((hop == 1) & (q < 3))
            def _():
                self.last_forward(q).start()

            @pl.when((hop == 1) & (q == 3))
            def _():
                for t in range(3):
                    self.third_copy(t).start()
            if not self.shared:
                for r in range(3):
                    self.sib_copy(src_dev(me, own_d, hop, r), q, hop * 12 + r * 4 + q).start()

        def arrive_last(self, q):
            if q < 3:
                self.hop_copy(anti, q, nbr[0], 24 + q, 24 + q).wait_recv()
            else:
                for t in range(3):
                    self.third_in(t).wait_recv()
            if not self.shared:
                self.sib_copy(anti, q, 24 + q).start()

        def sib_wait(self, hop, q):
            for r in range(3):
                self.sib_copy(src_dev(sib, sib_d, hop, r), q, hop * 12 + r * 4 + q).wait_recv()

        def sib_wait_own(self, q):
            self.sib_copy(sib, q, 28 + q).wait_recv()

        def sib_wait_last(self, q):
            self.sib_copy(anti_sib, q, 24 + q).wait_recv()

        def wait_sends(self):
            def body(q):
                for c in self.own_copies(q) + self.forward(q):
                    c.wait_send()
                if not self.shared:
                    for slot in (q, 4 + q, 8 + q, 12 + q, 16 + q, 20 + q, 24 + q):
                        self.sib_copy(me, q, slot).wait_send()
            loop(UNITS, body)
            if self.shared:
                for slot in (15, 19, 23, 24, 25, 26, 27, 28, 29, 30, 31):
                    self.sib_copy(me, 0, slot).wait_send()
            for q in range(3):
                self.last_forward(q).wait_send()
            for t in range(3):
                self.third_copy(t).wait_send()

    def phase(g, add, zero, finish, hook, first, whole=False):
        def a_wait(lo, hi):
            if first:
                for i in range(lo, hi):
                    a_copy(i).wait()

        zero()

        def halves(fn, n=2):
            if g.shared:
                fn(0)
                fn(1)
            else:
                loop(n, fn)

        def near(t):
            if first and t == 0:
                a_wait(0, 1)

            def wait_sib():
                for q in range(UNITS):
                    g.sib_wait_own(q)
                a_wait(1, 2)
            if not g.shared:
                pl.when(t == 1)(wait_sib)
            elif t == 1:
                wait_sib()
            dev = me + t * (sib - me)
            add([(dev, q) for q in range(UNITS)], t, -1)
        halves(near)
        hook(-1, None)

        def group(i):
            @pl.when(i < 8)
            def _():
                g.arrive(i // 4, i % 4)

            @pl.when(i == 8)
            def _():
                for j in range(3):
                    g.arrive_last(j)

            if g.shared:
                @pl.when(i == 9)
                def _():
                    g.arrive_last(3)
            hook(None, i)

            def half(t):
                if g.shared:
                    k, sb, live = i - t, t, (i - t >= 0) & (i - t <= 8)
                else:
                    k, sb = i - t * (2 - t), (t + 1) // 2
                    live = (t == 0) | ((t == 1) & (i >= 1) & (i <= 7)) | ((t == 2) & (i >= 7))
                hop, q, far = (k // 4) % 2, k % 4, k // 8

                if not g.shared:
                    @pl.when((t == 2) & (i == 8))
                    def _():
                        g.arrive_last(3)
                        add([(anti, 3)], 0, 9)

                @pl.when(live)
                def _():
                    def on_sib(cond, fn):
                        if not g.shared:
                            pl.when((t >= 1) & cond)(fn)
                        elif t == 1:
                            pl.when(cond)(fn)

                    on_sib(k < 8, lambda: g.sib_wait(hop, q))
                    on_sib(k == 8, lambda: [g.sib_wait_last(j) for j in range(3)] and None)
                    if first:
                        for key, (lo, hi) in {(0, 0): (2, 5), (0, 1): (5, 8), (4, 0): (8, 11), (4, 1): (11, 14),
                                              (8, 0): (14, 15), (8, 1): (15, 16)}.items():
                            if t == key[1]:
                                @pl.when(k == key[0])
                                def _(lo=lo, hi=hi):
                                    a_wait(lo, hi)
                    pairs = []
                    for r in range(3):
                        o, s = src_dev(me, own_d, hop, r), src_dev(sib, sib_d, hop, r)
                        near_dev = o + sb * (s - o)
                        far_dev = anti + sb * (anti_sib - anti)
                        pairs.append((near_dev + far * (far_dev - near_dev), q + far * (r - q)))
                    add(pairs, t, k)
            halves(half, 3)
        if g.shared:
            loop(10, group)
            add([(anti, 3)], 0, 9)
        else:
            loop(9, group)
            hook(None, 9)
        g.sib_wait_last(3)

        if whole:
            finish(None, [(anti_sib, 3)])
            return

        def last(m):
            @pl.when(m == UNITS - 1)
            def _():
                g.wait_sends()
            finish(m, [(anti_sib, 3)])
        loop(UNITS, last)

    gx = Gather(lambda dev, q: gb.at[uid(dev, q), pl.ds(0, unit), pl.ds(0, fin)], unit, 0,
                lambda dev, q: gb.at[uid(dev, q), pl.ds(0, unit), pl.ds(0, hid)])
    gh = Gather(lambda dev, q: hb.at[rows_of(dev, q)], unit, 1)
    gg = Gather(lambda dev, q: gb.at[uid(dev, q)], cpad, 0)

    def mrows(m):
        return pl.ds(pl.multiple_of(m * unit, unit), unit)

    def chunk(c):
        return pl.ds(pl.multiple_of(c * CHUNK, CHUNK), CHUNK)

    for q in range(UNITS):
        x_units[q].wait()
        gx.start_own(q)
    for i in range(2, 8):
        a_copy(i).start()
    for c in inputs:
        c.wait()
    w1b[...] = w1_ref[...].astype(BF16)
    w2acc[...] = jnp.zeros_like(w2acc)
    w2acc[:classes, :] = w2_ref[...]
    w2b[...] = w2acc[:cpad, :].astype(BF16)

    partners = [sib] + nbr

    def cnt_copy(k):
        return remote(cnt_src.at[k], cnt_rcv.at[k], cs_sem.at[k], cr_sem.at[k], partners[k])

    def cnt_next(k):
        cnt_copy(k).wait_recv()
        cnt_src[k + 1] = cnt_src[k] + cnt_rcv[k]
        if k < 3:
            cnt_copy(k + 1).start()

    local = jnp.sum(msk_ref[...].astype(F32), axis=1, keepdims=True)
    local = jnp.sum(local, axis=0, keepdims=True)
    cnt_src[0] = jnp.broadcast_to(local, (8, LANES))

    def hook1(pre, i):
        if i is None:
            for j in range(8, DEVICES):
                a_copy(j).start()
            cnt_copy(0).start()
            return

        @pl.when(i == 1)
        def _():
            cnt_next(0)

        @pl.when(i == 9)
        def _():
            cnt_next(1)

    def zero1():
        acc1[...] = jnp.zeros_like(acc1)

    def add_rows(acc, pairs, operand):
        def body(c):
            s = chunk(c)
            v = acc[s, :]
            for j, (dev, q) in enumerate(pairs):
                v = v + dot(a_v[s, rows_of(dev, q)], operand(j))
            acc[s, :] = v
        loop(rows // CHUNK, body)

    def add1(pairs, t, k):
        if t == 1:
            add_rows(acc1, pairs, lambda j: gb[uid(*pairs[j]), :unit, :hid])
            return
        n = len(pairs)
        if isinstance(k, int):
            at = 0 if k < 0 else 10
            slots = [28 + j for j in range(n)] if k < 0 else [27]
        else:
            hop, q, far = (k // 4) % 2, k % 4, k // 8
            at = UNITS + 3 * (k % 2)
            slots = [hop * 12 + r * 4 + q + far * (24 + r - hop * 12 - r * 4 - q) for r in range(3)]

            @pl.when(k >= 2)
            def _():
                back = k - 2
                for r in range(3):
                    gx.sib_copy(me, 0, (back // 4) * 12 + r * 4 + back % 4).wait_send()
        for j, (dev, q) in enumerate(pairs):
            ys[at + j, :unit, :hid] = dot(gb[uid(dev, q), :unit, :fin], w1b[...]).astype(BF16)

        def send():
            for j, (dev, q) in enumerate(pairs):
                gx.sib_copy(dev, q, slots[j], ys.at[at + j, pl.ds(0, unit), pl.ds(0, hid)]).start()
        if isinstance(k, int):
            send()
        add_rows(acc1, pairs, lambda j: ys[at + j, :unit, :hid])
        if not isinstance(k, int):
            send()

    def finish1(m, pairs):
        s = mrows(m)
        z = acc1[s, :]
        for dev, q in pairs:
            z = z + dot(a_v[s, rows_of(dev, q)], gb[uid(dev, q), :unit, :hid])
        acc1[s, :] = z
        h = jnp.maximum(z, 0.0).astype(BF16)
        hb[rows_of(me, m), :] = h
        hown[s, :] = h
        gh.start_own(m)

    phase(gx, add1, zero1, finish1, hook1, True)

    def zero2():
        acc2[...] = jnp.zeros_like(acc2)

    def y2(dev, q):
        return dot_nt(w2b[...], hb[rows_of(dev, q), :]).astype(BF16)

    def add_cols(acc, pairs, operand):
        def body(c):
            s = chunk(c)
            v = acc[:, s]
            for j, (dev, q) in enumerate(pairs):
                v = v + dot_nt(operand(j), a_v[s, rows_of(dev, q)])
            acc[:, s] = v
        loop(rows // CHUNK, body)

    def add2(pairs, t, k):
        for j, (dev, q) in enumerate(pairs):
            ys[j] = y2(dev, q)
        add_cols(acc2, pairs, lambda j: ys[j])

    loss_acc[...] = jnp.zeros_like(loss_acc)

    def hook2(pre, i):
        if i is None:
            for q in range(UNITS):
                xt[:, q * unit:(q + 1) * unit] = gb[uid(me, q), :unit, :fin].T
            return

        @pl.when(i == 0)
        def _():
            cnt_next(2)

        @pl.when(i == 9)
        def _():
            cnt_next(3)
            for k in range(4):
                cnt_copy(k).wait_send()

    def finish2(m, pairs):
        s = mrows(m)

        @pl.when(m == 0)
        def _():
            for j, (dev, q) in enumerate(pairs):
                ys[j] = y2(dev, q)
        z = acc2[:, s]
        for j, (dev, q) in enumerate(pairs):
            z = z + dot_nt(ys[j], a_v[s, rows_of(dev, q)])
        acc2[:, s] = z
        for h in range(unit // LANES):
            at = pl.ds(pl.multiple_of(m * unit + h * LANES, LANES), LANES)
            zc = acc2[:, at]
            row = lax.broadcasted_iota(jnp.int32, (cpad, LANES), 0)
            zm = jnp.where(row < classes, zc, -jnp.inf)
            top = jnp.max(zm, axis=0, keepdims=True)
            log_norm = top + jnp.log(jnp.sum(jnp.exp(zm - top), axis=0, keepdims=True))
            which = m * (unit // LANES) + h
            hot = row == lab_ref[pl.ds(which, 1), :]
            mask = msk_ref[pl.ds(which, 1), :].astype(F32)
            picked = jnp.sum(jnp.where(hot, zc, 0.0), axis=0, keepdims=True)
            loss_acc[...] = loss_acc[...] + mask * (log_norm - picked)
            gr = (jnp.exp(zm - log_norm) - jnp.where(hot, 1.0, 0.0)) * (mask / cnt_src[4][0:1, :])
            gb[uid(me, m), :, h * LANES:(h + 1) * LANES] = gr.astype(BF16)
        gg.start_own(m)

    phase(gh, add2, zero2, finish2, hook2, False)

    def finish3(m, pairs):
        s = mrows(m)
        z = acc2[:, s]
        for dev, q in pairs:
            z = z + dot_nt(gb[uid(dev, q)], a_v[s, rows_of(dev, q)])
        e = z.astype(BF16)
        ys[m] = e
        gz = dot_tn(e, w2b[...])
        hb[rows_of(me, m), :] = jnp.where(acc1[s, :] > 0.0, gz, 0.0).astype(BF16)
        gh.start_own(m)

    phase(gg, lambda pairs, t, k: add_cols(acc2, pairs, lambda j: gb[uid(*pairs[j])]), zero2, finish3,
          lambda pre, i: None, False)

    total_rows = w2acc.shape[0]
    half_rows = total_rows // 2
    piece = half_rows // 8
    chips = DEVICES // 2
    chip = me // 2

    def w2rows(start, n):
        return pl.ds(pl.multiple_of(start, 8), n)

    mine = w2rows(core * half_rows, half_rows)

    def w2_sib():
        out = w2acc.at[w2rows((1 - core) * half_rows, half_rows)]
        return remote(out, w2rcv, w2s_sem.at[0], w2r_sem.at[0], sib)

    def w2_scatter(j):
        to = (chip + j) % chips
        out = w2acc.at[w2rows(core * half_rows + to * piece, piece)]
        return remote(out, w2part.at[j], w2s_sem.at[j], w2r_sem.at[j], to * 2 + core)

    def w2_gather(j, frm):
        to = (chip + j) % chips
        out = w2f.at[w2rows(core * half_rows + frm * piece, piece)]
        return remote(out, out, w2s_sem.at[chips + j], w2r_sem.at[chips + j], to * 2 + core)

    def w2_sib_gather(c):
        out = w2f.at[w2rows(c * half_rows, half_rows)]
        return remote(out, out, w2s_sem.at[chips], w2r_sem.at[chips], sib)

    def hook4(pre, i):
        if i is None:
            w2acc[...] = jnp.zeros_like(w2acc)
            w2acc[:cpad, :] = sum(dot(ys[q], hown[q * unit:(q + 1) * unit, :]) for q in range(UNITS))
            w2acc[total_rows - 1:, :LANES] = loss_acc[...]
            return

        @pl.when(i == 0)
        def _():
            w2_sib().start()

        @pl.when(i == 1)
        def _():
            w2_sib().wait_recv()
            w2acc[mine, :] = w2acc[mine, :] + w2rcv[...]

        @pl.when(i == 7)
        def _():
            w2_sib().wait_send()
            for j in range(1, chips):
                w2_scatter(j).start()

    def finish4(m, pairs):
        z = acc1[...]
        for dev, q in pairs:
            z = z + dot(a_v[:, rows_of(dev, q)], hb[rows_of(dev, q), :])
        w1p[...] = dot(xt[...], z.astype(BF16))

    phase(gh, lambda pairs, t, k: add_rows(acc1, pairs, lambda j: hb[rows_of(*pairs[j]), :]), zero1, finish4, hook4, False, True)

    sl = fin // DEVICES

    def w1rows(dev):
        return pl.ds(pl.multiple_of(dev * sl, sl), sl)

    def w1_scatter(i):
        dev = (me + i) % DEVICES
        return remote(w1p.at[w1rows(dev)], w1r.at[i], w1s_sem.at[i], w1r_sem.at[i], dev)

    def w1_gather(i):
        dev = (me + i) % DEVICES
        return remote(w1f.at[w1rows(me)], w1f.at[w1rows(me)], w1gs_sem.at[i], w1gr_sem.at[i], dev)

    def w1_gather_in(i):
        dev = (me + DEVICES - i) % DEVICES
        return remote(w1f.at[w1rows(dev)], w1f.at[w1rows(dev)], w1gs_sem.at[i], w1gr_sem.at[i], dev)

    for i in range(1, DEVICES):
        w1_scatter(i).start()
    gh.wait_sends()
    own = w2rows(core * half_rows + chip * piece, piece)
    total2 = w2acc[own, :]
    for j in range(1, chips):
        w2_scatter(j).wait_recv()
    for j in range(1, chips):
        total2 = total2 + w2part[j]
    w2f[own, :] = total2
    for j in range(1, chips):
        w2_scatter(j).wait_send()
    for j in range(1, chips):
        w2_gather(j, chip).start()
    total = w1p[w1rows(me), :]
    for i in range(1, DEVICES):
        w1_scatter(i).wait_recv()
    for i in range(1, DEVICES):
        total = total + w1r[i]
    w1f[w1rows(me), :] = total
    for i in range(1, DEVICES):
        w1_scatter(i).wait_send()
    for i in range(1, DEVICES):
        w1_gather(i).start()
    for j in range(1, chips):
        w2_gather(j, (chip + chips - j) % chips).wait_recv()
    w2_sib_gather(core).start()
    for j in range(1, chips):
        w2_gather(j, chip).wait_send()
    w2_sib_gather(1 - core).wait_recv()
    g2_out[...] = w2f[:classes, :]
    loss_out[0, 0] = jnp.sum(w2f[total_rows - 1:, :LANES] / cnt_src[4][0:1, :])
    for i in range(1, DEVICES):
        w1_gather_in(i).wait_recv()
    g1_out[...] = w1f[...]
    w2_sib_gather(core).wait_send()
    for i in range(1, DEVICES):
        w1_gather(i).wait_send()


def solution(mesh):
    axis = mesh.axis_names[0]

    def local_step(adj, x, w1, w2, labels, mask):
        rows, nodes = adj.shape
        fin, hid = w1.shape
        classes = w2.shape[1]
        unit = rows // UNITS
        cpad = -(-classes // 16) * 16
        total_rows = -(-(cpad + 1) // LANES) * LANES
        dma = pltpu.SemaphoreType.DMA
        vm = pl.BlockSpec(memory_space=pltpu.VMEM)
        loss, g1, g2 = pl.pallas_call(
            functools.partial(step_kernel, classes),
            out_shape=(jax.ShapeDtypeStruct((1, 1), F32),
                       jax.ShapeDtypeStruct((fin, hid), F32),
                       jax.ShapeDtypeStruct((classes, hid), F32)),
            in_specs=[pl.BlockSpec(memory_space=pl.ANY)] * 6,
            out_specs=(pl.BlockSpec(memory_space=pltpu.SMEM), vm, vm),
            scratch_shapes=[
                pltpu.VMEM((fin, hid), F32),
                pltpu.VMEM((classes, hid), F32),
                pltpu.VMEM((rows // LANES, LANES), jnp.int32),
                pltpu.VMEM((rows // LANES, LANES), jnp.int32),
                dma((UNITS + 4,)),
                pltpu.VMEM((rows, nodes), BF16),
                pltpu.VMEM((nodes // unit, cpad, unit), BF16),
                pltpu.VMEM((nodes, hid), BF16),
                pltpu.VMEM((rows, hid), F32),
                pltpu.VMEM((cpad, rows), F32),
                pltpu.VMEM((UNITS + 7, cpad, unit), BF16),
                pltpu.VMEM((rows, hid), BF16),
                pltpu.VMEM((fin, hid), BF16),
                pltpu.VMEM((cpad, hid), BF16),
                pltpu.VMEM((total_rows, hid), F32),
                pltpu.VMEM((total_rows // 2, hid), F32),
                pltpu.VMEM((8, total_rows // 16, hid), F32),
                pltpu.VMEM((total_rows, hid), F32),
                pltpu.VMEM((fin, hid), F32),
                pltpu.VMEM((DEVICES, fin // DEVICES, hid), F32),
                pltpu.VMEM((fin, hid), F32),
                pltpu.VMEM((5, 8, LANES), F32),
                pltpu.VMEM((4, 8, LANES), F32),
                pltpu.VMEM((1, LANES), F32),
                pltpu.VMEM((fin, rows), BF16),
                dma((DEVICES,)),
                dma((2, 30)), dma((2, 30)), dma((2, 32)), dma((2, 32)),
                dma((DEVICES,)), dma((DEVICES,)), dma((DEVICES,)), dma((DEVICES,)),
                dma((DEVICES,)), dma((DEVICES,)), dma((DEVICES,)), dma((DEVICES,)),
            ],
            compiler_params=pltpu.CompilerParams(collective_id=0, has_side_effects=True,
                                                 vmem_limit_bytes=67043328),
            name="gcn_step",
        )(adj, x, w1, w2.T, labels.reshape(rows // LANES, LANES), mask.reshape(rows // LANES, LANES))
        return loss[0, 0], g1, g2.T

    return jax.shard_map(local_step, mesh=mesh,
                         in_specs=(P(axis, None), P(axis, None), P(None, None), P(None, None), P(axis), P(axis)),
                         out_specs=(P(), P(None, None), P(None, None)), check_vma=False)
```

```python
import functools

import jax
import jax.numpy as jnp
from jax import lax
from jax.experimental import pallas as pl
from jax.experimental.pallas import tpu as pltpu
from jax.sharding import PartitionSpec as P

F32 = jnp.float32
BF16 = jnp.bfloat16
MESH = pl.DeviceIdType.MESH
DEVICES = 16
UNITS = 4
LANES = 128
CHUNK = 1024


def dot(a, b):
    return jnp.dot(a, b, preferred_element_type=F32)


def dot_tn(a, b):
    return lax.dot_general(a, b, (((0,), (0,)), ((), ())), preferred_element_type=F32)


def dot_nt(a, b):
    return lax.dot_general(a, b, (((1,), (1,)), ((), ())), preferred_element_type=F32)


def loop(n, fn):
    lax.fori_loop(0, n, lambda i, c: (fn(i), c)[1], 0)


def step_kernel(classes, adj, x_hbm, w1_hbm, w2_hbm, lab_hbm, msk_hbm,
                loss_out, g1_out, g2_out,
                w1_ref, w2_ref, lab_ref, msk_ref, in_sem,
                a_v, gb, hb, acc1, acc2, ys, hown, w1b, w2b,
                w2acc, w2rcv, w2part, w2f, w1p, w1r, w1f, cnt_src, cnt_rcv, loss_acc, xt,
                a_sem, rsem, ssem, sib_rsem, sib_ssem, cs_sem, cr_sem,
                w2s_sem, w2r_sem, w1s_sem, w1r_sem, w1gs_sem, w1gr_sem):
    rows = x_hbm.shape[0]
    fin = x_hbm.shape[1]
    unit = rows // UNITS
    hid = w1_ref.shape[1]
    cpad = w2b.shape[0]
    me = lax.axis_index("nodes")
    core = me % 2
    sib = me + 1 - 2 * core
    bit = [(me // v) % 2 for v in (2, 4, 8)]
    step = [v * (1 - 2 * b) for v, b in zip((2, 4, 8), bit)]
    own_d = [(1 - core) * step[r] + core * step[(r + 1) % 3] for r in range(3)]
    sib_d = [core * step[r] + (1 - core) * step[(r + 1) % 3] for r in range(3)]
    role_bit = [(1 - core) * bit[r] + core * bit[(r + 1) % 3] for r in range(3)]
    nbr = [me + d for d in own_d]

    def src_dev(base, deltas, hop, r):
        return base + deltas[r] + hop * deltas[(r + 2) % 3]

    anti = me + own_d[0] + own_d[1] + own_d[2]
    anti_sib = anti + 1 - 2 * core

    def remote(src, dst, ss, rs, dev):
        return pltpu.make_async_remote_copy(src_ref=src, dst_ref=dst, send_sem=ss, recv_sem=rs,
                                            device_id=(dev,), device_id_type=MESH)

    barrier = pltpu.get_barrier_semaphore()
    for dev in [sib] + nbr:
        pl.semaphore_signal(barrier, inc=1, device_id=(dev,), device_id_type=MESH)

    def uid(dev, q):
        return dev * UNITS + q

    order = [me, sib]
    for hop in (0, 1):
        order += [src_dev(me, own_d, hop, r) for r in range(3)]
        order += [src_dev(sib, sib_d, hop, r) for r in range(3)]
    order += [anti, anti_sib]

    def a_cols(dev):
        return pl.ds(pl.multiple_of(dev * rows, rows), rows)

    def a_copy(i):
        return pltpu.make_async_copy(adj.at[:, a_cols(order[i])], a_v.at[:, a_cols(order[i])], a_sem.at[i])

    x_units = [pltpu.make_async_copy(x_hbm.at[pl.ds(q * unit, unit)], gb.at[uid(me, q), pl.ds(0, unit), pl.ds(0, fin)],
                                     in_sem.at[q]) for q in range(UNITS)]
    inputs = [pltpu.make_async_copy(src, dst, in_sem.at[UNITS + i]) for i, (src, dst) in enumerate(
        [(w1_hbm, w1_ref), (w2_hbm, w2_ref), (msk_hbm, msk_ref), (lab_hbm, lab_ref)])]
    for c in x_units + inputs:
        c.start()
    for i in range(2):
        a_copy(i).start()

    def rows_of(dev, q):
        return pl.ds(pl.multiple_of(dev * rows + q * unit, unit), unit)

    pl.semaphore_wait(barrier, 4)

    def pick(f, vals):
        return jnp.where(f == 0, vals[0], jnp.where(f == 1, vals[1], vals[2]))

    class Gather:
        def __init__(self, view, height, par, sib_view=None):
            self.view, self.height, self.par = view, height, par
            self.shared, self.sib_view = sib_view is not None, sib_view or view

        def hop_copy(self, dev, q, to, sslot, rslot):
            v = self.view(dev, q)
            return remote(v, v, ssem.at[self.par, sslot], rsem.at[self.par, rslot], to)

        def sib_copy(self, dev, q, slot, src=None):
            v = self.sib_view(dev, q)
            return remote(v if src is None else src, v, sib_ssem.at[self.par, slot], sib_rsem.at[self.par, slot], sib)

        def own_copies(self, q):
            hops = [self.hop_copy(me, q, nbr[r], r * 4 + q, r * 4 + q) for r in range(3)]
            return hops if self.shared else hops + [self.sib_copy(me, q, 28 + q)]

        def start_own(self, q):
            for c in self.own_copies(q):
                c.start()

        def forward(self, q):
            return [self.hop_copy(src_dev(me, own_d, 0, r), q, nbr[(r + 1) % 3], 12 + r * 4 + q,
                                  12 + ((r + 1) % 3) * 4 + q) for r in range(3)]

        def last_forward(self, q):
            to = q % 3
            dev = pick((to + 2) % 3, [src_dev(me, own_d, 1, r) for r in range(3)])
            return self.hop_copy(dev, q, pick(to, nbr), 24 + q, 24 + q)

        def thirds(self, dev):
            tiles = self.height // 16
            at = [0, tiles // 3 * 16, 2 * (tiles // 3) * 16, self.height]
            return [self.view(dev, 3).at[pl.ds(at[t], at[t + 1] - at[t])] for t in range(3)]

        def third_copy(self, t):
            v = self.thirds(src_dev(me, own_d, 1, (t + 2) % 3))[t]
            return remote(v, v, ssem.at[self.par, 27 + t], rsem.at[self.par, 27 + t], nbr[t])

        def third_in(self, t):
            v = self.thirds(anti)[t]
            return remote(v, v, ssem.at[self.par, 27 + t], rsem.at[self.par, 27 + t], nbr[t])

        def arrive(self, hop, q):
            for r in range(3):
                d = src_dev(me, own_d, hop, r)
                self.hop_copy(d, q, nbr[r], r * 4 + q, hop * 12 + r * 4 + q).wait_recv()

            @pl.when(hop == 0)
            def _():
                for c in self.forward(q):
                    c.start()

            @pl.when((hop == 1) & (q < 3))
            def _():
                self.last_forward(q).start()

            @pl.when((hop == 1) & (q == 3))
            def _():
                for t in range(3):
                    self.third_copy(t).start()
            if not self.shared:
                for r in range(3):
                    self.sib_copy(src_dev(me, own_d, hop, r), q, hop * 12 + r * 4 + q).start()

        def arrive_last(self, q):
            if q < 3:
                self.hop_copy(anti, q, nbr[0], 24 + q, 24 + q).wait_recv()
            else:
                for t in range(3):
                    self.third_in(t).wait_recv()
            if not self.shared:
                self.sib_copy(anti, q, 24 + q).start()

        def sib_wait(self, hop, q):
            for r in range(3):
                self.sib_copy(src_dev(sib, sib_d, hop, r), q, hop * 12 + r * 4 + q).wait_recv()

        def sib_wait_own(self, q):
            self.sib_copy(sib, q, 28 + q).wait_recv()

        def sib_wait_last(self, q):
            self.sib_copy(anti_sib, q, 24 + q).wait_recv()

        def wait_sends(self):
            def body(q):
                for c in self.own_copies(q) + self.forward(q):
                    c.wait_send()
                if not self.shared:
                    for slot in (q, 4 + q, 8 + q, 12 + q, 16 + q, 20 + q, 24 + q):
                        self.sib_copy(me, q, slot).wait_send()
            loop(UNITS, body)
            if self.shared:
                for slot in (15, 19, 23, 24, 25, 26, 27, 28, 29, 30, 31):
                    self.sib_copy(me, 0, slot).wait_send()
            for q in range(3):
                self.last_forward(q).wait_send()
            for t in range(3):
                self.third_copy(t).wait_send()

    def phase(g, add, zero, finish, hook, first, whole=False):
        def a_wait(lo, hi):
            if first:
                for i in range(lo, hi):
                    a_copy(i).wait()

        zero()

        def halves(fn, n=2):
            if g.shared:
                fn(0)
                fn(1)
            else:
                loop(n, fn)

        def near(t):
            if first and t == 0:
                a_wait(0, 1)

            def wait_sib():
                for q in range(UNITS):
                    g.sib_wait_own(q)
                a_wait(1, 2)
            if not g.shared:
                pl.when(t == 1)(wait_sib)
            elif t == 1:
                wait_sib()
            dev = me + t * (sib - me)
            add([(dev, q) for q in range(UNITS)], t, -1)
        halves(near)
        hook(-1, None)

        def group(i):
            @pl.when(i < 8)
            def _():
                g.arrive(i // 4, i % 4)

            @pl.when(i == 8)
            def _():
                for j in range(3):
                    g.arrive_last(j)

            hook(None, i)

            def half(t):
                if g.shared:
                    k, sb, live = i - t, t, (i - t >= 0) & (i - t <= 8)
                else:
                    k, sb = i - t * (2 - t), (t + 1) // 2
                    live = (t == 0) | ((t == 1) & (i >= 1) & (i <= 7)) | ((t == 2) & (i >= 7))
                hop, q, far = (k // 4) % 2, k % 4, k // 8

                def last_own():
                    g.arrive_last(3)
                    add([(anti, 3)], 0, 9)
                if not g.shared:
                    pl.when((t == 2) & (i == 8))(last_own)
                elif t == 1:
                    pl.when(i == 8)(last_own)

                @pl.when(live)
                def _():
                    def on_sib(cond, fn):
                        if not g.shared:
                            pl.when((t >= 1) & cond)(fn)
                        elif t == 1:
                            pl.when(cond)(fn)

                    on_sib(k < 8, lambda: g.sib_wait(hop, q))
                    on_sib(k == 8, lambda: [g.sib_wait_last(j) for j in range(3)] and None)
                    if first:
                        for key, (lo, hi) in {(0, 0): (2, 5), (0, 1): (5, 8), (4, 0): (8, 11), (4, 1): (11, 14),
                                              (8, 0): (14, 15), (8, 1): (15, 16)}.items():
                            if t == key[1]:
                                @pl.when(k == key[0])
                                def _(lo=lo, hi=hi):
                                    a_wait(lo, hi)
                    pairs = []
                    for r in range(3):
                        o, s = src_dev(me, own_d, hop, r), src_dev(sib, sib_d, hop, r)
                        near_dev = o + sb * (s - o)
                        far_dev = anti + sb * (anti_sib - anti)
                        pairs.append((near_dev + far * (far_dev - near_dev), q + far * (r - q)))
                    add(pairs, t, k)
            halves(half, 3)
        if g.shared:
            loop(10, group)
        else:
            loop(9, group)
            hook(None, 9)
        g.sib_wait_last(3)

        if whole:
            finish(None, [(anti_sib, 3)])
            return

        def last(m):
            @pl.when(m == UNITS - 1)
            def _():
                g.wait_sends()
            finish(m, [(anti_sib, 3)])
        loop(UNITS, last)

    gx = Gather(lambda dev, q: gb.at[uid(dev, q), pl.ds(0, unit), pl.ds(0, fin)], unit, 0,
                lambda dev, q: gb.at[uid(dev, q), pl.ds(0, unit), pl.ds(0, hid)])
    gh = Gather(lambda dev, q: hb.at[rows_of(dev, q)], unit, 1)
    gg = Gather(lambda dev, q: gb.at[uid(dev, q)], cpad, 0)

    def mrows(m):
        return pl.ds(pl.multiple_of(m * unit, unit), unit)

    def chunk(c):
        return pl.ds(pl.multiple_of(c * CHUNK, CHUNK), CHUNK)

    for q in range(UNITS):
        x_units[q].wait()
        gx.start_own(q)
    for i in range(2, 8):
        a_copy(i).start()
    for c in inputs:
        c.wait()
    w1b[...] = w1_ref[...].astype(BF16)
    w2acc[...] = jnp.zeros_like(w2acc)
    w2acc[:classes, :] = w2_ref[...]
    w2b[...] = w2acc[:cpad, :].astype(BF16)

    partners = [sib] + nbr

    def cnt_copy(k):
        return remote(cnt_src.at[k], cnt_rcv.at[k], cs_sem.at[k], cr_sem.at[k], partners[k])

    def cnt_next(k):
        cnt_copy(k).wait_recv()
        cnt_src[k + 1] = cnt_src[k] + cnt_rcv[k]
        if k < 3:
            cnt_copy(k + 1).start()

    local = jnp.sum(msk_ref[...].astype(F32), axis=1, keepdims=True)
    local = jnp.sum(local, axis=0, keepdims=True)
    cnt_src[0] = jnp.broadcast_to(local, (8, LANES))

    def hook1(pre, i):
        if i is None:
            for j in range(8, DEVICES):
                a_copy(j).start()
            cnt_copy(0).start()
            return

        @pl.when(i == 1)
        def _():
            cnt_next(0)

        @pl.when(i == 9)
        def _():
            cnt_next(1)

    def zero1():
        acc1[...] = jnp.zeros_like(acc1)

    def add_rows(acc, pairs, operand):
        def body(c):
            s = chunk(c)
            v = acc[s, :]
            for j, (dev, q) in enumerate(pairs):
                v = v + dot(a_v[s, rows_of(dev, q)], operand(j))
            acc[s, :] = v
        loop(rows // CHUNK, body)

    def add1(pairs, t, k):
        if t == 1:
            add_rows(acc1, pairs, lambda j: gb[uid(*pairs[j]), :unit, :hid])
            return
        n = len(pairs)
        if isinstance(k, int):
            at = 0 if k < 0 else 10
            slots = [28 + j for j in range(n)] if k < 0 else [27]
        else:
            hop, q, far = (k // 4) % 2, k % 4, k // 8
            at = UNITS + 3 * (k % 2)
            slots = [hop * 12 + r * 4 + q + far * (24 + r - hop * 12 - r * 4 - q) for r in range(3)]

            @pl.when(k >= 2)
            def _():
                back = k - 2
                for r in range(3):
                    gx.sib_copy(me, 0, (back // 4) * 12 + r * 4 + back % 4).wait_send()
        for j, (dev, q) in enumerate(pairs):
            ys[at + j, :unit, :hid] = dot(gb[uid(dev, q), :unit, :fin], w1b[...]).astype(BF16)

        def send():
            for j, (dev, q) in enumerate(pairs):
                gx.sib_copy(dev, q, slots[j], ys.at[at + j, pl.ds(0, unit), pl.ds(0, hid)]).start()
        if isinstance(k, int):
            send()
        add_rows(acc1, pairs, lambda j: ys[at + j, :unit, :hid])
        if not isinstance(k, int):
            send()

    def finish1(m, pairs):
        s = mrows(m)
        z = acc1[s, :]
        for dev, q in pairs:
            z = z + dot(a_v[s, rows_of(dev, q)], gb[uid(dev, q), :unit, :hid])
        acc1[s, :] = z
        h = jnp.maximum(z, 0.0).astype(BF16)
        hb[rows_of(me, m), :] = h
        hown[s, :] = h
        gh.start_own(m)

    phase(gx, add1, zero1, finish1, hook1, True)

    def zero2():
        acc2[...] = jnp.zeros_like(acc2)

    def y2(dev, q):
        return dot_nt(w2b[...], hb[rows_of(dev, q), :]).astype(BF16)

    def add_cols(acc, pairs, operand):
        def body(c):
            s = chunk(c)
            v = acc[:, s]
            for j, (dev, q) in enumerate(pairs):
                v = v + dot_nt(operand(j), a_v[s, rows_of(dev, q)])
            acc[:, s] = v
        loop(rows // CHUNK, body)

    def add2(pairs, t, k):
        for j, (dev, q) in enumerate(pairs):
            ys[j] = y2(dev, q)
        add_cols(acc2, pairs, lambda j: ys[j])

    loss_acc[...] = jnp.zeros_like(loss_acc)

    def hook2(pre, i):
        if i is None:
            for q in range(UNITS):
                xt[:, q * unit:(q + 1) * unit] = gb[uid(me, q), :unit, :fin].T
            return

        @pl.when(i == 0)
        def _():
            cnt_next(2)

        @pl.when(i == 9)
        def _():
            cnt_next(3)
            for k in range(4):
                cnt_copy(k).wait_send()

    def finish2(m, pairs):
        s = mrows(m)

        @pl.when(m == 0)
        def _():
            for j, (dev, q) in enumerate(pairs):
                ys[j] = y2(dev, q)
        z = acc2[:, s]
        for j, (dev, q) in enumerate(pairs):
            z = z + dot_nt(ys[j], a_v[s, rows_of(dev, q)])
        acc2[:, s] = z
        for h in range(unit // LANES):
            at = pl.ds(pl.multiple_of(m * unit + h * LANES, LANES), LANES)
            zc = acc2[:, at]
            row = lax.broadcasted_iota(jnp.int32, (cpad, LANES), 0)
            zm = jnp.where(row < classes, zc, -jnp.inf)
            top = jnp.max(zm, axis=0, keepdims=True)
            log_norm = top + jnp.log(jnp.sum(jnp.exp(zm - top), axis=0, keepdims=True))
            which = m * (unit // LANES) + h
            hot = row == lab_ref[pl.ds(which, 1), :]
            mask = msk_ref[pl.ds(which, 1), :].astype(F32)
            picked = jnp.sum(jnp.where(hot, zc, 0.0), axis=0, keepdims=True)
            loss_acc[...] = loss_acc[...] + mask * (log_norm - picked)
            gr = (jnp.exp(zm - log_norm) - jnp.where(hot, 1.0, 0.0)) * (mask / cnt_src[4][0:1, :])
            gb[uid(me, m), :, h * LANES:(h + 1) * LANES] = gr.astype(BF16)
        gg.start_own(m)

    phase(gh, add2, zero2, finish2, hook2, False)

    def finish3(m, pairs):
        s = mrows(m)
        z = acc2[:, s]
        for dev, q in pairs:
            z = z + dot_nt(gb[uid(dev, q)], a_v[s, rows_of(dev, q)])
        e = z.astype(BF16)
        ys[m] = e
        gz = dot_tn(e, w2b[...])
        hb[rows_of(me, m), :] = jnp.where(acc1[s, :] > 0.0, gz, 0.0).astype(BF16)
        gh.start_own(m)

    phase(gg, lambda pairs, t, k: add_cols(acc2, pairs, lambda j: gb[uid(*pairs[j])]), zero2, finish3,
          lambda pre, i: None, False)

    total_rows = w2acc.shape[0]
    half_rows = total_rows // 2
    piece = half_rows // 8
    chips = DEVICES // 2
    chip = me // 2

    def w2rows(start, n):
        return pl.ds(pl.multiple_of(start, 8), n)

    mine = w2rows(core * half_rows, half_rows)

    def w2_sib():
        out = w2acc.at[w2rows((1 - core) * half_rows, half_rows)]
        return remote(out, w2rcv, w2s_sem.at[0], w2r_sem.at[0], sib)

    def w2_scatter(j):
        to = (chip + j) % chips
        out = w2acc.at[w2rows(core * half_rows + to * piece, piece)]
        return remote(out, w2part.at[j], w2s_sem.at[j], w2r_sem.at[j], to * 2 + core)

    def w2_gather(j, frm):
        to = (chip + j) % chips
        out = w2f.at[w2rows(core * half_rows + frm * piece, piece)]
        return remote(out, out, w2s_sem.at[chips + j], w2r_sem.at[chips + j], to * 2 + core)

    def w2_sib_gather(c):
        out = w2f.at[w2rows(c * half_rows, half_rows)]
        return remote(out, out, w2s_sem.at[chips], w2r_sem.at[chips], sib)

    def hook4(pre, i):
        if i is None:
            w2acc[...] = jnp.zeros_like(w2acc)
            w2acc[:cpad, :] = sum(dot(ys[q], hown[q * unit:(q + 1) * unit, :]) for q in range(UNITS))
            w2acc[total_rows - 1:, :LANES] = loss_acc[...]
            return

        @pl.when(i == 0)
        def _():
            w2_sib().start()

        @pl.when(i == 1)
        def _():
            w2_sib().wait_recv()
            w2acc[mine, :] = w2acc[mine, :] + w2rcv[...]

        @pl.when(i == 7)
        def _():
            w2_sib().wait_send()
            for j in range(1, chips):
                w2_scatter(j).start()

    def finish4(m, pairs):
        z = acc1[...]
        for dev, q in pairs:
            z = z + dot(a_v[:, rows_of(dev, q)], hb[rows_of(dev, q), :])
        w1p[...] = dot(xt[...], z.astype(BF16))

    phase(gh, lambda pairs, t, k: add_rows(acc1, pairs, lambda j: hb[rows_of(*pairs[j]), :]), zero1, finish4, hook4, False, True)

    sl = fin // DEVICES

    def w1rows(dev):
        return pl.ds(pl.multiple_of(dev * sl, sl), sl)

    def w1_scatter(i):
        dev = (me + i) % DEVICES
        return remote(w1p.at[w1rows(dev)], w1r.at[i], w1s_sem.at[i], w1r_sem.at[i], dev)

    def w1_gather(i):
        dev = (me + i) % DEVICES
        return remote(w1f.at[w1rows(me)], w1f.at[w1rows(me)], w1gs_sem.at[i], w1gr_sem.at[i], dev)

    def w1_gather_in(i):
        dev = (me + DEVICES - i) % DEVICES
        return remote(w1f.at[w1rows(dev)], w1f.at[w1rows(dev)], w1gs_sem.at[i], w1gr_sem.at[i], dev)

    for i in range(1, DEVICES):
        w1_scatter(i).start()
    gh.wait_sends()
    own = w2rows(core * half_rows + chip * piece, piece)
    total2 = w2acc[own, :]
    for j in range(1, chips):
        w2_scatter(j).wait_recv()
    for j in range(1, chips):
        total2 = total2 + w2part[j]
    w2f[own, :] = total2
    for j in range(1, chips):
        w2_scatter(j).wait_send()
    for j in range(1, chips):
        w2_gather(j, chip).start()
    total = w1p[w1rows(me), :]
    for i in range(1, DEVICES):
        w1_scatter(i).wait_recv()
    for i in range(1, DEVICES):
        total = total + w1r[i]
    w1f[w1rows(me), :] = total
    for i in range(1, DEVICES):
        w1_scatter(i).wait_send()
    for i in range(1, DEVICES):
        w1_gather(i).start()
    for j in range(1, chips):
        w2_gather(j, (chip + chips - j) % chips).wait_recv()
    w2_sib_gather(core).start()
    for j in range(1, chips):
        w2_gather(j, chip).wait_send()
    w2_sib_gather(1 - core).wait_recv()
    g2_out[...] = w2f[:classes, :]
    loss_out[0, 0] = jnp.sum(w2f[total_rows - 1:, :LANES] / cnt_src[4][0:1, :])
    for i in range(1, DEVICES):
        w1_gather_in(i).wait_recv()
    g1_out[...] = w1f[...]
    w2_sib_gather(core).wait_send()
    for i in range(1, DEVICES):
        w1_gather(i).wait_send()


def solution(mesh):
    axis = mesh.axis_names[0]

    def local_step(adj, x, w1, w2, labels, mask):
        rows, nodes = adj.shape
        fin, hid = w1.shape
        classes = w2.shape[1]
        unit = rows // UNITS
        cpad = -(-classes // 16) * 16
        total_rows = -(-(cpad + 1) // LANES) * LANES
        dma = pltpu.SemaphoreType.DMA
        vm = pl.BlockSpec(memory_space=pltpu.VMEM)
        loss, g1, g2 = pl.pallas_call(
            functools.partial(step_kernel, classes),
            out_shape=(jax.ShapeDtypeStruct((1, 1), F32),
                       jax.ShapeDtypeStruct((fin, hid), F32),
                       jax.ShapeDtypeStruct((classes, hid), F32)),
            in_specs=[pl.BlockSpec(memory_space=pl.ANY)] * 6,
            out_specs=(pl.BlockSpec(memory_space=pltpu.SMEM), vm, vm),
            scratch_shapes=[
                pltpu.VMEM((fin, hid), F32),
                pltpu.VMEM((classes, hid), F32),
                pltpu.VMEM((rows // LANES, LANES), jnp.int32),
                pltpu.VMEM((rows // LANES, LANES), jnp.int32),
                dma((UNITS + 4,)),
                pltpu.VMEM((rows, nodes), BF16),
                pltpu.VMEM((nodes // unit, cpad, unit), BF16),
                pltpu.VMEM((nodes, hid), BF16),
                pltpu.VMEM((rows, hid), F32),
                pltpu.VMEM((cpad, rows), F32),
                pltpu.VMEM((UNITS + 7, cpad, unit), BF16),
                pltpu.VMEM((rows, hid), BF16),
                pltpu.VMEM((fin, hid), BF16),
                pltpu.VMEM((cpad, hid), BF16),
                pltpu.VMEM((total_rows, hid), F32),
                pltpu.VMEM((total_rows // 2, hid), F32),
                pltpu.VMEM((8, total_rows // 16, hid), F32),
                pltpu.VMEM((total_rows, hid), F32),
                pltpu.VMEM((fin, hid), F32),
                pltpu.VMEM((DEVICES, fin // DEVICES, hid), F32),
                pltpu.VMEM((fin, hid), F32),
                pltpu.VMEM((5, 8, LANES), F32),
                pltpu.VMEM((4, 8, LANES), F32),
                pltpu.VMEM((1, LANES), F32),
                pltpu.VMEM((fin, rows), BF16),
                dma((DEVICES,)),
                dma((2, 30)), dma((2, 30)), dma((2, 32)), dma((2, 32)),
                dma((DEVICES,)), dma((DEVICES,)), dma((DEVICES,)), dma((DEVICES,)),
                dma((DEVICES,)), dma((DEVICES,)), dma((DEVICES,)), dma((DEVICES,)),
            ],
            compiler_params=pltpu.CompilerParams(collective_id=0, has_side_effects=True,
                                                 vmem_limit_bytes=67043328),
            name="gcn_step",
        )(adj, x, w1, w2.T, labels.reshape(rows // LANES, LANES), mask.reshape(rows // LANES, LANES))
        return loss[0, 0], g1, g2.T

    return jax.shard_map(local_step, mesh=mesh,
                         in_specs=(P(axis, None), P(axis, None), P(None, None), P(None, None), P(axis), P(axis)),
                         out_specs=(P(), P(None, None), P(None, None)), check_vma=False)
```

```python
import functools

import jax
import jax.numpy as jnp
from jax import lax
from jax.experimental import pallas as pl
from jax.experimental.pallas import tpu as pltpu
from jax.sharding import PartitionSpec as P

F32 = jnp.float32
BF16 = jnp.bfloat16
MESH = pl.DeviceIdType.MESH
DEVICES = 16
UNITS = 4
LANES = 128
CHUNK = 1024


def dot(a, b):
    return jnp.dot(a, b, preferred_element_type=F32)


def dot_tn(a, b):
    return lax.dot_general(a, b, (((0,), (0,)), ((), ())), preferred_element_type=F32)


def dot_nt(a, b):
    return lax.dot_general(a, b, (((1,), (1,)), ((), ())), preferred_element_type=F32)


def loop(n, fn):
    lax.fori_loop(0, n, lambda i, c: (fn(i), c)[1], 0)


def step_kernel(classes, adj, x_hbm, w1_hbm, w2_hbm, lab_hbm, msk_hbm,
                loss_out, g1_out, g2_out,
                w1_ref, w2_ref, lab_ref, msk_ref, in_sem,
                a_v, gb, hb, acc1, acc2, ys, hown, w1b, w2b,
                w2acc, w2rcv, w2part, w2f, w1p, w1r, w1f, cnt_src, cnt_rcv, loss_acc, xt,
                a_sem, rsem, ssem, sib_rsem, sib_ssem, cs_sem, cr_sem,
                w2s_sem, w2r_sem, w1s_sem, w1r_sem, w1gs_sem, w1gr_sem):
    rows = x_hbm.shape[0]
    fin = x_hbm.shape[1]
    unit = rows // UNITS
    hid = w1_ref.shape[1]
    cpad = w2b.shape[0]
    me = lax.axis_index("nodes")
    core = me % 2
    sib = me + 1 - 2 * core
    bit = [(me // v) % 2 for v in (2, 4, 8)]
    step = [v * (1 - 2 * b) for v, b in zip((2, 4, 8), bit)]
    own_d = [(1 - core) * step[r] + core * step[(r + 1) % 3] for r in range(3)]
    sib_d = [core * step[r] + (1 - core) * step[(r + 1) % 3] for r in range(3)]
    role_bit = [(1 - core) * bit[r] + core * bit[(r + 1) % 3] for r in range(3)]
    nbr = [me + d for d in own_d]

    def src_dev(base, deltas, hop, r):
        return base + deltas[r] + hop * deltas[(r + 2) % 3]

    anti = me + own_d[0] + own_d[1] + own_d[2]
    anti_sib = anti + 1 - 2 * core

    def remote(src, dst, ss, rs, dev):
        return pltpu.make_async_remote_copy(src_ref=src, dst_ref=dst, send_sem=ss, recv_sem=rs,
                                            device_id=(dev,), device_id_type=MESH)

    barrier = pltpu.get_barrier_semaphore()
    for dev in [sib] + nbr:
        pl.semaphore_signal(barrier, inc=1, device_id=(dev,), device_id_type=MESH)

    def uid(dev, q):
        return dev * UNITS + q

    order = [me, sib]
    for hop in (0, 1):
        order += [src_dev(me, own_d, hop, r) for r in range(3)]
        order += [src_dev(sib, sib_d, hop, r) for r in range(3)]
    order += [anti, anti_sib]

    def a_cols(dev):
        return pl.ds(pl.multiple_of(dev * rows, rows), rows)

    def a_copy(i):
        return pltpu.make_async_copy(adj.at[:, a_cols(order[i])], a_v.at[:, a_cols(order[i])], a_sem.at[i])

    x_units = [pltpu.make_async_copy(x_hbm.at[pl.ds(q * unit, unit)], gb.at[uid(me, q), pl.ds(0, unit), pl.ds(0, fin)],
                                     in_sem.at[q]) for q in range(UNITS)]
    inputs = [pltpu.make_async_copy(src, dst, in_sem.at[UNITS + i]) for i, (src, dst) in enumerate(
        [(w1_hbm, w1_ref), (w2_hbm, w2_ref), (msk_hbm, msk_ref), (lab_hbm, lab_ref)])]
    for c in x_units + inputs:
        c.start()
    for i in range(2):
        a_copy(i).start()

    def rows_of(dev, q):
        return pl.ds(pl.multiple_of(dev * rows + q * unit, unit), unit)

    pl.semaphore_wait(barrier, 4)

    def pick(f, vals):
        return jnp.where(f == 0, vals[0], jnp.where(f == 1, vals[1], vals[2]))

    class Gather:
        def __init__(self, view, height, par, sib_view=None):
            self.view, self.height, self.par = view, height, par
            self.shared, self.sib_view = sib_view is not None, sib_view or view

        def hop_copy(self, dev, q, to, sslot, rslot):
            v = self.view(dev, q)
            return remote(v, v, ssem.at[self.par, sslot], rsem.at[self.par, rslot], to)

        def sib_copy(self, dev, q, slot, src=None):
            v = self.sib_view(dev, q)
            return remote(v if src is None else src, v, sib_ssem.at[self.par, slot], sib_rsem.at[self.par, slot], sib)

        def own_copies(self, q):
            hops = [self.hop_copy(me, q, nbr[r], r * 4 + q, r * 4 + q) for r in range(3)]
            return hops if self.shared else hops + [self.sib_copy(me, q, 28 + q)]

        def start_own(self, q):
            for c in self.own_copies(q):
                c.start()

        def forward(self, q):
            return [self.hop_copy(src_dev(me, own_d, 0, r), q, nbr[(r + 1) % 3], 12 + r * 4 + q,
                                  12 + ((r + 1) % 3) * 4 + q) for r in range(3)]

        def last_forward(self, q):
            to = q % 3
            dev = pick((to + 2) % 3, [src_dev(me, own_d, 1, r) for r in range(3)])
            return self.hop_copy(dev, q, pick(to, nbr), 24 + q, 24 + q)

        def thirds(self, dev):
            tiles = self.height // 16
            at = [0, tiles // 3 * 16, 2 * (tiles // 3) * 16, self.height]
            return [self.view(dev, 3).at[pl.ds(at[t], at[t + 1] - at[t])] for t in range(3)]

        def third_copy(self, t):
            v = self.thirds(src_dev(me, own_d, 1, (t + 2) % 3))[t]
            return remote(v, v, ssem.at[self.par, 27 + t], rsem.at[self.par, 27 + t], nbr[t])

        def third_in(self, t):
            v = self.thirds(anti)[t]
            return remote(v, v, ssem.at[self.par, 27 + t], rsem.at[self.par, 27 + t], nbr[t])

        def arrive(self, hop, q):
            for r in range(3):
                d = src_dev(me, own_d, hop, r)
                self.hop_copy(d, q, nbr[r], r * 4 + q, hop * 12 + r * 4 + q).wait_recv()

            @pl.when(hop == 0)
            def _():
                for c in self.forward(q):
                    c.start()

            @pl.when((hop == 1) & (q < 3))
            def _():
                self.last_forward(q).start()

            @pl.when((hop == 1) & (q == 3))
            def _():
                for t in range(3):
                    self.third_copy(t).start()
            if not self.shared:
                for r in range(3):
                    self.sib_copy(src_dev(me, own_d, hop, r), q, hop * 12 + r * 4 + q).start()

        def arrive_last(self, q):
            if q < 3:
                self.hop_copy(anti, q, nbr[0], 24 + q, 24 + q).wait_recv()
            else:
                for t in range(3):
                    self.third_in(t).wait_recv()
            if not self.shared:
                self.sib_copy(anti, q, 24 + q).start()

        def sib_wait(self, hop, q):
            for r in range(3):
                self.sib_copy(src_dev(sib, sib_d, hop, r), q, hop * 12 + r * 4 + q).wait_recv()

        def sib_wait_own(self, q):
            self.sib_copy(sib, q, 28 + q).wait_recv()

        def sib_wait_last(self, q):
            self.sib_copy(anti_sib, q, 24 + q).wait_recv()

        def wait_sends(self):
            def body(q):
                for c in self.own_copies(q) + self.forward(q):
                    c.wait_send()
                if not self.shared:
                    for slot in (q, 4 + q, 8 + q, 12 + q, 16 + q, 20 + q, 24 + q):
                        self.sib_copy(me, q, slot).wait_send()
            loop(UNITS, body)
            if self.shared:
                for slot in (15, 19, 23, 24, 25, 26, 27, 28, 29, 30, 31):
                    self.sib_copy(me, 0, slot).wait_send()
            for q in range(3):
                self.last_forward(q).wait_send()
            for t in range(3):
                self.third_copy(t).wait_send()

    def phase(g, add, zero, finish, hook, first, whole=False):
        def a_wait(lo, hi):
            if first:
                for i in range(lo, hi):
                    a_copy(i).wait()

        zero()

        def halves(fn, n=2):
            if g.shared:
                fn(0)
                fn(1)
            else:
                loop(n, fn)

        def near(t):
            if first and t == 0:
                a_wait(0, 1)

            def wait_sib():
                for q in range(UNITS):
                    g.sib_wait_own(q)
                a_wait(1, 2)
            if not g.shared:
                pl.when(t == 1)(wait_sib)
            elif t == 1:
                wait_sib()
            dev = me + t * (sib - me)
            add([(dev, q) for q in range(UNITS)], t, -1)
        halves(near)
        hook(-1, None)

        def group(i):
            @pl.when(i < 8)
            def _():
                g.arrive(i // 4, i % 4)

            @pl.when(i == 8)
            def _():
                for j in range(3):
                    g.arrive_last(j)

            if g.shared:
                @pl.when(i == 9)
                def _():
                    g.arrive_last(3)
            hook(None, i)

            def half(t):
                if g.shared:
                    k, sb, live = i - t, t, (i - t >= 0) & (i - t <= 8)
                else:
                    k, sb = i - t * (2 - t), (t + 1) // 2
                    live = (t == 0) | ((t == 1) & (i >= 1) & (i <= 7)) | ((t == 2) & (i >= 7))
                hop, q, far = (k // 4) % 2, k % 4, k // 8

                if not g.shared:
                    @pl.when((t == 2) & (i == 8))
                    def _():
                        g.arrive_last(3)
                        add([(anti, 3)], 0, 9)

                @pl.when(live)
                def _():
                    def on_sib(cond, fn):
                        if not g.shared:
                            pl.when((t >= 1) & cond)(fn)
                        elif t == 1:
                            pl.when(cond)(fn)

                    on_sib(k < 8, lambda: g.sib_wait(hop, q))
                    on_sib(k == 8, lambda: [g.sib_wait_last(j) for j in range(3)] and None)
                    if first:
                        for key, (lo, hi) in {(0, 0): (2, 5), (0, 1): (5, 8), (4, 0): (8, 11), (4, 1): (11, 14),
                                              (8, 0): (14, 15), (8, 1): (15, 16)}.items():
                            if t == key[1]:
                                @pl.when(k == key[0])
                                def _(lo=lo, hi=hi):
                                    a_wait(lo, hi)
                    pairs = []
                    for r in range(3):
                        o, s = src_dev(me, own_d, hop, r), src_dev(sib, sib_d, hop, r)
                        near_dev = o + sb * (s - o)
                        far_dev = anti + sb * (anti_sib - anti)
                        pairs.append((near_dev + far * (far_dev - near_dev), q + far * (r - q)))
                    add(pairs, t, k)
            halves(half, 3)
        if g.shared:
            loop(10, group)
            add([(anti, 3)], 0, 9)
        else:
            loop(9, group)
            hook(None, 9)
        g.sib_wait_last(3)

        if whole:
            finish(None, [(anti_sib, 3)])
            return

        def last(m):
            @pl.when(m == UNITS - 1)
            def _():
                g.wait_sends()
            finish(m, [(anti_sib, 3)])
        loop(UNITS, last)

    gx = Gather(lambda dev, q: gb.at[uid(dev, q), pl.ds(0, unit), pl.ds(0, fin)], unit, 0,
                lambda dev, q: gb.at[uid(dev, q), pl.ds(0, unit), pl.ds(0, hid)])
    gh = Gather(lambda dev, q: hb.at[rows_of(dev, q)], unit, 1)
    gg = Gather(lambda dev, q: gb.at[uid(dev, q)], cpad, 0)

    def mrows(m):
        return pl.ds(pl.multiple_of(m * unit, unit), unit)

    def chunk(c):
        return pl.ds(pl.multiple_of(c * CHUNK, CHUNK), CHUNK)

    for q in range(UNITS):
        x_units[q].wait()
        gx.start_own(q)
    for i in range(2, 8):
        a_copy(i).start()
    for c in inputs:
        c.wait()
    w1b[...] = w1_ref[...].astype(BF16)
    w2acc[...] = jnp.zeros_like(w2acc)
    w2acc[:classes, :] = w2_ref[...]
    w2b[...] = w2acc[:cpad, :].astype(BF16)

    partners = [sib] + nbr

    def cnt_copy(k):
        return remote(cnt_src.at[k], cnt_rcv.at[k], cs_sem.at[k], cr_sem.at[k], partners[k])

    def cnt_next(k):
        cnt_copy(k).wait_recv()
        cnt_src[k + 1] = cnt_src[k] + cnt_rcv[k]
        if k < 3:
            cnt_copy(k + 1).start()

    local = jnp.sum(msk_ref[...].astype(F32), axis=1, keepdims=True)
    local = jnp.sum(local, axis=0, keepdims=True)
    cnt_src[0] = jnp.broadcast_to(local, (8, LANES))

    def hook1(pre, i):
        if i is None:
            for j in range(8, DEVICES):
                a_copy(j).start()
            cnt_copy(0).start()
            return

        @pl.when(i == 1)
        def _():
            cnt_next(0)

        @pl.when(i == 9)
        def _():
            cnt_next(1)

    def zero1():
        acc1[...] = jnp.zeros_like(acc1)

    def add_rows(acc, pairs, operand):
        def body(c):
            s = chunk(c)
            v = acc[s, :]
            for j, (dev, q) in enumerate(pairs):
                v = v + dot(a_v[s, rows_of(dev, q)], operand(j))
            acc[s, :] = v
        loop(rows // CHUNK, body)

    def add1(pairs, t, k):
        if t == 1:
            add_rows(acc1, pairs, lambda j: gb[uid(*pairs[j]), :unit, :hid])
            return
        n = len(pairs)
        if isinstance(k, int):
            at = 0 if k < 0 else 10
            slots = [28 + j for j in range(n)] if k < 0 else [27]
        else:
            hop, q, far = (k // 4) % 2, k % 4, k // 8
            at = UNITS + 3 * (k % 2)
            slots = [hop * 12 + r * 4 + q + far * (24 + r - hop * 12 - r * 4 - q) for r in range(3)]

            @pl.when(k >= 2)
            def _():
                back = k - 2
                for r in range(3):
                    gx.sib_copy(me, 0, (back // 4) * 12 + r * 4 + back % 4).wait_send()
        for j, (dev, q) in enumerate(pairs):
            ys[at + j, :unit, :hid] = dot(gb[uid(dev, q), :unit, :fin], w1b[...]).astype(BF16)

        def send():
            for j, (dev, q) in enumerate(pairs):
                gx.sib_copy(dev, q, slots[j], ys.at[at + j, pl.ds(0, unit), pl.ds(0, hid)]).start()
        if isinstance(k, int):
            send()
        add_rows(acc1, pairs, lambda j: ys[at + j, :unit, :hid])
        if not isinstance(k, int):
            send()

    def finish1(m, pairs):
        s = mrows(m)
        z = acc1[s, :]
        for dev, q in pairs:
            z = z + dot(a_v[s, rows_of(dev, q)], gb[uid(dev, q), :unit, :hid])
        acc1[s, :] = z
        h = jnp.maximum(z, 0.0).astype(BF16)
        hb[rows_of(me, m), :] = h
        hown[s, :] = h
        gh.start_own(m)

    phase(gx, add1, zero1, finish1, hook1, True)

    def zero2():
        acc2[...] = jnp.zeros_like(acc2)

    def y2(dev, q):
        return dot_nt(w2b[...], hb[rows_of(dev, q), :]).astype(BF16)

    def add_cols(acc, pairs, operand):
        def body(c):
            s = chunk(c)
            v = acc[:, s]
            for j, (dev, q) in enumerate(pairs):
                v = v + dot_nt(operand(j), a_v[s, rows_of(dev, q)])
            acc[:, s] = v
        loop(rows // CHUNK, body)

    def add2(pairs, t, k):
        for j, (dev, q) in enumerate(pairs):
            ys[j] = y2(dev, q)
        add_cols(acc2, pairs, lambda j: ys[j])

    loss_acc[...] = jnp.zeros_like(loss_acc)

    def hook2(pre, i):
        if i is None:
            for q in range(UNITS):
                xt[:, q * unit:(q + 1) * unit] = gb[uid(me, q), :unit, :fin].T
            return

        @pl.when(i == 0)
        def _():
            cnt_next(2)

        @pl.when(i == 9)
        def _():
            cnt_next(3)
            for k in range(4):
                cnt_copy(k).wait_send()

    def finish2(m, pairs):
        s = mrows(m)

        @pl.when(m == 0)
        def _():
            for j, (dev, q) in enumerate(pairs):
                ys[j] = y2(dev, q)
        z = acc2[:, s]
        for j, (dev, q) in enumerate(pairs):
            z = z + dot_nt(ys[j], a_v[s, rows_of(dev, q)])
        acc2[:, s] = z
        for h in range(unit // LANES):
            at = pl.ds(pl.multiple_of(m * unit + h * LANES, LANES), LANES)
            zc = acc2[:, at]
            row = lax.broadcasted_iota(jnp.int32, (cpad, LANES), 0)
            zm = jnp.where(row < classes, zc, -jnp.inf)
            top = jnp.max(zm, axis=0, keepdims=True)
            log_norm = top + jnp.log(jnp.sum(jnp.exp(zm - top), axis=0, keepdims=True))
            which = m * (unit // LANES) + h
            hot = row == lab_ref[pl.ds(which, 1), :]
            mask = msk_ref[pl.ds(which, 1), :].astype(F32)
            picked = jnp.sum(jnp.where(hot, zc, 0.0), axis=0, keepdims=True)
            loss_acc[...] = loss_acc[...] + mask * (log_norm - picked)
            gr = (jnp.exp(zm - log_norm) - jnp.where(hot, 1.0, 0.0)) * (mask / cnt_src[4][0:1, :])
            gb[uid(me, m), :, h * LANES:(h + 1) * LANES] = gr.astype(BF16)
        gg.start_own(m)

    phase(gh, add2, zero2, finish2, hook2, False)

    def finish3(m, pairs):
        s = mrows(m)
        z = acc2[:, s]
        for dev, q in pairs:
            z = z + dot_nt(gb[uid(dev, q)], a_v[s, rows_of(dev, q)])
        e = z.astype(BF16)
        ys[m] = e
        gz = dot_tn(e, w2b[...])
        hb[rows_of(me, m), :] = jnp.where(acc1[s, :] > 0.0, gz, 0.0).astype(BF16)
        gh.start_own(m)

    phase(gg, lambda pairs, t, k: add_cols(acc2, pairs, lambda j: gb[uid(*pairs[j])]), zero2, finish3,
          lambda pre, i: None, False)

    total_rows = w2acc.shape[0]
    half_rows = total_rows // 2
    piece = half_rows // 8
    chips = DEVICES // 2
    chip = me // 2

    def w2rows(start, n):
        return pl.ds(pl.multiple_of(start, 8), n)

    mine = w2rows(core * half_rows, half_rows)

    def w2_sib():
        out = w2acc.at[w2rows((1 - core) * half_rows, half_rows)]
        return remote(out, w2rcv, w2s_sem.at[0], w2r_sem.at[0], sib)

    def w2_scatter(j):
        to = (chip + j) % chips
        out = w2acc.at[w2rows(core * half_rows + to * piece, piece)]
        return remote(out, w2part.at[j], w2s_sem.at[j], w2r_sem.at[j], to * 2 + core)

    def w2_gather(j, frm):
        to = (chip + j) % chips
        out = w2f.at[w2rows(core * half_rows + frm * piece, piece)]
        return remote(out, out, w2s_sem.at[chips + j], w2r_sem.at[chips + j], to * 2 + core)

    def w2_sib_gather(c):
        out = w2f.at[w2rows(c * half_rows, half_rows)]
        return remote(out, out, w2s_sem.at[chips], w2r_sem.at[chips], sib)

    def hook4(pre, i):
        if i is None:
            w2acc[...] = jnp.zeros_like(w2acc)
            w2acc[:cpad, :] = sum(dot(ys[q], hown[q * unit:(q + 1) * unit, :]) for q in range(UNITS))
            w2acc[total_rows - 1:, :LANES] = loss_acc[...]
            return

        @pl.when(i == 0)
        def _():
            w2_sib().start()

        @pl.when(i == 1)
        def _():
            w2_sib().wait_recv()
            w2acc[mine, :] = w2acc[mine, :] + w2rcv[...]

        @pl.when(i == 7)
        def _():
            w2_sib().wait_send()
            for j in range(1, chips):
                w2_scatter(j).start()

    def finish4(m, pairs):
        z = acc1[...]
        for dev, q in pairs:
            z = z + dot(a_v[:, rows_of(dev, q)], hb[rows_of(dev, q), :])
        w1p[...] = dot(xt[...], z.astype(BF16))

    phase(gh, lambda pairs, t, k: add_rows(acc1, pairs, lambda j: hb[rows_of(*pairs[j]), :]), zero1, finish4, hook4, False, True)

    sl = fin // DEVICES

    def w1rows(dev):
        return pl.ds(pl.multiple_of(dev * sl, sl), sl)

    def flip(i):
        return me + (i & 1) * (1 - 2 * core) + sum(((i >> (j + 1)) & 1) * step[j] for j in range(3))

    far_first = sorted(range(1, DEVICES), key=lambda i: -bin(i >> 1).count("1"))

    def w1_scatter(i):
        dev = flip(i)
        return remote(w1p.at[w1rows(dev)], w1r.at[i], w1s_sem.at[i], w1r_sem.at[i], dev)

    def w1_gather(i):
        dev = flip(i)
        return remote(w1f.at[w1rows(me)], w1f.at[w1rows(me)], w1gs_sem.at[i], w1gr_sem.at[i], dev)

    def w1_gather_in(i):
        dev = flip(i)
        return remote(w1f.at[w1rows(dev)], w1f.at[w1rows(dev)], w1gs_sem.at[i], w1gr_sem.at[i], dev)

    for i in far_first:
        w1_scatter(i).start()
    gh.wait_sends()
    own = w2rows(core * half_rows + chip * piece, piece)
    total2 = w2acc[own, :]
    for j in range(1, chips):
        w2_scatter(j).wait_recv()
    for j in range(1, chips):
        total2 = total2 + w2part[j]
    w2f[own, :] = total2
    for j in range(1, chips):
        w2_scatter(j).wait_send()
    for j in range(1, chips):
        w2_gather(j, chip).start()
    total = w1p[w1rows(me), :]
    for i in range(1, DEVICES):
        w1_scatter(i).wait_recv()
    for i in range(1, DEVICES):
        total = total + w1r[i]
    w1f[w1rows(me), :] = total
    for i in range(1, DEVICES):
        w1_scatter(i).wait_send()
    for i in far_first:
        w1_gather(i).start()
    for j in range(1, chips):
        w2_gather(j, (chip + chips - j) % chips).wait_recv()
    w2_sib_gather(core).start()
    for j in range(1, chips):
        w2_gather(j, chip).wait_send()
    w2_sib_gather(1 - core).wait_recv()
    g2_out[...] = w2f[:classes, :]
    loss_out[0, 0] = jnp.sum(w2f[total_rows - 1:, :LANES] / cnt_src[4][0:1, :])
    for i in range(1, DEVICES):
        w1_gather_in(i).wait_recv()
    g1_out[...] = w1f[...]
    w2_sib_gather(core).wait_send()
    for i in range(1, DEVICES):
        w1_gather(i).wait_send()


def solution(mesh):
    axis = mesh.axis_names[0]

    def local_step(adj, x, w1, w2, labels, mask):
        rows, nodes = adj.shape
        fin, hid = w1.shape
        classes = w2.shape[1]
        unit = rows // UNITS
        cpad = -(-classes // 16) * 16
        total_rows = -(-(cpad + 1) // LANES) * LANES
        dma = pltpu.SemaphoreType.DMA
        vm = pl.BlockSpec(memory_space=pltpu.VMEM)
        loss, g1, g2 = pl.pallas_call(
            functools.partial(step_kernel, classes),
            out_shape=(jax.ShapeDtypeStruct((1, 1), F32),
                       jax.ShapeDtypeStruct((fin, hid), F32),
                       jax.ShapeDtypeStruct((classes, hid), F32)),
            in_specs=[pl.BlockSpec(memory_space=pl.ANY)] * 6,
            out_specs=(pl.BlockSpec(memory_space=pltpu.SMEM), vm, vm),
            scratch_shapes=[
                pltpu.VMEM((fin, hid), F32),
                pltpu.VMEM((classes, hid), F32),
                pltpu.VMEM((rows // LANES, LANES), jnp.int32),
                pltpu.VMEM((rows // LANES, LANES), jnp.int32),
                dma((UNITS + 4,)),
                pltpu.VMEM((rows, nodes), BF16),
                pltpu.VMEM((nodes // unit, cpad, unit), BF16),
                pltpu.VMEM((nodes, hid), BF16),
                pltpu.VMEM((rows, hid), F32),
                pltpu.VMEM((cpad, rows), F32),
                pltpu.VMEM((UNITS + 7, cpad, unit), BF16),
                pltpu.VMEM((rows, hid), BF16),
                pltpu.VMEM((fin, hid), BF16),
                pltpu.VMEM((cpad, hid), BF16),
                pltpu.VMEM((total_rows, hid), F32),
                pltpu.VMEM((total_rows // 2, hid), F32),
                pltpu.VMEM((8, total_rows // 16, hid), F32),
                pltpu.VMEM((total_rows, hid), F32),
                pltpu.VMEM((fin, hid), F32),
                pltpu.VMEM((DEVICES, fin // DEVICES, hid), F32),
                pltpu.VMEM((fin, hid), F32),
                pltpu.VMEM((5, 8, LANES), F32),
                pltpu.VMEM((4, 8, LANES), F32),
                pltpu.VMEM((1, LANES), F32),
                pltpu.VMEM((fin, rows), BF16),
                dma((DEVICES,)),
                dma((2, 30)), dma((2, 30)), dma((2, 32)), dma((2, 32)),
                dma((DEVICES,)), dma((DEVICES,)), dma((DEVICES,)), dma((DEVICES,)),
                dma((DEVICES,)), dma((DEVICES,)), dma((DEVICES,)), dma((DEVICES,)),
            ],
            compiler_params=pltpu.CompilerParams(collective_id=0, has_side_effects=True,
                                                 vmem_limit_bytes=67043328),
            name="gcn_step",
        )(adj, x, w1, w2.T, labels.reshape(rows // LANES, LANES), mask.reshape(rows // LANES, LANES))
        return loss[0, 0], g1, g2.T

    return jax.shard_map(local_step, mesh=mesh,
                         in_specs=(P(axis, None), P(axis, None), P(None, None), P(None, None), P(axis), P(axis)),
                         out_specs=(P(), P(None, None), P(None, None)), check_vma=False)
```
